256 devices in a mesh: slab: 128 (over z, y, x), sub: 2 (over core).
Axes of the slice: x: 4, y: 4, z: 8, core: 2. Of those that a mesh axis runs over, the one named last changes fastest.
Arguments:
- start: float32 [4, 768, 32, 256], P(None, 'slab', 'sub'), may hold values from -6 to 6
- wind: float32 [3, 768, 32, 256], P(None, 'slab', 'sub'), may hold values from -4 to 4
- reaction: float32 [768, 32, 256], P('slab', 'sub'), may hold values from 0.5 to 4
- mass: float32 [768, 32, 256], P('slab', 'sub'), may hold values from 0.5 to 2
Outputs:
- basis: float32 [4, 4, 768, 32, 256], P(None, None, 'slab', 'sub')
- search: float32 [3, 4, 768, 32, 256], P(None, None, 'slab', 'sub')
- hessenberg: float32 [4, 3], replicated
The draws below stay inside these ranges and needn't reach their ends.
All inputs are finite; a program needn't handle non-finite values.
Results may differ from the reference program's by a relative error of at most 0.0003.
Values sent between devices are 32-bit elements; how exact they have to be, the bound alone decides.
A program may use at most 64 MiB of HBM per device.

```python
import math
import jax
import jax.numpy as jnp

NZ = 256
ITERS = 3
NX = 768
NY = 32


def level_of(key, shape, split, low, top_value):
    loudness, own = 1.0, jax.random.fold_in(key, 6)
    for axis_at, blocks in split:
        draws = jnp.exp(jax.random.uniform(jax.random.fold_in(own, axis_at), (blocks,), jnp.float32, low / len(split), top_value / len(split)))
        loudness = loudness * jnp.repeat(draws, shape[axis_at] // blocks).reshape([-1 if axis == axis_at else 1 for axis in range(len(shape))])
    return loudness


def normal_values(own_key, shape, spread, reach, split=(), held_as=jnp.bfloat16):
    loudness = level_of(own_key, shape, split, -0.22, 0.18) if split else 1.0
    values = jax.random.normal(own_key, shape, jnp.float32) * spread * loudness
    return jnp.minimum(jnp.maximum(values, -reach), reach).astype(held_as)


def setup_inputs(seed: int = 0) -> dict:
    splits = jax.random.split(jax.random.key(seed), 5)
    return {
        "start": normal_values(splits[0], (4, NX, NY, NZ), 1.0, 6.0, ((1, 128), (2, 2)), jnp.float32),
        "wind": normal_values(splits[1], (3, NX, NY, NZ), 1.0, 4.0, ((1, 128), (2, 2)), jnp.float32),
        "reaction": jnp.clip(jnp.exp(math.log(4.0) - 2.0794415 * jax.random.uniform(splits[2], (NX, NY, NZ), jnp.float32) ** level_of(splits[2], (NX, NY, NZ), ((0, 128), (1, 2)), -0.2, 0.2)), 0.5, 4.0),
        "mass": jnp.clip(jnp.exp(math.log(2.0) - 1.3862944 * jax.random.uniform(splits[3], (NX, NY, NZ), jnp.float32) ** level_of(splits[3], (NX, NY, NZ), ((0, 128), (1, 2)), -0.2, 0.2)), 0.5, 2.0),
    }


def grid_pad(field):
    return jnp.pad(field, [(0, 0)] * (field.ndim - 3) + [(1, 1), (1, 1), (0, 0)])

def neighbour_sets(padded):
    center = padded[..., 1:-1, 1:-1, :]
    zero_face = jnp.zeros_like(center[..., :1])
    plus_side = (padded[..., 2:, 1:-1, :], padded[..., 1:-1, 2:, :], jnp.concatenate([center[..., 1:], zero_face], -1))
    minus_side = (padded[..., :-2, 1:-1, :], padded[..., 1:-1, :-2, :], jnp.concatenate([zero_face, center[..., :-1]], -1))
    return (center, plus_side, minus_side)

def six_sum(plus_side, minus_side):
    total = plus_side[0] + minus_side[0]
    total = total + plus_side[1] + minus_side[1]
    return total + plus_side[2] + minus_side[2]

def transport(padded, reaction_k, wind_k):
    center, plus_side, minus_side = neighbour_sets(padded)
    convect = wind_k[0] * (plus_side[0] - minus_side[0])
    convect = convect + wind_k[1] * (plus_side[1] - minus_side[1])
    convect = convect + wind_k[2] * (plus_side[2] - minus_side[2])
    return (6.0 + reaction_k) * center - six_sum(plus_side, minus_side) + 0.5 * convect

def gradient(padded):
    center, plus_side, minus_side = neighbour_sets(padded)
    return jnp.stack([0.5 * (plus_side[dim_index] - minus_side[dim_index]) for dim_index in range(3)])

def divergence(padded):
    center, plus_side, minus_side = neighbour_sets(padded)
    total = 0.5 * (plus_side[0][0] - minus_side[0][0])
    total = total + 0.5 * (plus_side[1][1] - minus_side[1][1])
    return total + 0.5 * (plus_side[2][2] - minus_side[2][2])

def pressure_poisson(padded):
    center, plus_side, minus_side = neighbour_sets(padded)
    return 7.0 * center - six_sum(plus_side, minus_side)

def oseen_apply(padded, reaction_k, wind_k):
    upper = transport(padded[:3], reaction_k, wind_k) + gradient(padded[3])
    center, plus_side, minus_side = neighbour_sets(padded[3])
    lower = -divergence(padded[:3]) - 0.5 * (6.0 * center - six_sum(plus_side, minus_side))
    return jnp.concatenate([upper, lower[None]], 0)

def precondition(vector, wind, reaction, mass):
    pressure = vector[3]
    first_guess = pressure / 7.0
    second_guess = first_guess + (pressure - pressure_poisson(grid_pad(first_guess))) / 7.0
    schur = -transport(grid_pad(second_guess), reaction, wind) / mass
    residue = vector[:3] - gradient(grid_pad(schur))
    diagonal = 6.0 + reaction
    velocity_first = residue / diagonal
    velocity = velocity_first + (residue - transport(grid_pad(velocity_first), reaction, wind)) / diagonal
    return jnp.concatenate([velocity, schur[None]], 0)

def reference(start, wind, reaction, mass):
    scale_start = jnp.sqrt(jnp.sum(start * start))
    vectors = [start / scale_start]
    searches = []
    hess = jnp.zeros((ITERS + 1, ITERS), jnp.float32)
    for column in range(ITERS):
        found = precondition(vectors[column], wind, reaction, mass)
        searches.append(found)
        image = oseen_apply(grid_pad(found), reaction, wind)
        projected = jnp.stack([jnp.sum(vectors[row] * image) for row in range(column + 1)])
        for row in range(column + 1):
            image = image - projected[row] * vectors[row]
        norm_next = jnp.sqrt(jnp.sum(image * image))
        hess = hess.at[:column + 1, column].set(projected)
        hess = hess.at[column + 1, column].set(norm_next)
        vectors.append(image / norm_next)
    return (jnp.stack(vectors), jnp.stack(searches), hess)
```

```python
import functools

import jax
import jax.numpy as jnp
from jax import lax
from jax.experimental import pallas as pl
from jax.experimental.pallas import tpu as pltpu
from jax.sharding import PartitionSpec as P

MESH_ID = pl.DeviceIdType.MESH
NX_T, NY_T, NZ_T = 4, 4, 8
ROWS = 24
HALF = 128


def lane_is(lane):
    return lax.broadcasted_iota(jnp.int32, (ROWS, HALF), 1) == lane


def get(ref, *lead):
    return ref[(*lead, slice(None), pl.ds(0, HALF))], ref[(*lead, slice(None), pl.ds(HALF, HALF))]


def put(ref, value, *lead):
    ref[(*lead, slice(None), pl.ds(0, HALF))] = value[0]
    ref[(*lead, slice(None), pl.ds(HALF, HALF))] = value[1]


def up_z(f, last):
    low, high = pltpu.roll(f[0], HALF - 1, 1), pltpu.roll(f[1], HALF - 1, 1)
    return jnp.where(last, high, low), jnp.where(last, 0.0, high)


def down_z(f, first):
    low, high = pltpu.roll(f[0], 1, 1), pltpu.roll(f[1], 1, 1)
    return jnp.where(first, 0.0, low), jnp.where(first, low, high)


def up_y(f):
    return tuple(pltpu.roll(h, ROWS - 1, 0) for h in f)


def down_y(f):
    return tuple(pltpu.roll(h, 1, 0) for h in f)


def krylov_kernel(
    start, wind, reac, mass,
    w0_out, w1_out, w2_out, z0_out, z1_out, z2_out, gram_out,
    vec, coef, work, t1, q, res, y0, y1, w2, part, slots_a, slots_b, slots_c,
    send_sems, recv_sems, load_sems, store_sems,
):
    slab, sub = lax.axis_index("slab"), lax.axis_index("sub")
    slabs = lax.axis_size("slab")
    other = 1 - sub
    x, y, z = lax.rem(slab, NX_T), lax.rem(lax.div(slab, NX_T), NY_T), lax.div(slab, NX_T * NY_T)
    has_left, has_right = slab > 0, slab < slabs - 1
    left, right = jnp.maximum(slab - 1, 0), jnp.minimum(slab + 1, slabs - 1)
    own_rows = pl.ds(pl.multiple_of(8 * sub, 8), 16)
    out_tile = pl.ds(8, 8)
    in_tile = pl.ds(pl.multiple_of(16 * sub, 8), 8)
    hbm_tile = pl.ds(pl.multiple_of(8 * other, 8), 8)

    def peers(stage):
        if stage == 0:
            for k in range(1, 2 * NX_T):
                at = lax.rem(2 * x + sub + k, 2 * NX_T)
                yield (slab - x + lax.div(at, 2), lax.rem(at, 2))
        elif stage == 1:
            for k in range(1, NY_T):
                yield (slab + NX_T * (lax.rem(y + k, NY_T) - y), sub)
        else:
            for k in range(1, NZ_T):
                yield (slab + NX_T * NY_T * (lax.rem(z + k, NZ_T) - z), sub)

    loads = [
        pltpu.make_async_copy(start, vec.at[0, :, pl.ds(5, 6), own_rows], load_sems.at[0]),
        pltpu.make_async_copy(wind, coef.at[pl.ds(0, 3), pl.ds(3, 6), own_rows], load_sems.at[1]),
        pltpu.make_async_copy(reac, coef.at[3, pl.ds(3, 6), own_rows], load_sems.at[2]),
        pltpu.make_async_copy(mass, coef.at[4, pl.ds(3, 6), own_rows], load_sems.at[3]),
    ]
    for copy in loads:
        copy.start()

    barrier = pltpu.get_barrier_semaphore()
    count = 0
    for stage in range(3):
        for peer in peers(stage):
            pl.semaphore_signal(barrier, inc=1, device_id=peer, device_id_type=MESH_ID)
            count += 1

    @pl.when(has_left)
    def _():
        pl.semaphore_signal(barrier, inc=1, device_id=(left, sub), device_id_type=MESH_ID)

    @pl.when(has_right)
    def _():
        pl.semaphore_signal(barrier, inc=1, device_id=(right, sub), device_id_type=MESH_ID)

    def clear(planes, coef_planes):
        for k in range(3):
            for f in range(4):
                vec[k, f, planes] = jnp.zeros((5, ROWS, 256), jnp.float32)
        for f in range(5):
            coef[f, coef_planes] = jnp.zeros((3, ROWS, 256), jnp.float32)

    @pl.when(jnp.logical_not(has_left))
    def _():
        clear(pl.ds(0, 5), pl.ds(0, 3))

    @pl.when(jnp.logical_not(has_right))
    def _():
        clear(pl.ds(11, 5), pl.ds(9, 3))

    pl.semaphore_wait(
        barrier, count + has_left.astype(jnp.int32) + has_right.astype(jnp.int32)
    )

    used = [0]

    def remote(src, dst, device):
        at = used[0]
        used[0] += 1
        return pltpu.make_async_remote_copy(
            src_ref=src, dst_ref=dst, send_sem=send_sems.at[at], recv_sem=recv_sems.at[at],
            device_id=device, device_id_type=MESH_ID,
        )

    started = []

    def go(copy, condition=None):
        started.append((copy, condition))
        if condition is None:
            copy.start()
        else:
            pl.when(condition)(copy.start)

    def arrive(copy, condition=None):
        if condition is None:
            copy.wait_recv()
        else:
            pl.when(condition)(copy.wait_recv)

    class Halo:
        def __init__(self, src_low, src_high, src_tile, buffer, low, high, own):
            self.to_right = remote(src_high, buffer(low, own_rows), (right, sub))
            self.to_left = remote(src_low, buffer(high, own_rows), (left, sub))
            self.to_other = remote(src_tile, buffer(own, in_tile), (slab, other))
            self.low_on = remote(buffer(low, out_tile), buffer(low, in_tile), (slab, other))
            self.high_on = remote(buffer(high, out_tile), buffer(high, in_tile), (slab, other))

        def send(self):
            go(self.to_right, has_right)
            go(self.to_left, has_left)
            go(self.to_other)

        def forward(self):
            arrive(self.to_right, has_left)
            go(self.low_on, has_left)
            arrive(self.to_left, has_right)
            go(self.high_on, has_right)

        def finish(self):
            arrive(self.to_other)
            arrive(self.low_on, has_left)
            arrive(self.high_on, has_right)

    def vec_halo(k):
        def pressure(planes, rows):
            return vec.at[k, 3, planes, rows]

        def velocity(planes, rows):
            return vec.at[k, pl.ds(0, 3), planes, rows]

        if k == 0:
            p_src = (start.at[3, pl.ds(0, 5)], start.at[3, pl.ds(1, 5)], start.at[3, :, hbm_tile])
            u_src = tuple(
                start.at[pl.ds(0, 3), planes] for planes in (pl.ds(0, 2), pl.ds(4, 2))
            ) + (start.at[pl.ds(0, 3), :, hbm_tile],)
        else:
            p_src = (
                pressure(pl.ds(5, 5), own_rows), pressure(pl.ds(6, 5), own_rows),
                pressure(pl.ds(5, 6), out_tile),
            )
            u_src = (
                velocity(pl.ds(5, 2), own_rows), velocity(pl.ds(9, 2), own_rows),
                velocity(pl.ds(5, 6), out_tile),
            )
        p_halo = Halo(*p_src, pressure, pl.ds(0, 5), pl.ds(11, 5), pl.ds(5, 6))
        u_halo = Halo(*u_src, velocity, pl.ds(3, 2), pl.ds(11, 2), pl.ds(5, 6))
        return p_halo, u_halo

    def coef_halo(src, buffer):
        if len(src.shape) == 4:
            parts = (src.at[:, pl.ds(0, 3)], src.at[:, pl.ds(3, 3)], src.at[:, :, hbm_tile])
        else:
            parts = (src.at[pl.ds(0, 3)], src.at[pl.ds(3, 3)], src.at[:, hbm_tile])
        return Halo(*parts, buffer, pl.ds(0, 3), pl.ds(9, 3), pl.ds(3, 6))

    p_halo, u_halo = vec_halo(0)
    coef_halos = [
        coef_halo(wind, lambda planes, rows: coef.at[pl.ds(0, 3), planes, rows]),
        coef_halo(reac, lambda planes, rows: coef.at[3, planes, rows]),
        coef_halo(mass, lambda planes, rows: coef.at[4, planes, rows]),
    ]
    p_halo.send()
    for halo in coef_halos:
        halo.send()
    u_halo.send()

    last, first = lane_is(HALF - 1), lane_is(0)
    row = lax.broadcasted_iota(jnp.int32, (ROWS, HALF), 0)
    live = row != (ROWS - 1) * other

    def inside(plane):
        at = slab * 6 + plane - 5
        return jnp.logical_and(at >= 0, at < slabs * 6)

    def prepare(j, _):
        ok = jnp.logical_and(live, inside(j + 2))
        for d in range(3):
            half = [0.5 * h for h in get(coef, d, j)]
            put(work, [h - 1.0 for h in half], d, j)
            put(work, [-1.0 - h for h in half], d + 3, j)
        diagonal = [6.0 + h for h in get(coef, 3, j)]
        put(work, diagonal, 6, j)
        put(work, [jnp.where(ok, 1.0 / h, 0.0) for h in diagonal], 7, j)
        put(work, [jnp.where(ok, -1.0 / h, 0.0) for h in get(coef, 4, j)], 8, j)
        return 0

    def six(fxm, f, fxp):
        total = [a + b for a, b in zip(fxm, fxp)]
        for g in (up_y(f), down_y(f), up_z(f, last), down_z(f, first)):
            total = [a + b for a, b in zip(total, g)]
        return total

    def weights(j):
        return [get(work, i, j) for i in range(7)]

    def transport(fxm, f, fxp, w):
        total = [a * b for a, b in zip(w[6], f)]
        terms = ((0, fxp), (3, fxm), (1, up_y(f)), (4, down_y(f)), (2, up_z(f, last)), (5, down_z(f, first)))
        for i, g in terms:
            total = [t + a * b for t, a, b in zip(total, w[i], g)]
        return total

    def half_difference(a, b):
        return [0.5 * (m - n) for m, n in zip(a, b)]

    def gradient(fxm, f, fxp):
        return (
            half_difference(fxp, fxm),
            half_difference(up_y(f), down_y(f)),
            half_difference(up_z(f, last), down_z(f, first)),
        )

    def pressure_part(k):
        def masked(j):
            return [jnp.where(live, h, 0.0) for h in get(vec, k, 3, j)]

        def guess(j, _):
            scale = jnp.where(jnp.logical_and(live, inside(j)), 1.0 / 49.0, 0.0)
            f = masked(j)
            total = six(get(vec, k, 3, j - 1), f, get(vec, k, 3, j + 1))
            put(t1, [scale * (7.0 * a + b) for a, b in zip(f, total)], j)
            return 0

        lax.fori_loop(1, 15, guess, 0)

        def schur(j, _):
            value = transport(get(t1, j + 1), get(t1, j + 2), get(t1, j + 3), weights(j))
            put(q, [a * b for a, b in zip(value, get(work, 8, j))], k, j)
            return 0

        lax.fori_loop(0, 12, schur, 0)

    def velocity_part(k, target):
        def first_guess(j, _):
            slope = gradient(get(q, k, j), get(q, k, j + 1), get(q, k, j + 2))
            inverse = get(work, 7, j + 1)
            for d in range(3):
                r = [a - b for a, b in zip(get(vec, k, d, j + 3), slope[d])]
                put(res, r, d, j)
                put(y0, [a * b for a, b in zip(r, inverse)], d, j)
            return 0

        lax.fori_loop(0, 10, first_guess, 0)

        def second_guess(j, _):
            w = weights(j + 2)
            inverse = get(work, 7, j + 2)
            for d in range(3):
                f = get(y0, d, j + 1)
                value = transport(get(y0, d, j), f, get(y0, d, j + 2), w)
                r = get(res, d, j + 1)
                put(y1, [a + (b - c) * i for a, b, c, i in zip(f, r, value, inverse)], k, d, j)
            return 0

        lax.fori_loop(0, 8, second_guess, 0)

        def store(f, j, value):
            for i, h in enumerate(value):
                mine = jnp.where(sub == 0, h[0:16], h[8:24])
                target(f, j)[own_rows if k < 2 else slice(None), pl.ds(HALF * i, HALF)] = mine

        def image(j, _):
            w = weights(j + 3)
            pm, pc, pp = get(q, k, j + 2), get(q, k, j + 3), get(q, k, j + 4)
            slope = gradient(pm, pc, pp)
            flow = None
            for d in range(3):
                fm, f, fp = get(y1, k, d, j), get(y1, k, d, j + 1), get(y1, k, d, j + 2)
                value = transport(fm, f, fp, w)
                store(d, j, [a + b for a, b in zip(value, slope[d])])
                ends = ((fp, fm), (up_y(f), down_y(f)), (up_z(f, last), down_z(f, first)))[d]
                part_flow = [a - b for a, b in zip(*ends)]
                flow = part_flow if flow is None else [a + b for a, b in zip(flow, part_flow)]
            total = six(pm, pc, pp)
            store(3, j, [-0.5 * (a + (6.0 * b - c)) for a, b, c in zip(flow, pc, total)])
            return 0

        lax.fori_loop(0, 6, image, 0)

    lane8 = lax.broadcasted_iota(jnp.int32, (8, HALF), 1)

    def vectors(i, f, j):
        if i < 3:
            block = vec[i, f, 5 + j, own_rows, :]
        else:
            block = w2[f, j]
        return block

    def dots(new, olds):
        def step(i, accs):
            f, j = lax.div(i, 6), lax.rem(i, 6)
            b = vectors(new, f, j)
            out = []
            for acc, old in zip(accs, olds):
                prod = b * (b if old == new else vectors(old, f, j))
                out.append(acc + ((prod[0:8, 0:HALF] + prod[0:8, HALF:]) + (prod[8:16, 0:HALF] + prod[8:16, HALF:])))
            return tuple(out)

        zero = jnp.zeros((8, HALF), jnp.float32)
        return lax.fori_loop(0, 24, step, tuple(zero for _ in olds))

    def pack(total, sums, at):
        for i, s in enumerate(sums):
            total = jnp.where(lane8 == at + i, jnp.sum(s, axis=1, keepdims=True), total)
        return total

    for copy in loads:
        copy.wait()
    p_halo.forward()
    for halo in coef_halos:
        halo.forward()
    p_halo.finish()
    for halo in coef_halos:
        halo.finish()
    lax.fori_loop(0, 12, prepare, 0)
    pressure_part(0)
    u_halo.forward()
    u_halo.finish()
    velocity_part(0, lambda f, j: vec.at[1, f, 5 + j])

    stores = []

    def save(src, dst):
        copy = pltpu.make_async_copy(src, dst, store_sems.at[len(stores)])
        copy.start()
        stores.append(copy)

    gram = jnp.zeros((8, HALF), jnp.float32)
    at = 0
    for k, (w_out, z_out) in enumerate(((w0_out, z0_out), (w1_out, z1_out))):
        p_halo, u_halo = vec_halo(k + 1)
        p_halo.send()
        u_halo.send()
        save(vec.at[k + 1, :, pl.ds(5, 6), own_rows], w_out)
        save(y1.at[k, :, pl.ds(1, 6), own_rows], z_out.at[pl.ds(0, 3)])
        save(q.at[k, pl.ds(3, 6), own_rows], z_out.at[3])
        if k == 0:
            gram = pack(gram, dots(0, (0,)), 0)
            at = 1
        olds = tuple(range(k + 2))
        gram = pack(gram, dots(k + 1, olds), at)
        at += len(olds)
        p_halo.forward()
        p_halo.finish()
        pressure_part(k + 1)
        u_halo.forward()
        u_halo.finish()
        velocity_part(k + 1, (lambda f, j: vec.at[2, f, 5 + j]) if k == 0 else (lambda f, j: w2.at[f, j]))
    gram = pack(gram, dots(3, (0, 1, 2, 3)), at)
    save(y1.at[2, :, pl.ds(1, 6), own_rows], z2_out.at[pl.ds(0, 3)])
    save(q.at[2, pl.ds(3, 6), own_rows], z2_out.at[3])
    save(w2, w2_out)

    places = (2 * x + sub, y, z)
    for stage, slots in enumerate((slots_a, slots_b, slots_c)):
        place = places[stage]
        part[stage] = gram
        slots[place] = gram
        copies = [remote(part.at[stage], slots.at[place], peer) for peer in peers(stage)]
        for copy in copies:
            go(copy)
        for copy in copies:
            arrive(copy)
        gram = slots[0]
        for i in range(1, slots.shape[0]):
            gram = gram + slots[i]
    gram_out[...] = gram

    for copy, condition in started:
        if condition is None:
            copy.wait_send()
        else:
            pl.when(condition)(copy.wait_send)
    for copy in stores:
        copy.wait()


def combine_kernel(
    start, w0, w1, w2, z0, z1, z2, gram, basis, search, hess, y_in, z_in, b_out, s_out, in_sems, out_sems
):
    reads = []
    for f in range(4):
        group = []
        for i, src in enumerate((start, w0, w1, w2)):
            group.append(pltpu.make_async_copy(src.at[f], y_in.at[i, f], in_sems.at[f, i]))
        for i, src in enumerate((z0, z1, z2)):
            group.append(pltpu.make_async_copy(src.at[f], z_in.at[i, f], in_sems.at[f, 4 + i]))
        for copy in group:
            copy.start()
        reads.append(group)

    total = jnp.sum(gram[...], axis=0, keepdims=True)
    lane = lax.broadcasted_iota(jnp.int32, (1, HALF), 1)

    def entry(i):
        return jnp.broadcast_to(jnp.sum(jnp.where(lane == i, total, 0.0), axis=1, keepdims=True), (1, HALF))

    low = {}
    inverse = {}
    for i in range(4):
        for j in range(i + 1):
            value = entry(i * (i + 1) // 2 + j)
            for m in range(j):
                value = value - low[i, m] * low[j, m]
            if i == j:
                low[i, i] = jnp.sqrt(value)
                inverse[i] = 1.0 / low[i, i]
            else:
                low[i, j] = value * inverse[j]
    h = {}
    for j in range(3):
        for i in range(j + 2):
            value = low[j + 1, i]
            for m in range(j):
                if i <= m + 1:
                    value = value - low[j, m] * h[i, m]
            h[i, j] = value * inverse[j]
    at_row = lax.broadcasted_iota(jnp.int32, (4, HALF), 0)
    at_col = lax.broadcasted_iota(jnp.int32, (4, HALF), 1)
    table = jnp.zeros((4, HALF), jnp.float32)
    for (i, j), value in h.items():
        table = jnp.where(jnp.logical_and(at_row == i, at_col == j), value, table)
    hess[...] = table[:, 0:3]

    def wide(v):
        return jnp.concatenate([v, v], axis=1)

    scale = {key: wide(v) for key, v in low.items()}
    inv = {key: wide(v) for key, v in inverse.items()}

    writes = []
    for f in range(4):
        for copy in reads[f]:
            copy.wait()

        def body(j, _):
            for src, dst, n in ((y_in, b_out, 4), (z_in, s_out, 3)):
                done = []
                for i in range(n):
                    value = src[i, f, j]
                    for m in range(i):
                        value = value - scale[i, m] * done[m]
                    value = value * inv[i]
                    dst[i, f, j] = value
                    done.append(value)
            return 0

        lax.fori_loop(0, 6, body, 0)
        for i, (src, dst) in enumerate(((b_out, basis), (s_out, search))):
            copy = pltpu.make_async_copy(src.at[:, f], dst.at[:, f], out_sems.at[f, i])
            copy.start()
            writes.append(copy)
    for copy in writes:
        copy.wait()


def per_device(start, wind, reaction, mass):
    f32 = jnp.float32
    block = jax.ShapeDtypeStruct((4, 6, 16, 256), f32)
    any_spec = pl.BlockSpec(memory_space=pl.ANY)
    vmem_spec = pl.BlockSpec(memory_space=pltpu.VMEM)
    n_remote = 10 * 3 + 15 + 7 + 3 + 7
    outs = pl.pallas_call(
        krylov_kernel,
        out_shape=(block,) * 6 + (jax.ShapeDtypeStruct((8, HALF), f32),),
        in_specs=[any_spec] * 4,
        out_specs=(any_spec,) * 6 + (vmem_spec,),
        scratch_shapes=[
            pltpu.VMEM((3, 4, 16, ROWS, 256), f32),
            pltpu.VMEM((5, 12, ROWS, 256), f32),
            pltpu.VMEM((9, 12, ROWS, 256), f32),
            pltpu.VMEM((16, ROWS, 256), f32),
            pltpu.VMEM((3, 12, ROWS, 256), f32),
            pltpu.VMEM((3, 10, ROWS, 256), f32),
            pltpu.VMEM((3, 10, ROWS, 256), f32),
            pltpu.VMEM((3, 3, 8, ROWS, 256), f32),
            pltpu.VMEM((4, 6, 16, 256), f32),
            pltpu.VMEM((3, 8, HALF), f32),
            pltpu.VMEM((8, 8, HALF), f32),
            pltpu.VMEM((4, 8, HALF), f32),
            pltpu.VMEM((8, 8, HALF), f32),
            pltpu.SemaphoreType.DMA((n_remote,)),
            pltpu.SemaphoreType.DMA((n_remote,)),
            pltpu.SemaphoreType.DMA((4,)),
            pltpu.SemaphoreType.DMA((9,)),
        ],
        compiler_params=pltpu.CompilerParams(
            collective_id=0, has_side_effects=True, vmem_limit_bytes=40 * 2**20
        ),
        name="krylov",
    )(start, wind, reaction, mass)
    return tuple(pl.pallas_call(
        combine_kernel,
        out_shape=(
            jax.ShapeDtypeStruct((4, 4, 6, 16, 256), f32),
            jax.ShapeDtypeStruct((3, 4, 6, 16, 256), f32),
            jax.ShapeDtypeStruct((4, 3), f32),
        ),
        in_specs=[any_spec] * 7 + [vmem_spec],
        out_specs=(any_spec, any_spec, vmem_spec),
        scratch_shapes=[
            pltpu.VMEM((4, 4, 6, 16, 256), f32),
            pltpu.VMEM((3, 4, 6, 16, 256), f32),
            pltpu.VMEM((4, 4, 6, 16, 256), f32),
            pltpu.VMEM((3, 4, 6, 16, 256), f32),
            pltpu.SemaphoreType.DMA((4, 7)),
            pltpu.SemaphoreType.DMA((4, 2)),
        ],
        name="combine",
    )(start, *outs))


def solution(mesh):
    in_specs = (
        P(None, "slab", "sub", None),
        P(None, "slab", "sub", None),
        P("slab", "sub", None),
        P("slab", "sub", None),
    )
    out_specs = (P(None, None, "slab", "sub", None), P(None, None, "slab", "sub", None), P())
    return jax.shard_map(per_device, mesh=mesh, in_specs=in_specs, out_specs=out_specs, check_vma=False)
```

```python
import functools

import jax
import jax.numpy as jnp
from jax import lax
from jax.experimental import pallas as pl
from jax.experimental.pallas import tpu as pltpu
from jax.sharding import PartitionSpec as P

MESH_ID = pl.DeviceIdType.MESH
NX_T, NY_T, NZ_T = 4, 4, 8
ROWS = 24
HALF = 128


def lane_is(lane):
    return lax.broadcasted_iota(jnp.int32, (ROWS, HALF), 1) == lane


def get(ref, *lead):
    return ref[(*lead, slice(None), pl.ds(0, HALF))], ref[(*lead, slice(None), pl.ds(HALF, HALF))]


def put(ref, value, *lead):
    ref[(*lead, slice(None), pl.ds(0, HALF))] = value[0]
    ref[(*lead, slice(None), pl.ds(HALF, HALF))] = value[1]


def up_z(f, last):
    low, high = pltpu.roll(f[0], HALF - 1, 1), pltpu.roll(f[1], HALF - 1, 1)
    return jnp.where(last, high, low), jnp.where(last, 0.0, high)


def down_z(f, first):
    low, high = pltpu.roll(f[0], 1, 1), pltpu.roll(f[1], 1, 1)
    return jnp.where(first, 0.0, low), jnp.where(first, low, high)


def up_y(f):
    return tuple(pltpu.roll(h, ROWS - 1, 0) for h in f)


def down_y(f):
    return tuple(pltpu.roll(h, 1, 0) for h in f)


def krylov_kernel(
    start, wind, reac, mass,
    vec, w2, y1, q, gram_out,
    coef, work, t1, res, y0, part, slots_a, slots_b, slots_c,
    send_sems, recv_sems, load_sems,
):
    slab, sub = lax.axis_index("slab"), lax.axis_index("sub")
    slabs = lax.axis_size("slab")
    other = 1 - sub
    x, y, z = lax.rem(slab, NX_T), lax.rem(lax.div(slab, NX_T), NY_T), lax.div(slab, NX_T * NY_T)
    has_left, has_right = slab > 0, slab < slabs - 1
    left, right = jnp.maximum(slab - 1, 0), jnp.minimum(slab + 1, slabs - 1)
    own_rows = pl.ds(pl.multiple_of(8 * sub, 8), 16)
    out_tile = pl.ds(8, 8)
    in_tile = pl.ds(pl.multiple_of(16 * sub, 8), 8)
    hbm_tile = pl.ds(pl.multiple_of(8 * other, 8), 8)

    def peers(stage):
        if stage == 0:
            for k in range(1, 2 * NX_T):
                at = lax.rem(2 * x + sub + k, 2 * NX_T)
                yield (slab - x + lax.div(at, 2), lax.rem(at, 2))
        elif stage == 1:
            for k in range(1, NY_T):
                yield (slab + NX_T * (lax.rem(y + k, NY_T) - y), sub)
        else:
            for k in range(1, NZ_T):
                yield (slab + NX_T * NY_T * (lax.rem(z + k, NZ_T) - z), sub)

    loads = [
        pltpu.make_async_copy(start, vec.at[0, :, pl.ds(5, 6), own_rows], load_sems.at[0]),
        pltpu.make_async_copy(wind, coef.at[pl.ds(0, 3), pl.ds(3, 6), own_rows], load_sems.at[1]),
        pltpu.make_async_copy(reac, coef.at[3, pl.ds(3, 6), own_rows], load_sems.at[2]),
        pltpu.make_async_copy(mass, coef.at[4, pl.ds(3, 6), own_rows], load_sems.at[3]),
    ]
    for copy in loads:
        copy.start()

    barrier = pltpu.get_barrier_semaphore()
    count = 0
    for stage in range(3):
        for peer in peers(stage):
            pl.semaphore_signal(barrier, inc=1, device_id=peer, device_id_type=MESH_ID)
            count += 1

    @pl.when(has_left)
    def _():
        pl.semaphore_signal(barrier, inc=1, device_id=(left, sub), device_id_type=MESH_ID)

    @pl.when(has_right)
    def _():
        pl.semaphore_signal(barrier, inc=1, device_id=(right, sub), device_id_type=MESH_ID)

    def clear(planes, coef_planes):
        for k in range(3):
            for f in range(4):
                vec[k, f, planes] = jnp.zeros((5, ROWS, 256), jnp.float32)
        for f in range(5):
            coef[f, coef_planes] = jnp.zeros((3, ROWS, 256), jnp.float32)

    @pl.when(jnp.logical_not(has_left))
    def _():
        clear(pl.ds(0, 5), pl.ds(0, 3))

    @pl.when(jnp.logical_not(has_right))
    def _():
        clear(pl.ds(11, 5), pl.ds(9, 3))

    pl.semaphore_wait(
        barrier, count + has_left.astype(jnp.int32) + has_right.astype(jnp.int32)
    )

    used = [0]

    def remote(src, dst, device):
        at = used[0]
        used[0] += 1
        return pltpu.make_async_remote_copy(
            src_ref=src, dst_ref=dst, send_sem=send_sems.at[at], recv_sem=recv_sems.at[at],
            device_id=device, device_id_type=MESH_ID,
        )

    started = []

    def go(copy, condition=None):
        started.append((copy, condition))
        if condition is None:
            copy.start()
        else:
            pl.when(condition)(copy.start)

    def arrive(copy, condition=None):
        if condition is None:
            copy.wait_recv()
        else:
            pl.when(condition)(copy.wait_recv)

    class Halo:
        def __init__(self, src_low, src_high, src_tile, buffer, low, high, own):
            self.to_right = remote(src_high, buffer(low, own_rows), (right, sub))
            self.to_left = remote(src_low, buffer(high, own_rows), (left, sub))
            self.to_other = remote(src_tile, buffer(own, in_tile), (slab, other))
            self.low_on = remote(buffer(low, out_tile), buffer(low, in_tile), (slab, other))
            self.high_on = remote(buffer(high, out_tile), buffer(high, in_tile), (slab, other))

        def send(self):
            go(self.to_right, has_right)
            go(self.to_left, has_left)
            go(self.to_other)

        def forward(self):
            arrive(self.to_right, has_left)
            go(self.low_on, has_left)
            arrive(self.to_left, has_right)
            go(self.high_on, has_right)

        def finish(self):
            arrive(self.to_other)
            arrive(self.low_on, has_left)
            arrive(self.high_on, has_right)

    def vec_halo(k):
        def pressure(planes, rows):
            return vec.at[k, 3, planes, rows]

        def velocity(planes, rows):
            return vec.at[k, pl.ds(0, 3), planes, rows]

        if k == 0:
            p_src = (start.at[3, pl.ds(0, 5)], start.at[3, pl.ds(1, 5)], start.at[3, :, hbm_tile])
            u_src = tuple(
                start.at[pl.ds(0, 3), planes] for planes in (pl.ds(0, 2), pl.ds(4, 2))
            ) + (start.at[pl.ds(0, 3), :, hbm_tile],)
        else:
            p_src = (
                pressure(pl.ds(5, 5), own_rows), pressure(pl.ds(6, 5), own_rows),
                pressure(pl.ds(5, 6), out_tile),
            )
            u_src = (
                velocity(pl.ds(5, 2), own_rows), velocity(pl.ds(9, 2), own_rows),
                velocity(pl.ds(5, 6), out_tile),
            )
        p_halo = Halo(*p_src, pressure, pl.ds(0, 5), pl.ds(11, 5), pl.ds(5, 6))
        u_halo = Halo(*u_src, velocity, pl.ds(3, 2), pl.ds(11, 2), pl.ds(5, 6))
        return p_halo, u_halo

    def coef_halo(src, buffer):
        if len(src.shape) == 4:
            parts = (src.at[:, pl.ds(0, 3)], src.at[:, pl.ds(3, 3)], src.at[:, :, hbm_tile])
        else:
            parts = (src.at[pl.ds(0, 3)], src.at[pl.ds(3, 3)], src.at[:, hbm_tile])
        return Halo(*parts, buffer, pl.ds(0, 3), pl.ds(9, 3), pl.ds(3, 6))

    p_halo, u_halo = vec_halo(0)
    coef_halos = [
        coef_halo(wind, lambda planes, rows: coef.at[pl.ds(0, 3), planes, rows]),
        coef_halo(reac, lambda planes, rows: coef.at[3, planes, rows]),
        coef_halo(mass, lambda planes, rows: coef.at[4, planes, rows]),
    ]
    p_halo.send()
    for halo in coef_halos:
        halo.send()
    u_halo.send()

    last, first = lane_is(HALF - 1), lane_is(0)
    row = lax.broadcasted_iota(jnp.int32, (ROWS, HALF), 0)
    live = row != (ROWS - 1) * other

    def inside(plane):
        at = slab * 6 + plane - 5
        return jnp.logical_and(at >= 0, at < slabs * 6)

    def prepare(j, _):
        ok = jnp.logical_and(live, inside(j + 2))
        for d in range(3):
            half = [0.5 * h for h in get(coef, d, j)]
            put(work, [h - 1.0 for h in half], d, j)
            put(work, [-1.0 - h for h in half], d + 3, j)
        diagonal = [6.0 + h for h in get(coef, 3, j)]
        put(work, diagonal, 6, j)
        put(work, [jnp.where(ok, 1.0 / h, 0.0) for h in diagonal], 7, j)
        put(work, [jnp.where(ok, -1.0 / h, 0.0) for h in get(coef, 4, j)], 8, j)
        return 0

    def six(fxm, f, fxp):
        total = [a + b for a, b in zip(fxm, fxp)]
        for g in (up_y(f), down_y(f), up_z(f, last), down_z(f, first)):
            total = [a + b for a, b in zip(total, g)]
        return total

    def weights(j):
        return [get(work, i, j) for i in range(7)]

    def transport(fxm, f, fxp, w):
        total = [a * b for a, b in zip(w[6], f)]
        terms = ((0, fxp), (3, fxm), (1, up_y(f)), (4, down_y(f)), (2, up_z(f, last)), (5, down_z(f, first)))
        for i, g in terms:
            total = [t + a * b for t, a, b in zip(total, w[i], g)]
        return total

    def half_difference(a, b):
        return [0.5 * (m - n) for m, n in zip(a, b)]

    def gradient(fxm, f, fxp):
        return (
            half_difference(fxp, fxm),
            half_difference(up_y(f), down_y(f)),
            half_difference(up_z(f, last), down_z(f, first)),
        )

    def pressure_part(k):
        def masked(j):
            return [jnp.where(live, h, 0.0) for h in get(vec, k, 3, j)]

        def guess(j, _):
            scale = jnp.where(jnp.logical_and(live, inside(j)), 1.0 / 49.0, 0.0)
            f = masked(j)
            total = six(get(vec, k, 3, j - 1), f, get(vec, k, 3, j + 1))
            put(t1, [scale * (7.0 * a + b) for a, b in zip(f, total)], j)
            return 0

        lax.fori_loop(1, 15, guess, 0)

        def schur(j, _):
            value = transport(get(t1, j + 1), get(t1, j + 2), get(t1, j + 3), weights(j))
            put(q, [a * b for a, b in zip(value, get(work, 8, j))], k, j)
            return 0

        lax.fori_loop(0, 12, schur, 0)

    def velocity_part(k, target):
        def first_guess(j, _):
            slope = gradient(get(q, k, j), get(q, k, j + 1), get(q, k, j + 2))
            inverse = get(work, 7, j + 1)
            for d in range(3):
                r = [a - b for a, b in zip(get(vec, k, d, j + 3), slope[d])]
                put(res, r, d, j)
                put(y0, [a * b for a, b in zip(r, inverse)], d, j)
            return 0

        lax.fori_loop(0, 10, first_guess, 0)

        def second_guess(j, _):
            w = weights(j + 2)
            inverse = get(work, 7, j + 2)
            for d in range(3):
                f = get(y0, d, j + 1)
                value = transport(get(y0, d, j), f, get(y0, d, j + 2), w)
                r = get(res, d, j + 1)
                put(y1, [a + (b - c) * i for a, b, c, i in zip(f, r, value, inverse)], k, d, j)
            return 0

        lax.fori_loop(0, 8, second_guess, 0)

        def store(f, j, value):
            for i, h in enumerate(value):
                mine = jnp.where(sub == 0, h[0:16], h[8:24])
                target(f, j)[own_rows if k < 2 else slice(None), pl.ds(HALF * i, HALF)] = mine

        def image(j, _):
            w = weights(j + 3)
            pm, pc, pp = get(q, k, j + 2), get(q, k, j + 3), get(q, k, j + 4)
            slope = gradient(pm, pc, pp)
            flow = None
            for d in range(3):
                fm, f, fp = get(y1, k, d, j), get(y1, k, d, j + 1), get(y1, k, d, j + 2)
                value = transport(fm, f, fp, w)
                store(d, j, [a + b for a, b in zip(value, slope[d])])
                ends = ((fp, fm), (up_y(f), down_y(f)), (up_z(f, last), down_z(f, first)))[d]
                part_flow = [a - b for a, b in zip(*ends)]
                flow = part_flow if flow is None else [a + b for a, b in zip(flow, part_flow)]
            total = six(pm, pc, pp)
            store(3, j, [-0.5 * (a + (6.0 * b - c)) for a, b, c in zip(flow, pc, total)])
            return 0

        lax.fori_loop(0, 6, image, 0)

    lane8 = lax.broadcasted_iota(jnp.int32, (8, HALF), 1)

    def vectors(i, f, j):
        if i < 3:
            block = vec[i, f, 5 + j, own_rows, :]
        else:
            block = w2[f, j]
        return block

    def dots(new, olds):
        def step(i, accs):
            f, j = lax.div(i, 6), lax.rem(i, 6)
            b = vectors(new, f, j)
            out = []
            for acc, old in zip(accs, olds):
                prod = b * (b if old == new else vectors(old, f, j))
                out.append(acc + ((prod[0:8, 0:HALF] + prod[0:8, HALF:]) + (prod[8:16, 0:HALF] + prod[8:16, HALF:])))
            return tuple(out)

        zero = jnp.zeros((8, HALF), jnp.float32)
        return lax.fori_loop(0, 24, step, tuple(zero for _ in olds))

    def pack(total, sums, at):
        for i, s in enumerate(sums):
            total = jnp.where(lane8 == at + i, jnp.sum(s, axis=1, keepdims=True), total)
        return total

    for copy in loads:
        copy.wait()
    p_halo.forward()
    for halo in coef_halos:
        halo.forward()
    p_halo.finish()
    for halo in coef_halos:
        halo.finish()
    lax.fori_loop(0, 12, prepare, 0)
    pressure_part(0)
    u_halo.forward()
    u_halo.finish()
    velocity_part(0, lambda f, j: vec.at[1, f, 5 + j])

    gram = jnp.zeros((8, HALF), jnp.float32)
    at = 0
    for k in range(2):
        p_halo, u_halo = vec_halo(k + 1)
        p_halo.send()
        u_halo.send()
        if k == 0:
            gram = pack(gram, dots(0, (0,)), 0)
            at = 1
        olds = tuple(range(k + 2))
        gram = pack(gram, dots(k + 1, olds), at)
        at += len(olds)
        p_halo.forward()
        p_halo.finish()
        pressure_part(k + 1)
        u_halo.forward()
        u_halo.finish()
        velocity_part(k + 1, (lambda f, j: vec.at[2, f, 5 + j]) if k == 0 else (lambda f, j: w2.at[f, j]))
    gram = pack(gram, dots(3, (0, 1, 2, 3)), at)

    places = (2 * x + sub, y, z)
    for stage, slots in enumerate((slots_a, slots_b, slots_c)):
        place = places[stage]
        part[stage] = gram
        slots[place] = gram
        copies = [remote(part.at[stage], slots.at[place], peer) for peer in peers(stage)]
        for copy in copies:
            go(copy)
        for copy in copies:
            arrive(copy)
        gram = slots[0]
        for i in range(1, slots.shape[0]):
            gram = gram + slots[i]
    gram_out[...] = gram

    for copy, condition in started:
        if condition is None:
            copy.wait_send()
        else:
            pl.when(condition)(copy.wait_send)


def combine_kernel(vec, w2, y1, q, gram, basis, search, hess, b_out, s_out, out_sems):
    own_rows = pl.ds(pl.multiple_of(8 * lax.axis_index("sub"), 8), 16)

    total = jnp.sum(gram[...], axis=0, keepdims=True)
    lane = lax.broadcasted_iota(jnp.int32, (1, HALF), 1)

    def entry(i):
        return jnp.broadcast_to(jnp.sum(jnp.where(lane == i, total, 0.0), axis=1, keepdims=True), (1, HALF))

    low = {}
    inverse = {}
    for i in range(4):
        for j in range(i + 1):
            value = entry(i * (i + 1) // 2 + j)
            for m in range(j):
                value = value - low[i, m] * low[j, m]
            if i == j:
                low[i, i] = jnp.sqrt(value)
                inverse[i] = 1.0 / low[i, i]
            else:
                low[i, j] = value * inverse[j]
    h = {}
    for j in range(3):
        for i in range(j + 2):
            value = low[j + 1, i]
            for m in range(j):
                if i <= m + 1:
                    value = value - low[j, m] * h[i, m]
            h[i, j] = value * inverse[j]
    at_row = lax.broadcasted_iota(jnp.int32, (4, HALF), 0)
    at_col = lax.broadcasted_iota(jnp.int32, (4, HALF), 1)
    table = jnp.zeros((4, HALF), jnp.float32)
    for (i, j), value in h.items():
        table = jnp.where(jnp.logical_and(at_row == i, at_col == j), value, table)
    hess[...] = table[:, 0:3]

    def wide(v):
        return jnp.concatenate([v, v], axis=1)

    scale = {key: wide(v) for key, v in low.items()}
    inv = {key: wide(v) for key, v in inverse.items()}

    writes = []
    for f in range(4):

        def body(j, _):
            raw = [vec[i, f, 5 + j, own_rows, :] for i in range(3)] + [w2[f, j]]
            found = [y1[i, f, 1 + j, own_rows, :] if f < 3 else q[i, 3 + j, own_rows, :] for i in range(3)]
            for values, dst in ((raw, b_out), (found, s_out)):
                done = []
                for i, value in enumerate(values):
                    for m in range(i):
                        value = value - scale[i, m] * done[m]
                    value = value * inv[i]
                    dst[i, f, j] = value
                    done.append(value)
            return 0

        lax.fori_loop(0, 6, body, 0)
        for i, (src, dst) in enumerate(((b_out, basis), (s_out, search))):
            copy = pltpu.make_async_copy(src.at[:, f], dst.at[:, f], out_sems.at[f, i])
            copy.start()
            writes.append(copy)
    for copy in writes:
        copy.wait()


def per_device(start, wind, reaction, mass):
    f32 = jnp.float32
    hbm_spec = pl.BlockSpec(memory_space=pltpu.HBM)
    vmem_spec = pl.BlockSpec(memory_space=pltpu.VMEM)
    n_remote = 10 * 3 + 15 + 7 + 3 + 7
    kept = (
        jax.ShapeDtypeStruct((3, 4, 16, ROWS, 256), f32),
        jax.ShapeDtypeStruct((4, 6, 16, 256), f32),
        jax.ShapeDtypeStruct((3, 3, 8, ROWS, 256), f32),
        jax.ShapeDtypeStruct((3, 12, ROWS, 256), f32),
        jax.ShapeDtypeStruct((8, HALF), f32),
    )
    arrays = [pltpu.with_memory_space_constraint(a, pltpu.HBM) for a in (start, wind, reaction, mass)]
    outs = pl.pallas_call(
        krylov_kernel,
        out_shape=kept,
        in_specs=[hbm_spec] * 4,
        out_specs=(vmem_spec,) * 5,
        scratch_shapes=[
            pltpu.VMEM((5, 12, ROWS, 256), f32),
            pltpu.VMEM((9, 12, ROWS, 256), f32),
            pltpu.VMEM((16, ROWS, 256), f32),
            pltpu.VMEM((3, 10, ROWS, 256), f32),
            pltpu.VMEM((3, 10, ROWS, 256), f32),
            pltpu.VMEM((3, 8, HALF), f32),
            pltpu.VMEM((8, 8, HALF), f32),
            pltpu.VMEM((4, 8, HALF), f32),
            pltpu.VMEM((8, 8, HALF), f32),
            pltpu.SemaphoreType.DMA((n_remote,)),
            pltpu.SemaphoreType.DMA((n_remote,)),
            pltpu.SemaphoreType.DMA((4,)),
        ],
        compiler_params=pltpu.CompilerParams(
            collective_id=0, has_side_effects=True, vmem_limit_bytes=24 * 2**20
        ),
        name="krylov",
    )(*arrays)
    return tuple(pl.pallas_call(
        combine_kernel,
        out_shape=(
            jax.ShapeDtypeStruct((4, 4, 6, 16, 256), f32),
            jax.ShapeDtypeStruct((3, 4, 6, 16, 256), f32),
            jax.ShapeDtypeStruct((4, 3), f32),
        ),
        in_specs=[vmem_spec] * 5,
        out_specs=(hbm_spec, hbm_spec, vmem_spec),
        scratch_shapes=[
            pltpu.VMEM((4, 4, 6, 16, 256), f32),
            pltpu.VMEM((3, 4, 6, 16, 256), f32),
            pltpu.SemaphoreType.DMA((4, 2)),
        ],
        compiler_params=pltpu.CompilerParams(vmem_limit_bytes=24 * 2**20),
        name="combine",
    )(*outs))


def solution(mesh):
    in_specs = (
        P(None, "slab", "sub", None),
        P(None, "slab", "sub", None),
        P("slab", "sub", None),
        P("slab", "sub", None),
    )
    out_specs = (P(None, None, "slab", "sub", None), P(None, None, "slab", "sub", None), P())
    return jax.shard_map(per_device, mesh=mesh, in_specs=in_specs, out_specs=out_specs, check_vma=False)
```

```python
import functools

import jax
import jax.numpy as jnp
from jax import lax
from jax.experimental import pallas as pl
from jax.experimental.pallas import tpu as pltpu
from jax.sharding import PartitionSpec as P

MESH_ID = pl.DeviceIdType.MESH
NX_T, NY_T, NZ_T = 4, 4, 8
ROWS = 24
HALF = 128


def lane_is(lane):
    return lax.broadcasted_iota(jnp.int32, (ROWS, HALF), 1) == lane


def get(ref, *lead):
    return ref[(*lead, slice(None), pl.ds(0, HALF))], ref[(*lead, slice(None), pl.ds(HALF, HALF))]


def put(ref, value, *lead):
    ref[(*lead, slice(None), pl.ds(0, HALF))] = value[0]
    ref[(*lead, slice(None), pl.ds(HALF, HALF))] = value[1]


def up_z(f, last):
    low, high = pltpu.roll(f[0], HALF - 1, 1), pltpu.roll(f[1], HALF - 1, 1)
    return jnp.where(last, high, low), jnp.where(last, 0.0, high)


def down_z(f, first):
    low, high = pltpu.roll(f[0], 1, 1), pltpu.roll(f[1], 1, 1)
    return jnp.where(first, 0.0, low), jnp.where(first, low, high)


def up_y(f):
    return tuple(pltpu.roll(h, ROWS - 1, 0) for h in f)


def down_y(f):
    return tuple(pltpu.roll(h, 1, 0) for h in f)


def krylov_kernel(
    start, wind, reac, mass,
    vec, w2, y1, q, gram_out,
    coef, work, t1, res, y0, part, slots_a, slots_b,
    send_sems, recv_sems, load_sems,
):
    slab, sub = lax.axis_index("slab"), lax.axis_index("sub")
    slabs = lax.axis_size("slab")
    other = 1 - sub
    z = lax.div(slab, NX_T * NY_T)
    has_left, has_right = slab > 0, slab < slabs - 1
    left, right = jnp.maximum(slab - 1, 0), jnp.minimum(slab + 1, slabs - 1)
    own_rows = pl.ds(pl.multiple_of(8 * sub, 8), 16)
    out_tile = pl.ds(8, 8)
    in_tile = pl.ds(pl.multiple_of(16 * sub, 8), 8)

    plane = 2 * NX_T * NY_T
    in_plane = lax.rem(2 * slab + sub, plane)

    def peers(stage):
        if stage == 0:
            for k in range(1, plane):
                at = lax.rem(in_plane + k, plane)
                yield (z * (NX_T * NY_T) + lax.div(at, 2), lax.rem(at, 2))
        else:
            for k in range(1, NZ_T):
                yield (slab + NX_T * NY_T * (lax.rem(z + k, NZ_T) - z), sub)

    loads = [
        pltpu.make_async_copy(start, vec.at[0, :, pl.ds(5, 6), own_rows], load_sems.at[0]),
        pltpu.make_async_copy(wind, coef.at[pl.ds(0, 3), pl.ds(3, 6), own_rows], load_sems.at[1]),
        pltpu.make_async_copy(reac, coef.at[3, pl.ds(3, 6), own_rows], load_sems.at[2]),
        pltpu.make_async_copy(mass, coef.at[4, pl.ds(3, 6), own_rows], load_sems.at[3]),
    ]
    for copy in loads:
        copy.start()

    barrier = pltpu.get_barrier_semaphore()
    count = 0
    for stage in range(2):
        for peer in peers(stage):
            pl.semaphore_signal(barrier, inc=1, device_id=peer, device_id_type=MESH_ID)
            count += 1

    @pl.when(has_left)
    def _():
        pl.semaphore_signal(barrier, inc=1, device_id=(left, sub), device_id_type=MESH_ID)

    @pl.when(has_right)
    def _():
        pl.semaphore_signal(barrier, inc=1, device_id=(right, sub), device_id_type=MESH_ID)

    def clear(planes, coef_planes):
        for k in range(3):
            for f in range(4):
                vec[k, f, planes] = jnp.zeros((5, ROWS, 256), jnp.float32)
        for f in range(5):
            coef[f, coef_planes] = jnp.zeros((3, ROWS, 256), jnp.float32)

    @pl.when(jnp.logical_not(has_left))
    def _():
        clear(pl.ds(0, 5), pl.ds(0, 3))

    @pl.when(jnp.logical_not(has_right))
    def _():
        clear(pl.ds(11, 5), pl.ds(9, 3))

    pl.semaphore_wait(
        barrier, count + has_left.astype(jnp.int32) + has_right.astype(jnp.int32)
    )

    used = [0]

    def remote(src, dst, device):
        at = used[0]
        used[0] += 1
        return pltpu.make_async_remote_copy(
            src_ref=src, dst_ref=dst, send_sem=send_sems.at[at], recv_sem=recv_sems.at[at],
            device_id=device, device_id_type=MESH_ID,
        )

    started = []

    def go(copy, condition=None):
        started.append((copy, condition))
        if condition is None:
            copy.start()
        else:
            pl.when(condition)(copy.start)

    def arrive(copy, condition=None):
        if condition is None:
            copy.wait_recv()
        else:
            pl.when(condition)(copy.wait_recv)

    class Halo:
        def __init__(self, src_low, src_high, src_tile, buffer, low, high, own):
            self.to_right = remote(src_high, buffer(low, own_rows), (right, sub))
            self.to_left = remote(src_low, buffer(high, own_rows), (left, sub))
            self.to_other = remote(src_tile, buffer(own, in_tile), (slab, other))
            self.low_on = remote(buffer(low, out_tile), buffer(low, in_tile), (slab, other))
            self.high_on = remote(buffer(high, out_tile), buffer(high, in_tile), (slab, other))

        def send(self):
            go(self.to_right, has_right)
            go(self.to_left, has_left)
            go(self.to_other)

        def forward(self):
            arrive(self.to_right, has_left)
            go(self.low_on, has_left)
            arrive(self.to_left, has_right)
            go(self.high_on, has_right)

        def finish(self):
            arrive(self.to_other)
            arrive(self.low_on, has_left)
            arrive(self.high_on, has_right)

    def vec_halo(k):
        def pressure(planes, rows):
            return vec.at[k, 3, planes, rows]

        def velocity(planes, rows):
            return vec.at[k, pl.ds(0, 3), planes, rows]

        p_src = (
            pressure(pl.ds(5, 5), own_rows), pressure(pl.ds(6, 5), own_rows),
            pressure(pl.ds(5, 6), out_tile),
        )
        u_src = (
            velocity(pl.ds(5, 2), own_rows), velocity(pl.ds(9, 2), own_rows),
            velocity(pl.ds(5, 6), out_tile),
        )
        p_halo = Halo(*p_src, pressure, pl.ds(0, 5), pl.ds(11, 5), pl.ds(5, 6))
        u_halo = Halo(*u_src, velocity, pl.ds(3, 2), pl.ds(11, 2), pl.ds(5, 6))
        return p_halo, u_halo

    def coef_halo(buffer):
        parts = (
            buffer(pl.ds(3, 3), own_rows), buffer(pl.ds(6, 3), own_rows), buffer(pl.ds(3, 6), out_tile),
        )
        return Halo(*parts, buffer, pl.ds(0, 3), pl.ds(9, 3), pl.ds(3, 6))

    p_halo, u_halo = vec_halo(0)
    coef_halos = [coef_halo(lambda planes, rows: coef.at[:, planes, rows])]
    loads[0].wait()
    p_halo.send()
    for copy in loads[1:]:
        copy.wait()
    for halo in coef_halos:
        halo.send()
    u_halo.send()

    last, first = lane_is(HALF - 1), lane_is(0)
    row = lax.broadcasted_iota(jnp.int32, (ROWS, HALF), 0)
    live = row != (ROWS - 1) * other

    def inside(plane):
        at = slab * 6 + plane - 5
        return jnp.logical_and(at >= 0, at < slabs * 6)

    def prepare(j, _):
        ok = jnp.logical_and(live, inside(j + 2))
        for d in range(3):
            half = [0.5 * h for h in get(coef, d, j)]
            put(work, [h - 1.0 for h in half], d, j)
            put(work, [-1.0 - h for h in half], d + 3, j)
        diagonal = [6.0 + h for h in get(coef, 3, j)]
        put(work, diagonal, 6, j)
        put(work, [jnp.where(ok, 1.0 / h, 0.0) for h in diagonal], 7, j)
        put(work, [jnp.where(ok, -1.0 / h, 0.0) for h in get(coef, 4, j)], 8, j)
        return 0

    def six(fxm, f, fxp):
        total = [a + b for a, b in zip(fxm, fxp)]
        for g in (up_y(f), down_y(f), up_z(f, last), down_z(f, first)):
            total = [a + b for a, b in zip(total, g)]
        return total

    def weights(j):
        return [get(work, i, j) for i in range(7)]

    def transport(fxm, f, fxp, w):
        total = [a * b for a, b in zip(w[6], f)]
        terms = ((0, fxp), (3, fxm), (1, up_y(f)), (4, down_y(f)), (2, up_z(f, last)), (5, down_z(f, first)))
        for i, g in terms:
            total = [t + a * b for t, a, b in zip(total, w[i], g)]
        return total

    def half_difference(a, b):
        return [0.5 * (m - n) for m, n in zip(a, b)]

    def gradient(fxm, f, fxp):
        return (
            half_difference(fxp, fxm),
            half_difference(up_y(f), down_y(f)),
            half_difference(up_z(f, last), down_z(f, first)),
        )

    def pressure_part(k):
        def masked(j):
            return [jnp.where(live, h, 0.0) for h in get(vec, k, 3, j)]

        def guess(j, _):
            scale = jnp.where(jnp.logical_and(live, inside(j)), 1.0 / 49.0, 0.0)
            f = masked(j)
            total = six(get(vec, k, 3, j - 1), f, get(vec, k, 3, j + 1))
            put(t1, [scale * (7.0 * a + b) for a, b in zip(f, total)], j)
            return 0

        lax.fori_loop(1, 15, guess, 0, unroll=7)

        def schur(j, _):
            value = transport(get(t1, j + 1), get(t1, j + 2), get(t1, j + 3), weights(j))
            put(q, [a * b for a, b in zip(value, get(work, 8, j))], k, j)
            return 0

        lax.fori_loop(0, 12, schur, 0, unroll=6)

    def velocity_part(k, target, after_pressure=lambda: None):
        def first_guess(j, _):
            slope = gradient(get(q, k, j), get(q, k, j + 1), get(q, k, j + 2))
            inverse = get(work, 7, j + 1)
            for d in range(3):
                r = [a - b for a, b in zip(get(vec, k, d, j + 3), slope[d])]
                put(res, r, d, j)
                put(y0, [a * b for a, b in zip(r, inverse)], d, j)
            return 0

        lax.fori_loop(0, 10, first_guess, 0, unroll=5)

        def second_guess(j, _):
            w = weights(j + 2)
            inverse = get(work, 7, j + 2)
            for d in range(3):
                f = get(y0, d, j + 1)
                value = transport(get(y0, d, j), f, get(y0, d, j + 2), w)
                r = get(res, d, j + 1)
                put(y1, [a + (b - c) * i for a, b, c, i in zip(f, r, value, inverse)], k, d, j)
            return 0

        lax.fori_loop(0, 8, second_guess, 0, unroll=4)

        def store(f, j, value):
            for i, h in enumerate(value):
                mine = jnp.where(sub == 0, h[0:16], h[8:24])
                target(f, j)[own_rows if k < 2 else slice(None), pl.ds(HALF * i, HALF)] = mine

        def image_pressure(j, _):
            pc = get(q, k, j + 3)
            total = six(get(q, k, j + 2), pc, get(q, k, j + 4))
            yc, zc = get(y1, k, 1, j + 1), get(y1, k, 2, j + 1)
            ends = (
                (get(y1, k, 0, j + 2), get(y1, k, 0, j)), (up_y(yc), down_y(yc)),
                (up_z(zc, last), down_z(zc, first)),
            )
            flow = [a - b for a, b in zip(*ends[0])]
            for high, low in ends[1:]:
                flow = [t + (a - b) for t, a, b in zip(flow, high, low)]
            store(3, j, [-0.5 * (a + (6.0 * b - c)) for a, b, c in zip(flow, pc, total)])
            return 0

        lax.fori_loop(0, 6, image_pressure, 0, unroll=6)
        after_pressure()

        def image_velocity(j, _):
            w = weights(j + 3)
            slope = gradient(get(q, k, j + 2), get(q, k, j + 3), get(q, k, j + 4))
            for d in range(3):
                value = transport(get(y1, k, d, j), get(y1, k, d, j + 1), get(y1, k, d, j + 2), w)
                store(d, j, [a + b for a, b in zip(value, slope[d])])
            return 0

        lax.fori_loop(0, 6, image_velocity, 0, unroll=3)

    lane8 = lax.broadcasted_iota(jnp.int32, (8, HALF), 1)

    def vectors(i, f, j):
        return vec[i, f, 5 + j, own_rows, :] if i < 3 else w2[f, j]

    def dots(new, olds):
        def step(j, accs):
            accs = list(accs)
            for f in range(4):
                b = vectors(new, f, j)
                for i, old in enumerate(olds):
                    prod = b * (b if old == new else vectors(old, f, j))
                    accs[i] = accs[i] + (
                        (prod[0:8, 0:HALF] + prod[0:8, HALF:]) + (prod[8:16, 0:HALF] + prod[8:16, HALF:])
                    )
            return tuple(accs)

        zero = jnp.zeros((8, HALF), jnp.float32)
        return lax.fori_loop(0, 6, step, tuple(zero for _ in olds), unroll=2)

    def pack(total, sums, at):
        for i, s in enumerate(sums):
            total = jnp.where(lane8 == at + i, jnp.sum(s, axis=1, keepdims=True), total)
        return total

    p_halo.forward()
    for halo in coef_halos:
        halo.forward()
    p_halo.finish()
    for halo in coef_halos:
        halo.finish()
    lax.fori_loop(0, 12, prepare, 0, unroll=2)
    pressure_part(0)
    u_halo.forward()
    u_halo.finish()
    halos = [vec_halo(1), vec_halo(2)]
    velocity_part(0, lambda f, j: vec.at[1, f, 5 + j], halos[0][0].send)

    gram = jnp.zeros((8, HALF), jnp.float32)
    at = 0
    for k in range(2):
        p_halo, u_halo = halos[k]
        u_halo.send()
        if k == 0:
            gram = pack(gram, dots(0, (0,)), 0)
            at = 1
        olds = tuple(range(k + 2))
        gram = pack(gram, dots(k + 1, olds), at)
        at += len(olds)
        p_halo.forward()
        p_halo.finish()
        pressure_part(k + 1)
        u_halo.forward()
        u_halo.finish()
        if k == 0:
            velocity_part(1, lambda f, j: vec.at[2, f, 5 + j], halos[1][0].send)
        else:
            velocity_part(2, lambda f, j: w2.at[f, j])
    gram = pack(gram, dots(3, (0, 1, 2, 3)), at)

    row_sum = jnp.sum(gram, axis=0, keepdims=True)
    for stage, (place, slots) in enumerate(((in_plane, slots_a), (z, slots_b))):
        part[stage] = row_sum
        slots[place] = row_sum
        copies = [remote(part.at[stage], slots.at[place], peer) for peer in peers(stage)]
        for copy in copies:
            go(copy)
        for copy in copies:
            arrive(copy)
        row_sum = jnp.sum(slots[...], axis=0)
    gram_out[...] = row_sum

    for copy, condition in started:
        if condition is None:
            copy.wait_send()
        else:
            pl.when(condition)(copy.wait_send)


def combine_kernel(vec, w2, y1, q, gram, basis, search, hess, b_out, s_out, out_sems):
    own_rows = pl.ds(pl.multiple_of(8 * lax.axis_index("sub"), 8), 16)

    total = gram[...]
    lane = lax.broadcasted_iota(jnp.int32, (1, HALF), 1)

    def entry(i):
        return jnp.broadcast_to(jnp.sum(jnp.where(lane == i, total, 0.0), axis=1, keepdims=True), (1, HALF))

    low = {}
    inverse = {}
    for i in range(4):
        for j in range(i + 1):
            value = entry(i * (i + 1) // 2 + j)
            for m in range(j):
                value = value - low[i, m] * low[j, m]
            if i == j:
                low[i, i] = jnp.sqrt(value)
                inverse[i] = 1.0 / low[i, i]
            else:
                low[i, j] = value * inverse[j]
    h = {}
    for j in range(3):
        for i in range(j + 2):
            value = low[j + 1, i]
            for m in range(j):
                if i <= m + 1:
                    value = value - low[j, m] * h[i, m]
            h[i, j] = value * inverse[j]
    at_row = lax.broadcasted_iota(jnp.int32, (4, HALF), 0)
    at_col = lax.broadcasted_iota(jnp.int32, (4, HALF), 1)
    table = jnp.zeros((4, HALF), jnp.float32)
    for (i, j), value in h.items():
        table = jnp.where(jnp.logical_and(at_row == i, at_col == j), value, table)
    hess[...] = table[:, 0:3]

    def wide(v):
        return jnp.concatenate([v, v], axis=1)

    scale = {key: wide(v) for key, v in low.items()}
    inv = {key: wide(v) for key, v in inverse.items()}

    writes = []
    for f in range(4):

        def body(j, _):
            raw = [vec[i, f, 5 + j, own_rows, :] for i in range(3)] + [w2[f, j]]
            found = [y1[i, f, 1 + j, own_rows, :] if f < 3 else q[i, 3 + j, own_rows, :] for i in range(3)]
            for values, dst in ((raw, b_out), (found, s_out)):
                done = []
                for i, value in enumerate(values):
                    for m in range(i):
                        value = value - scale[i, m] * done[m]
                    value = value * inv[i]
                    dst[i, f, j] = value
                    done.append(value)
            return 0

        lax.fori_loop(0, 6, body, 0)
        for i, (src, dst) in enumerate(((b_out, basis), (s_out, search))):
            copy = pltpu.make_async_copy(src.at[:, f], dst.at[:, f], out_sems.at[f, i])
            copy.start()
            writes.append(copy)
    for copy in writes:
        copy.wait()


def per_device(start, wind, reaction, mass):
    f32 = jnp.float32
    hbm_spec = pl.BlockSpec(memory_space=pltpu.HBM)
    vmem_spec = pl.BlockSpec(memory_space=pltpu.VMEM)
    n_remote = 10 * 3 + 5 + 2 * NX_T * NY_T + NZ_T
    kept = (
        jax.ShapeDtypeStruct((3, 4, 16, ROWS, 256), f32),
        jax.ShapeDtypeStruct((4, 6, 16, 256), f32),
        jax.ShapeDtypeStruct((3, 3, 8, ROWS, 256), f32),
        jax.ShapeDtypeStruct((3, 12, ROWS, 256), f32),
        jax.ShapeDtypeStruct((1, HALF), f32),
    )
    arrays = [pltpu.with_memory_space_constraint(a, pltpu.HBM) for a in (start, wind, reaction, mass)]
    outs = pl.pallas_call(
        krylov_kernel,
        out_shape=kept,
        in_specs=[hbm_spec] * 4,
        out_specs=(vmem_spec,) * 5,
        scratch_shapes=[
            pltpu.VMEM((5, 12, ROWS, 256), f32),
            pltpu.VMEM((9, 12, ROWS, 256), f32),
            pltpu.VMEM((16, ROWS, 256), f32),
            pltpu.VMEM((3, 10, ROWS, 256), f32),
            pltpu.VMEM((3, 10, ROWS, 256), f32),
            pltpu.VMEM((2, 1, HALF), f32),
            pltpu.VMEM((2 * NX_T * NY_T, 1, HALF), f32),
            pltpu.VMEM((NZ_T, 1, HALF), f32),
            pltpu.SemaphoreType.DMA((n_remote,)),
            pltpu.SemaphoreType.DMA((n_remote,)),
            pltpu.SemaphoreType.DMA((4,)),
        ],
        compiler_params=pltpu.CompilerParams(
            collective_id=0, has_side_effects=True, vmem_limit_bytes=24 * 2**20
        ),
        name="krylov",
    )(*arrays)
    return tuple(pl.pallas_call(
        combine_kernel,
        out_shape=(
            jax.ShapeDtypeStruct((4, 4, 6, 16, 256), f32),
            jax.ShapeDtypeStruct((3, 4, 6, 16, 256), f32),
            jax.ShapeDtypeStruct((4, 3), f32),
        ),
        in_specs=[vmem_spec] * 5,
        out_specs=(hbm_spec, hbm_spec, vmem_spec),
        scratch_shapes=[
            pltpu.VMEM((4, 4, 6, 16, 256), f32),
            pltpu.VMEM((3, 4, 6, 16, 256), f32),
            pltpu.SemaphoreType.DMA((4, 2)),
        ],
        compiler_params=pltpu.CompilerParams(vmem_limit_bytes=24 * 2**20),
        name="combine",
    )(*outs))


def solution(mesh):
    in_specs = (
        P(None, "slab", "sub", None),
        P(None, "slab", "sub", None),
        P("slab", "sub", None),
        P("slab", "sub", None),
    )
    out_specs = (P(None, None, "slab", "sub", None), P(None, None, "slab", "sub", None), P())
    return jax.shard_map(per_device, mesh=mesh, in_specs=in_specs, out_specs=out_specs, check_vma=False)
```

```python
import functools

import jax
import jax.numpy as jnp
from jax import lax
from jax.experimental import pallas as pl
from jax.experimental.pallas import tpu as pltpu
from jax.sharding import PartitionSpec as P

MESH_ID = pl.DeviceIdType.MESH
NX_T, NY_T, NZ_T = 4, 4, 8
ROWS = 24
HALF = 128


def lane_is(lane):
    return lax.broadcasted_iota(jnp.int32, (ROWS, HALF), 1) == lane


def get(ref, *lead):
    return ref[(*lead, slice(None), pl.ds(0, HALF))], ref[(*lead, slice(None), pl.ds(HALF, HALF))]


def put(ref, value, *lead):
    ref[(*lead, slice(None), pl.ds(0, HALF))] = value[0]
    ref[(*lead, slice(None), pl.ds(HALF, HALF))] = value[1]


def up_z(f, last):
    low, high = pltpu.roll(f[0], HALF - 1, 1), pltpu.roll(f[1], HALF - 1, 1)
    return jnp.where(last, high, low), jnp.where(last, 0.0, high)


def down_z(f, first):
    low, high = pltpu.roll(f[0], 1, 1), pltpu.roll(f[1], 1, 1)
    return jnp.where(first, 0.0, low), jnp.where(first, low, high)


def up_y(f):
    return tuple(pltpu.roll(h, ROWS - 1, 0) for h in f)


def down_y(f):
    return tuple(pltpu.roll(h, 1, 0) for h in f)


def krylov_kernel(
    start, wind, reac, mass,
    vec, w2, y1, q, gram_out,
    coef, work, t1, res, y0, part, slots_a, slots_b,
    send_sems, recv_sems, load_sems,
):
    slab, sub = lax.axis_index("slab"), lax.axis_index("sub")
    slabs = lax.axis_size("slab")
    other = 1 - sub
    z = lax.div(slab, NX_T * NY_T)
    has_left, has_right = slab > 0, slab < slabs - 1
    left, right = jnp.maximum(slab - 1, 0), jnp.minimum(slab + 1, slabs - 1)
    own_rows = pl.ds(pl.multiple_of(8 * sub, 8), 16)
    out_tile = pl.ds(8, 8)
    in_tile = pl.ds(pl.multiple_of(16 * sub, 8), 8)

    plane = 2 * NX_T * NY_T
    in_plane = lax.rem(2 * slab + sub, plane)

    def peers(stage):
        if stage == 0:
            for k in range(1, plane):
                at = lax.rem(in_plane + k, plane)
                yield (z * (NX_T * NY_T) + lax.div(at, 2), lax.rem(at, 2))
        else:
            for k in range(1, NZ_T):
                yield (slab + NX_T * NY_T * (lax.rem(z + k, NZ_T) - z), sub)

    loads = [
        pltpu.make_async_copy(start, vec.at[0, :, pl.ds(5, 6), own_rows], load_sems.at[0]),
        pltpu.make_async_copy(wind, coef.at[pl.ds(0, 3), pl.ds(3, 6), own_rows], load_sems.at[1]),
        pltpu.make_async_copy(reac, coef.at[3, pl.ds(3, 6), own_rows], load_sems.at[2]),
        pltpu.make_async_copy(mass, coef.at[4, pl.ds(3, 6), own_rows], load_sems.at[3]),
    ]
    for copy in loads:
        copy.start()

    barrier = pltpu.get_barrier_semaphore()
    count = 0
    for stage in range(2):
        for peer in peers(stage):
            pl.semaphore_signal(barrier, inc=1, device_id=peer, device_id_type=MESH_ID)
            count += 1

    @pl.when(has_left)
    def _():
        pl.semaphore_signal(barrier, inc=1, device_id=(left, sub), device_id_type=MESH_ID)

    @pl.when(has_right)
    def _():
        pl.semaphore_signal(barrier, inc=1, device_id=(right, sub), device_id_type=MESH_ID)

    halo_rows = pl.ds(pl.multiple_of(16 * other, 8), 8)
    for k in range(3):
        for d in range(3):
            for plane_at in (3, 12):
                vec[k, d, plane_at, halo_rows] = jnp.zeros((8, 256), jnp.float32)

    def clear(planes, coef_planes):
        for k in range(3):
            for f in range(4):
                vec[k, f, planes] = jnp.zeros((5, ROWS, 256), jnp.float32)
        for f in range(5):
            coef[f, coef_planes] = jnp.zeros((3, ROWS, 256), jnp.float32)

    @pl.when(jnp.logical_not(has_left))
    def _():
        clear(pl.ds(0, 5), pl.ds(0, 3))

    @pl.when(jnp.logical_not(has_right))
    def _():
        clear(pl.ds(11, 5), pl.ds(9, 3))

    pl.semaphore_wait(
        barrier, count + has_left.astype(jnp.int32) + has_right.astype(jnp.int32)
    )

    used = [0]

    def remote(src, dst, device):
        at = used[0]
        used[0] += 1
        return pltpu.make_async_remote_copy(
            src_ref=src, dst_ref=dst, send_sem=send_sems.at[at], recv_sem=recv_sems.at[at],
            device_id=device, device_id_type=MESH_ID,
        )

    started = []

    def go(copy, condition=None):
        started.append((copy, condition))
        if condition is None:
            copy.start()
        else:
            pl.when(condition)(copy.start)

    def arrive(copy, condition=None):
        if condition is None:
            copy.wait_recv()
        else:
            pl.when(condition)(copy.wait_recv)

    class Halo:
        def __init__(self, src_low, src_high, src_tile, buffer, low, high, own):
            self.to_right = remote(src_high, buffer(low, own_rows), (right, sub))
            self.to_left = remote(src_low, buffer(high, own_rows), (left, sub))
            self.to_other = remote(src_tile, buffer(own, in_tile), (slab, other))
            self.low_on = remote(buffer(low, out_tile), buffer(low, in_tile), (slab, other))
            self.high_on = remote(buffer(high, out_tile), buffer(high, in_tile), (slab, other))

        def send(self):
            go(self.to_right, has_right)
            go(self.to_left, has_left)
            go(self.to_other)

        def forward(self):
            arrive(self.to_right, has_left)
            go(self.low_on, has_left)
            arrive(self.to_left, has_right)
            go(self.high_on, has_right)

        def finish(self):
            arrive(self.to_other)
            arrive(self.low_on, has_left)
            arrive(self.high_on, has_right)

    class FarHalo:
        def __init__(self, to_right, to_left):
            self.to_right, self.to_left = to_right, to_left

        def send(self):
            go(self.to_right, has_right)
            go(self.to_left, has_left)

        def finish(self):
            arrive(self.to_right, has_left)
            arrive(self.to_left, has_right)

    def vec_halo(k):
        def pressure(planes, rows):
            return vec.at[k, 3, planes, rows]

        def velocity(planes, rows):
            return vec.at[k, pl.ds(0, 3), planes, rows]

        p_src = (
            pressure(pl.ds(5, 5), own_rows), pressure(pl.ds(6, 5), own_rows),
            pressure(pl.ds(5, 6), out_tile),
        )
        near_src = (
            velocity(pl.ds(5, 1), own_rows), velocity(pl.ds(10, 1), own_rows),
            velocity(pl.ds(5, 6), out_tile),
        )
        p_halo = Halo(*p_src, pressure, pl.ds(0, 5), pl.ds(11, 5), pl.ds(5, 6))
        near = Halo(*near_src, velocity, pl.ds(4, 1), pl.ds(11, 1), pl.ds(5, 6))
        far = FarHalo(
            remote(velocity(pl.ds(9, 1), own_rows), velocity(pl.ds(3, 1), own_rows), (right, sub)),
            remote(velocity(pl.ds(6, 1), own_rows), velocity(pl.ds(12, 1), own_rows), (left, sub)),
        )
        return p_halo, near, far

    def coef_halo(buffer):
        parts = (
            buffer(pl.ds(3, 3), own_rows), buffer(pl.ds(6, 3), own_rows), buffer(pl.ds(3, 6), out_tile),
        )
        return Halo(*parts, buffer, pl.ds(0, 3), pl.ds(9, 3), pl.ds(3, 6))

    p_halo, near, far = vec_halo(0)
    coef_halos = [coef_halo(lambda planes, rows: coef.at[:, planes, rows])]
    loads[0].wait()
    p_halo.send()
    for copy in loads[1:]:
        copy.wait()
    for halo in coef_halos:
        halo.send()
    near.send()
    far.send()

    last, first = lane_is(HALF - 1), lane_is(0)
    row = lax.broadcasted_iota(jnp.int32, (ROWS, HALF), 0)
    live = row != (ROWS - 1) * other

    def inside(plane):
        at = slab * 6 + plane - 5
        return jnp.logical_and(at >= 0, at < slabs * 6)

    def prepare(j, _):
        ok = jnp.logical_and(live, inside(j + 2))
        for d in range(3):
            half = [0.5 * h for h in get(coef, d, j)]
            put(work, [h - 1.0 for h in half], d, j)
            put(work, [-1.0 - h for h in half], d + 3, j)
        diagonal = [6.0 + h for h in get(coef, 3, j)]
        put(work, diagonal, 6, j)
        put(work, [jnp.where(ok, 1.0 / h, 0.0) for h in diagonal], 7, j)
        put(work, [jnp.where(ok, -1.0 / h, 0.0) for h in get(coef, 4, j)], 8, j)
        return 0

    def six(fxm, f, fxp):
        total = [a + b for a, b in zip(fxm, fxp)]
        for g in (up_y(f), down_y(f), up_z(f, last), down_z(f, first)):
            total = [a + b for a, b in zip(total, g)]
        return total

    def weights(j):
        return [get(work, i, j) for i in range(7)]

    def transport(fxm, f, fxp, w):
        total = [a * b for a, b in zip(w[6], f)]
        terms = ((0, fxp), (3, fxm), (1, up_y(f)), (4, down_y(f)), (2, up_z(f, last)), (5, down_z(f, first)))
        for i, g in terms:
            total = [t + a * b for t, a, b in zip(total, w[i], g)]
        return total

    def half_difference(a, b):
        return [0.5 * (m - n) for m, n in zip(a, b)]

    def gradient(fxm, f, fxp):
        return (
            half_difference(fxp, fxm),
            half_difference(up_y(f), down_y(f)),
            half_difference(up_z(f, last), down_z(f, first)),
        )

    def pressure_part(k):
        def masked(j):
            return [jnp.where(live, h, 0.0) for h in get(vec, k, 3, j)]

        def guess(j, _):
            scale = jnp.where(jnp.logical_and(live, inside(j)), 1.0 / 49.0, 0.0)
            f = masked(j)
            total = six(get(vec, k, 3, j - 1), f, get(vec, k, 3, j + 1))
            put(t1, [scale * (7.0 * a + b) for a, b in zip(f, total)], j)
            return 0

        lax.fori_loop(1, 15, guess, 0, unroll=7)

        def schur(j, _):
            value = transport(get(t1, j + 1), get(t1, j + 2), get(t1, j + 3), weights(j))
            put(q, [a * b for a, b in zip(value, get(work, 8, j))], k, j)
            return 0

        lax.fori_loop(0, 12, schur, 0, unroll=6)

    def velocity_part(k, target, after_pressure=lambda: None):
        def first_guess(j, _):
            slope = gradient(get(q, k, j), get(q, k, j + 1), get(q, k, j + 2))
            inverse = get(work, 7, j + 1)
            for d in range(3):
                r = [a - b for a, b in zip(get(vec, k, d, j + 3), slope[d])]
                put(res, r, d, j)
                put(y0, [a * b for a, b in zip(r, inverse)], d, j)
            return 0

        lax.fori_loop(0, 10, first_guess, 0, unroll=5)

        def second_guess(j, _):
            w = weights(j + 2)
            inverse = get(work, 7, j + 2)
            for d in range(3):
                f = get(y0, d, j + 1)
                value = transport(get(y0, d, j), f, get(y0, d, j + 2), w)
                r = get(res, d, j + 1)
                put(y1, [a + (b - c) * i for a, b, c, i in zip(f, r, value, inverse)], k, d, j)
            return 0

        lax.fori_loop(0, 8, second_guess, 0, unroll=4)

        def store(f, j, value):
            for i, h in enumerate(value):
                mine = jnp.where(sub == 0, h[0:16], h[8:24])
                target(f, j)[own_rows if k < 2 else slice(None), pl.ds(HALF * i, HALF)] = mine

        def image_pressure(j, _):
            pc = get(q, k, j + 3)
            total = six(get(q, k, j + 2), pc, get(q, k, j + 4))
            yc, zc = get(y1, k, 1, j + 1), get(y1, k, 2, j + 1)
            ends = (
                (get(y1, k, 0, j + 2), get(y1, k, 0, j)), (up_y(yc), down_y(yc)),
                (up_z(zc, last), down_z(zc, first)),
            )
            flow = [a - b for a, b in zip(*ends[0])]
            for high, low in ends[1:]:
                flow = [t + (a - b) for t, a, b in zip(flow, high, low)]
            store(3, j, [-0.5 * (a + (6.0 * b - c)) for a, b, c in zip(flow, pc, total)])
            return 0

        lax.fori_loop(0, 6, image_pressure, 0, unroll=6)
        after_pressure()

        def image_velocity(j, _):
            w = weights(j + 3)
            slope = gradient(get(q, k, j + 2), get(q, k, j + 3), get(q, k, j + 4))
            for d in range(3):
                value = transport(get(y1, k, d, j), get(y1, k, d, j + 1), get(y1, k, d, j + 2), w)
                store(d, j, [a + b for a, b in zip(value, slope[d])])
            return 0

        lax.fori_loop(0, 6, image_velocity, 0, unroll=3)

    lane8 = lax.broadcasted_iota(jnp.int32, (8, HALF), 1)

    def vectors(i, f, j):
        return vec[i, f, 5 + j, own_rows, :] if i < 3 else w2[f, j]

    def dots(new, olds):
        def step(j, accs):
            accs = list(accs)
            for f in range(4):
                b = vectors(new, f, j)
                for i, old in enumerate(olds):
                    prod = b * (b if old == new else vectors(old, f, j))
                    accs[i] = accs[i] + (
                        (prod[0:8, 0:HALF] + prod[0:8, HALF:]) + (prod[8:16, 0:HALF] + prod[8:16, HALF:])
                    )
            return tuple(accs)

        zero = jnp.zeros((8, HALF), jnp.float32)
        return lax.fori_loop(0, 6, step, tuple(zero for _ in olds), unroll=2)

    def pack(total, sums, at):
        for i, s in enumerate(sums):
            total = jnp.where(lane8 == at + i, jnp.sum(s, axis=1, keepdims=True), total)
        return total

    p_halo.forward()
    for halo in coef_halos:
        halo.forward()
    p_halo.finish()
    for halo in coef_halos:
        halo.finish()
    near.forward()
    lax.fori_loop(0, 12, prepare, 0, unroll=2)
    pressure_part(0)
    near.finish()
    far.finish()
    halos = [vec_halo(1), vec_halo(2)]
    velocity_part(0, lambda f, j: vec.at[1, f, 5 + j], halos[0][0].send)

    gram = jnp.zeros((8, HALF), jnp.float32)
    at = 0
    for k in range(2):
        p_halo, near, far = halos[k]
        near.send()
        far.send()
        if k == 0:
            gram = pack(gram, dots(0, (0,)), 0)
            at = 1
        olds = tuple(range(k + 2))
        gram = pack(gram, dots(k + 1, olds), at)
        at += len(olds)
        p_halo.forward()
        p_halo.finish()
        near.forward()
        pressure_part(k + 1)
        near.finish()
        far.finish()
        if k == 0:
            velocity_part(1, lambda f, j: vec.at[2, f, 5 + j], halos[1][0].send)
        else:
            velocity_part(2, lambda f, j: w2.at[f, j])
    gram = pack(gram, dots(3, (0, 1, 2, 3)), at)

    row_sum = jnp.sum(gram, axis=0, keepdims=True)
    for stage, (place, slots) in enumerate(((in_plane, slots_a), (z, slots_b))):
        part[stage] = row_sum
        slots[place] = row_sum
        copies = [remote(part.at[stage], slots.at[place], peer) for peer in peers(stage)]
        for copy in copies:
            go(copy)
        for copy in copies:
            arrive(copy)
        row_sum = jnp.sum(slots[...], axis=0)
    gram_out[...] = row_sum

    for copy, condition in started:
        if condition is None:
            copy.wait_send()
        else:
            pl.when(condition)(copy.wait_send)


def combine_kernel(vec, w2, y1, q, gram, basis, search, hess, b_out, s_out, out_sems):
    own_rows = pl.ds(pl.multiple_of(8 * lax.axis_index("sub"), 8), 16)

    total = gram[...]
    lane = lax.broadcasted_iota(jnp.int32, (1, HALF), 1)

    def entry(i):
        return jnp.broadcast_to(jnp.sum(jnp.where(lane == i, total, 0.0), axis=1, keepdims=True), (1, HALF))

    low = {}
    inverse = {}
    for i in range(4):
        for j in range(i + 1):
            value = entry(i * (i + 1) // 2 + j)
            for m in range(j):
                value = value - low[i, m] * low[j, m]
            if i == j:
                low[i, i] = jnp.sqrt(value)
                inverse[i] = 1.0 / low[i, i]
            else:
                low[i, j] = value * inverse[j]
    h = {}
    for j in range(3):
        for i in range(j + 2):
            value = low[j + 1, i]
            for m in range(j):
                if i <= m + 1:
                    value = value - low[j, m] * h[i, m]
            h[i, j] = value * inverse[j]
    at_row = lax.broadcasted_iota(jnp.int32, (4, HALF), 0)
    at_col = lax.broadcasted_iota(jnp.int32, (4, HALF), 1)
    table = jnp.zeros((4, HALF), jnp.float32)
    for (i, j), value in h.items():
        table = jnp.where(jnp.logical_and(at_row == i, at_col == j), value, table)
    hess[...] = table[:, 0:3]

    def wide(v):
        return jnp.concatenate([v, v], axis=1)

    scale = {key: wide(v) for key, v in low.items()}
    inv = {key: wide(v) for key, v in inverse.items()}

    writes = []
    for f in range(4):

        def body(j, _):
            raw = [vec[i, f, 5 + j, own_rows, :] for i in range(3)] + [w2[f, j]]
            found = [y1[i, f, 1 + j, own_rows, :] if f < 3 else q[i, 3 + j, own_rows, :] for i in range(3)]
            for values, dst in ((raw, b_out), (found, s_out)):
                done = []
                for i, value in enumerate(values):
                    for m in range(i):
                        value = value - scale[i, m] * done[m]
                    value = value * inv[i]
                    dst[i, f, j] = value
                    done.append(value)
            return 0

        lax.fori_loop(0, 6, body, 0, unroll=3)
        for i, (src, dst) in enumerate(((b_out, basis), (s_out, search))):
            copy = pltpu.make_async_copy(src.at[:, f], dst.at[:, f], out_sems.at[f, i])
            copy.start()
            writes.append(copy)
    for copy in writes:
        copy.wait()


def per_device(start, wind, reaction, mass):
    f32 = jnp.float32
    hbm_spec = pl.BlockSpec(memory_space=pltpu.HBM)
    vmem_spec = pl.BlockSpec(memory_space=pltpu.VMEM)
    n_remote = 12 * 3 + 5 + 2 * NX_T * NY_T + NZ_T
    kept = (
        jax.ShapeDtypeStruct((3, 4, 16, ROWS, 256), f32),
        jax.ShapeDtypeStruct((4, 6, 16, 256), f32),
        jax.ShapeDtypeStruct((3, 3, 8, ROWS, 256), f32),
        jax.ShapeDtypeStruct((3, 12, ROWS, 256), f32),
        jax.ShapeDtypeStruct((1, HALF), f32),
    )
    arrays = [pltpu.with_memory_space_constraint(a, pltpu.HBM) for a in (start, wind, reaction, mass)]
    outs = pl.pallas_call(
        krylov_kernel,
        out_shape=kept,
        in_specs=[hbm_spec] * 4,
        out_specs=(vmem_spec,) * 5,
        scratch_shapes=[
            pltpu.VMEM((5, 12, ROWS, 256), f32),
            pltpu.VMEM((9, 12, ROWS, 256), f32),
            pltpu.VMEM((16, ROWS, 256), f32),
            pltpu.VMEM((3, 10, ROWS, 256), f32),
            pltpu.VMEM((3, 10, ROWS, 256), f32),
            pltpu.VMEM((2, 1, HALF), f32),
            pltpu.VMEM((2 * NX_T * NY_T, 1, HALF), f32),
            pltpu.VMEM((NZ_T, 1, HALF), f32),
            pltpu.SemaphoreType.DMA((n_remote,)),
            pltpu.SemaphoreType.DMA((n_remote,)),
            pltpu.SemaphoreType.DMA((4,)),
        ],
        compiler_params=pltpu.CompilerParams(
            collective_id=0, has_side_effects=True, vmem_limit_bytes=24 * 2**20
        ),
        name="krylov",
    )(*arrays)
    return tuple(pl.pallas_call(
        combine_kernel,
        out_shape=(
            jax.ShapeDtypeStruct((4, 4, 6, 16, 256), f32),
            jax.ShapeDtypeStruct((3, 4, 6, 16, 256), f32),
            jax.ShapeDtypeStruct((4, 3), f32),
        ),
        in_specs=[vmem_spec] * 5,
        out_specs=(hbm_spec, hbm_spec, vmem_spec),
        scratch_shapes=[
            pltpu.VMEM((4, 4, 6, 16, 256), f32),
            pltpu.VMEM((3, 4, 6, 16, 256), f32),
            pltpu.SemaphoreType.DMA((4, 2)),
        ],
        compiler_params=pltpu.CompilerParams(vmem_limit_bytes=24 * 2**20),
        name="combine",
    )(*outs))


def solution(mesh):
    in_specs = (
        P(None, "slab", "sub", None),
        P(None, "slab", "sub", None),
        P("slab", "sub", None),
        P("slab", "sub", None),
    )
    out_specs = (P(None, None, "slab", "sub", None), P(None, None, "slab", "sub", None), P())
    return jax.shard_map(per_device, mesh=mesh, in_specs=in_specs, out_specs=out_specs, check_vma=False)
```

```python
import functools

import jax
import jax.numpy as jnp
from jax import lax
from jax.experimental import pallas as pl
from jax.experimental.pallas import tpu as pltpu
from jax.sharding import PartitionSpec as P

MESH_ID = pl.DeviceIdType.MESH
NX_T, NY_T, NZ_T = 4, 4, 8
ROWS = 24
HALF = 128


def lane_is(lane):
    return lax.broadcasted_iota(jnp.int32, (ROWS, HALF), 1) == lane


def get(ref, *lead):
    return ref[(*lead, slice(None), pl.ds(0, HALF))], ref[(*lead, slice(None), pl.ds(HALF, HALF))]


def put(ref, value, *lead):
    ref[(*lead, slice(None), pl.ds(0, HALF))] = value[0]
    ref[(*lead, slice(None), pl.ds(HALF, HALF))] = value[1]


def up_z(f, last):
    low, high = pltpu.roll(f[0], HALF - 1, 1), pltpu.roll(f[1], HALF - 1, 1)
    return jnp.where(last, high, low), jnp.where(last, 0.0, high)


def down_z(f, first):
    low, high = pltpu.roll(f[0], 1, 1), pltpu.roll(f[1], 1, 1)
    return jnp.where(first, 0.0, low), jnp.where(first, low, high)


def up_y(f):
    return tuple(pltpu.roll(h, ROWS - 1, 0) for h in f)


def down_y(f):
    return tuple(pltpu.roll(h, 1, 0) for h in f)


def krylov_kernel(
    start, wind, reac, mass,
    vec, w2, y1, q, gram_out,
    coef, work, t1, res, y0, part, slots_a, slots_b,
    send_sems, recv_sems, load_sems,
):
    slab, sub = lax.axis_index("slab"), lax.axis_index("sub")
    slabs = lax.axis_size("slab")
    other = 1 - sub
    z = lax.div(slab, NX_T * NY_T)
    has_left, has_right = slab > 0, slab < slabs - 1
    left, right = jnp.maximum(slab - 1, 0), jnp.minimum(slab + 1, slabs - 1)
    own_rows = pl.ds(pl.multiple_of(8 * sub, 8), 16)
    out_tile = pl.ds(8, 8)
    in_tile = pl.ds(pl.multiple_of(16 * sub, 8), 8)

    plane = 2 * NX_T * NY_T
    in_plane = lax.rem(2 * slab + sub, plane)

    def peers(stage):
        if stage == 0:
            for k in range(1, plane):
                at = lax.rem(in_plane + k, plane)
                yield (z * (NX_T * NY_T) + lax.div(at, 2), lax.rem(at, 2))
        else:
            for k in range(1, NZ_T):
                yield (slab + NX_T * NY_T * (lax.rem(z + k, NZ_T) - z), sub)

    loads = [
        pltpu.make_async_copy(start, vec.at[0, :, pl.ds(5, 6), own_rows], load_sems.at[0]),
        pltpu.make_async_copy(wind, coef.at[pl.ds(0, 3), pl.ds(2, 6), own_rows], load_sems.at[1]),
        pltpu.make_async_copy(reac, coef.at[3, pl.ds(2, 6), own_rows], load_sems.at[2]),
        pltpu.make_async_copy(mass, coef.at[4, pl.ds(2, 6), own_rows], load_sems.at[3]),
    ]
    for copy in loads:
        copy.start()

    barrier = pltpu.get_barrier_semaphore()
    count = 0
    for stage in range(2):
        for peer in peers(stage):
            pl.semaphore_signal(barrier, inc=1, device_id=peer, device_id_type=MESH_ID)
            count += 1

    @pl.when(has_left)
    def _():
        pl.semaphore_signal(barrier, inc=1, device_id=(left, sub), device_id_type=MESH_ID)

    @pl.when(has_right)
    def _():
        pl.semaphore_signal(barrier, inc=1, device_id=(right, sub), device_id_type=MESH_ID)

    halo_rows = pl.ds(pl.multiple_of(16 * other, 8), 8)
    for k in range(3):
        for d in range(3):
            for plane_at in (3, 12):
                vec[k, d, plane_at, halo_rows] = jnp.zeros((8, 256), jnp.float32)
        for plane_at in (0, 11):
            q[k, plane_at, halo_rows] = jnp.zeros((8, 256), jnp.float32)

    def clear(planes, coef_planes, far_plane):
        for k in range(3):
            for f in range(4):
                vec[k, f, planes] = jnp.zeros((5, ROWS, 256), jnp.float32)
        for f in range(5):
            coef[f, coef_planes] = jnp.zeros((2, ROWS, 256), jnp.float32)
        for k in range(3):
            q[k, far_plane] = jnp.zeros((ROWS, 256), jnp.float32)

    @pl.when(jnp.logical_not(has_left))
    def _():
        clear(pl.ds(0, 5), pl.ds(0, 2), 0)

    @pl.when(jnp.logical_not(has_right))
    def _():
        clear(pl.ds(11, 5), pl.ds(8, 2), 11)

    pl.semaphore_wait(
        barrier, count + has_left.astype(jnp.int32) + has_right.astype(jnp.int32)
    )

    used = [0]

    def remote(src, dst, device):
        at = used[0]
        used[0] += 1
        return pltpu.make_async_remote_copy(
            src_ref=src, dst_ref=dst, send_sem=send_sems.at[at], recv_sem=recv_sems.at[at],
            device_id=device, device_id_type=MESH_ID,
        )

    started = []

    def go(copy, condition=None):
        started.append((copy, condition))
        if condition is None:
            copy.start()
        else:
            pl.when(condition)(copy.start)

    def arrive(copy, condition=None):
        if condition is None:
            copy.wait_recv()
        else:
            pl.when(condition)(copy.wait_recv)

    class Halo:
        def __init__(self, src_low, src_high, src_tile, buffer, low, high, own):
            self.to_right = remote(src_high, buffer(low, own_rows), (right, sub))
            self.to_left = remote(src_low, buffer(high, own_rows), (left, sub))
            self.to_other = remote(src_tile, buffer(own, in_tile), (slab, other))
            self.low_on = remote(buffer(low, out_tile), buffer(low, in_tile), (slab, other))
            self.high_on = remote(buffer(high, out_tile), buffer(high, in_tile), (slab, other))

        def send(self):
            go(self.to_right, has_right)
            go(self.to_left, has_left)
            go(self.to_other)

        def forward(self):
            arrive(self.to_right, has_left)
            go(self.low_on, has_left)
            arrive(self.to_left, has_right)
            go(self.high_on, has_right)

        def finish(self):
            arrive(self.low_on, has_left)
            arrive(self.high_on, has_right)

    class FarHalo:
        def __init__(self, to_right, to_left):
            self.to_right, self.to_left = to_right, to_left

        def send(self):
            go(self.to_right, has_right)
            go(self.to_left, has_left)

        def finish(self):
            arrive(self.to_right, has_left)
            arrive(self.to_left, has_right)

    def vec_halo(k):
        def pressure(planes, rows):
            return vec.at[k, 3, planes, rows]

        def velocity(planes, rows):
            return vec.at[k, pl.ds(0, 3), planes, rows]

        p_src = (
            pressure(pl.ds(5, 4), own_rows), pressure(pl.ds(7, 4), own_rows),
            pressure(pl.ds(5, 6), out_tile),
        )
        near_src = (
            velocity(pl.ds(5, 1), own_rows), velocity(pl.ds(10, 1), own_rows),
            velocity(pl.ds(5, 6), out_tile),
        )
        p_halo = Halo(*p_src, pressure, pl.ds(1, 4), pl.ds(11, 4), pl.ds(5, 6))
        near = Halo(*near_src, velocity, pl.ds(4, 1), pl.ds(11, 1), pl.ds(5, 6))
        far = FarHalo(
            remote(velocity(pl.ds(9, 1), own_rows), velocity(pl.ds(3, 1), own_rows), (right, sub)),
            remote(velocity(pl.ds(6, 1), own_rows), velocity(pl.ds(12, 1), own_rows), (left, sub)),
        )
        schur_far = FarHalo(
            remote(q.at[k, 6, own_rows], q.at[k, 0, own_rows], (right, sub)),
            remote(q.at[k, 5, own_rows], q.at[k, 11, own_rows], (left, sub)),
        )
        return p_halo, near, far, schur_far

    def coef_halo(buffer):
        parts = (
            buffer(pl.ds(2, 2), own_rows), buffer(pl.ds(6, 2), own_rows), buffer(pl.ds(2, 6), out_tile),
        )
        return Halo(*parts, buffer, pl.ds(0, 2), pl.ds(8, 2), pl.ds(2, 6))

    halos = [vec_halo(k) for k in range(3)]
    coef_halo = coef_halo(lambda planes, rows: coef.at[:, planes, rows])
    loads[0].wait()
    halos[0][0].send()
    for copy in loads[1:]:
        copy.wait()
    coef_halo.send()
    for halo in halos[0][1:3]:
        halo.send()

    last, first = lane_is(HALF - 1), lane_is(0)
    row = lax.broadcasted_iota(jnp.int32, (ROWS, HALF), 0)
    live = row != (ROWS - 1) * other

    def inside(plane):
        at = slab * 6 + plane - 5
        return jnp.logical_and(at >= 0, at < slabs * 6)

    def prepare(j, _):
        ok = jnp.logical_and(live, inside(j + 3))
        for d in range(3):
            half = [0.5 * h for h in get(coef, d, j)]
            put(work, [h - 1.0 for h in half], d, j)
            put(work, [-1.0 - h for h in half], d + 3, j)
        diagonal = [6.0 + h for h in get(coef, 3, j)]
        put(work, diagonal, 6, j)
        put(work, [jnp.where(ok, 1.0 / h, 0.0) for h in diagonal], 7, j)
        put(work, [jnp.where(ok, -1.0 / h, 0.0) for h in get(coef, 4, j)], 8, j)
        return 0

    def six(fxm, f, fxp):
        total = [a + b for a, b in zip(fxm, fxp)]
        for g in (up_y(f), down_y(f), up_z(f, last), down_z(f, first)):
            total = [a + b for a, b in zip(total, g)]
        return total

    def weights(j):
        return [get(work, i, j) for i in range(7)]

    def transport(fxm, f, fxp, w):
        total = [a * b for a, b in zip(w[6], f)]
        terms = ((0, fxp), (3, fxm), (1, up_y(f)), (4, down_y(f)), (2, up_z(f, last)), (5, down_z(f, first)))
        for i, g in terms:
            total = [t + a * b for t, a, b in zip(total, w[i], g)]
        return total

    def half_difference(a, b):
        return [0.5 * (m - n) for m, n in zip(a, b)]

    def gradient(fxm, f, fxp):
        return (
            half_difference(fxp, fxm),
            half_difference(up_y(f), down_y(f)),
            half_difference(up_z(f, last), down_z(f, first)),
        )

    def loop(count, body, plane, unroll):
        def step(i, _):
            body(plane(i))
            return 0

        lax.fori_loop(0, count, step, 0, unroll=unroll)

    def guess(k, j):
        scale = jnp.where(jnp.logical_and(live, inside(j)), 1.0 / 49.0, 0.0)
        f = [jnp.where(live, h, 0.0) for h in get(vec, k, 3, j)]
        total = six(get(vec, k, 3, j - 1), f, get(vec, k, 3, j + 1))
        put(t1, [scale * (7.0 * a + b) for a, b in zip(f, total)], j)

    def schur(k, j):
        value = transport(get(t1, j - 1), get(t1, j), get(t1, j + 1), weights(j - 3))
        put(q, [a * b for a, b in zip(value, get(work, 8, j - 3))], k, j - 2)

    def pressure_inner(k):
        loop(4, functools.partial(guess, k), lambda i: i + 6, 4)
        loop(2, functools.partial(schur, k), lambda i: i + 7, 2)

    def pressure_outer(k):
        loop(8, functools.partial(guess, k), lambda i: i + 2 + 4 * lax.div(i, 4), 4)
        loop(8, functools.partial(schur, k), lambda i: i + 3 + 2 * lax.div(i, 4), 4)

    def first_guess(k, j):
        slope = gradient(get(q, k, j), get(q, k, j + 1), get(q, k, j + 2))
        inverse = get(work, 7, j)
        for d in range(3):
            r = [a - b for a, b in zip(get(vec, k, d, j + 3), slope[d])]
            put(res, r, d, j)
            put(y0, [a * b for a, b in zip(r, inverse)], d, j)

    def second_guess(k, j):
        w = weights(j + 1)
        inverse = get(work, 7, j + 1)
        for d in range(3):
            f = get(y0, d, j + 1)
            value = transport(get(y0, d, j), f, get(y0, d, j + 2), w)
            r = get(res, d, j + 1)
            put(y1, [a + (b - c) * i for a, b, c, i in zip(f, r, value, inverse)], k, d, j)

    def velocity_inner(k):
        loop(8, functools.partial(first_guess, k), lambda i: i + 1, 4)
        loop(6, functools.partial(second_guess, k), lambda i: i + 1, 3)

    def velocity_outer(k, target, after_pressure=lambda: None):
        loop(2, functools.partial(first_guess, k), lambda i: 9 * i, 2)
        loop(2, functools.partial(second_guess, k), lambda i: 7 * i, 2)

        def store(f, j, value):
            for i, h in enumerate(value):
                mine = jnp.where(sub == 0, h[0:16], h[8:24])
                target(f, j)[own_rows if k < 2 else slice(None), pl.ds(HALF * i, HALF)] = mine

        def image_pressure(j, _):
            pc = get(q, k, j + 3)
            total = six(get(q, k, j + 2), pc, get(q, k, j + 4))
            yc, zc = get(y1, k, 1, j + 1), get(y1, k, 2, j + 1)
            ends = (
                (get(y1, k, 0, j + 2), get(y1, k, 0, j)), (up_y(yc), down_y(yc)),
                (up_z(zc, last), down_z(zc, first)),
            )
            flow = [a - b for a, b in zip(*ends[0])]
            for high, low in ends[1:]:
                flow = [t + (a - b) for t, a, b in zip(flow, high, low)]
            store(3, j, [-0.5 * (a + (6.0 * b - c)) for a, b, c in zip(flow, pc, total)])
            return 0

        lax.fori_loop(0, 6, image_pressure, 0, unroll=6)
        after_pressure()

        def image_velocity(j, _):
            w = weights(j + 2)
            slope = gradient(get(q, k, j + 2), get(q, k, j + 3), get(q, k, j + 4))
            for d in range(3):
                value = transport(get(y1, k, d, j), get(y1, k, d, j + 1), get(y1, k, d, j + 2), w)
                store(d, j, [a + b for a, b in zip(value, slope[d])])
            return 0

        lax.fori_loop(0, 6, image_velocity, 0, unroll=3)

    lane8 = lax.broadcasted_iota(jnp.int32, (8, HALF), 1)

    def vectors(i, f, j):
        return vec[i, f, 5 + j, own_rows, :] if i < 3 else w2[f, j]

    def dots(new, olds):
        def step(j, accs):
            accs = list(accs)
            for f in range(4):
                b = vectors(new, f, j)
                for i, old in enumerate(olds):
                    prod = b * (b if old == new else vectors(old, f, j))
                    accs[i] = accs[i] + (
                        (prod[0:8, 0:HALF] + prod[0:8, HALF:]) + (prod[8:16, 0:HALF] + prod[8:16, HALF:])
                    )
            return tuple(accs)

        zero = jnp.zeros((8, HALF), jnp.float32)
        return lax.fori_loop(0, 6, step, tuple(zero for _ in olds), unroll=2)

    def pack(total, sums, at):
        for i, s in enumerate(sums):
            total = jnp.where(lane8 == at + i, jnp.sum(s, axis=1, keepdims=True), total)
        return total

    def application(k, target, after_pressure=lambda: None):
        p_halo, near, far, schur_far = halos[k]
        arrive(p_halo.to_other)
        if k == 0:
            arrive(coef_halo.to_other)
            lax.fori_loop(2, 8, prepare, 0, unroll=2)
        pressure_inner(k)
        schur_far.send()
        p_halo.forward()
        if k == 0:
            coef_halo.forward()
        p_halo.finish()
        near.forward()
        if k == 0:
            coef_halo.finish()
            for planes in (0, 8):
                lax.fori_loop(planes, planes + 2, prepare, 0, unroll=2)
        pressure_outer(k)
        arrive(near.to_other)
        near.finish()
        velocity_inner(k)
        far.finish()
        schur_far.finish()
        velocity_outer(k, target, after_pressure)

    application(0, lambda f, j: vec.at[1, f, 5 + j], halos[1][0].send)
    gram = jnp.zeros((8, HALF), jnp.float32)
    at = 0
    for k in range(2):
        halos[k + 1][1].send()
        halos[k + 1][2].send()
        if k == 0:
            gram = pack(gram, dots(0, (0,)), 0)
            at = 1
        olds = tuple(range(k + 2))
        gram = pack(gram, dots(k + 1, olds), at)
        at += len(olds)
        if k == 0:
            application(1, lambda f, j: vec.at[2, f, 5 + j], halos[2][0].send)
        else:
            application(2, lambda f, j: w2.at[f, j])
    gram = pack(gram, dots(3, (0, 1, 2, 3)), at)

    row_sum = jnp.sum(gram, axis=0, keepdims=True)
    for stage, (place, slots) in enumerate(((in_plane, slots_a), (z, slots_b))):
        part[stage] = row_sum
        slots[place] = row_sum
        copies = [remote(part.at[stage], slots.at[place], peer) for peer in peers(stage)]
        for copy in copies:
            go(copy)
        for copy in copies:
            arrive(copy)
        row_sum = jnp.sum(slots[...], axis=0)
    gram_out[...] = row_sum

    for copy, condition in started:
        if condition is None:
            copy.wait_send()
        else:
            pl.when(condition)(copy.wait_send)


def combine_kernel(vec, w2, y1, q, gram, basis, search, hess, b_out, s_out, out_sems):
    own_rows = pl.ds(pl.multiple_of(8 * lax.axis_index("sub"), 8), 16)

    total = gram[...]
    lane = lax.broadcasted_iota(jnp.int32, (1, HALF), 1)

    def entry(i):
        return jnp.broadcast_to(jnp.sum(jnp.where(lane == i, total, 0.0), axis=1, keepdims=True), (1, HALF))

    low = {}
    inverse = {}
    for i in range(4):
        for j in range(i + 1):
            value = entry(i * (i + 1) // 2 + j)
            for m in range(j):
                value = value - low[i, m] * low[j, m]
            if i == j:
                low[i, i] = jnp.sqrt(value)
                inverse[i] = 1.0 / low[i, i]
            else:
                low[i, j] = value * inverse[j]
    h = {}
    for j in range(3):
        for i in range(j + 2):
            value = low[j + 1, i]
            for m in range(j):
                if i <= m + 1:
                    value = value - low[j, m] * h[i, m]
            h[i, j] = value * inverse[j]
    at_row = lax.broadcasted_iota(jnp.int32, (4, HALF), 0)
    at_col = lax.broadcasted_iota(jnp.int32, (4, HALF), 1)
    table = jnp.zeros((4, HALF), jnp.float32)
    for (i, j), value in h.items():
        table = jnp.where(jnp.logical_and(at_row == i, at_col == j), value, table)
    hess[...] = table[:, 0:3]

    def wide(v):
        return jnp.concatenate([v, v], axis=1)

    scale = {key: wide(v) for key, v in low.items()}
    inv = {key: wide(v) for key, v in inverse.items()}

    writes = []
    for f in range(4):

        def body(j, _):
            raw = [vec[i, f, 5 + j, own_rows, :] for i in range(3)] + [w2[f, j]]
            found = [y1[i, f, 1 + j, own_rows, :] if f < 3 else q[i, 3 + j, own_rows, :] for i in range(3)]
            for values, dst in ((raw, b_out), (found, s_out)):
                done = []
                for i, value in enumerate(values):
                    for m in range(i):
                        value = value - scale[i, m] * done[m]
                    value = value * inv[i]
                    dst[i, f, j] = value
                    done.append(value)
            return 0

        lax.fori_loop(0, 6, body, 0, unroll=3)
        for i, (src, dst) in enumerate(((b_out, basis), (s_out, search))):
            copy = pltpu.make_async_copy(src.at[:, f], dst.at[:, f], out_sems.at[f, i])
            copy.start()
            writes.append(copy)
    for copy in writes:
        copy.wait()


def per_device(start, wind, reaction, mass):
    f32 = jnp.float32
    hbm_spec = pl.BlockSpec(memory_space=pltpu.HBM)
    vmem_spec = pl.BlockSpec(memory_space=pltpu.VMEM)
    n_remote = 14 * 3 + 5 + 2 * NX_T * NY_T + NZ_T
    kept = (
        jax.ShapeDtypeStruct((3, 4, 16, ROWS, 256), f32),
        jax.ShapeDtypeStruct((4, 6, 16, 256), f32),
        jax.ShapeDtypeStruct((3, 3, 8, ROWS, 256), f32),
        jax.ShapeDtypeStruct((3, 12, ROWS, 256), f32),
        jax.ShapeDtypeStruct((1, HALF), f32),
    )
    arrays = [pltpu.with_memory_space_constraint(a, pltpu.HBM) for a in (start, wind, reaction, mass)]
    outs = pl.pallas_call(
        krylov_kernel,
        out_shape=kept,
        in_specs=[hbm_spec] * 4,
        out_specs=(vmem_spec,) * 5,
        scratch_shapes=[
            pltpu.VMEM((5, 10, ROWS, 256), f32),
            pltpu.VMEM((9, 10, ROWS, 256), f32),
            pltpu.VMEM((16, ROWS, 256), f32),
            pltpu.VMEM((3, 10, ROWS, 256), f32),
            pltpu.VMEM((3, 10, ROWS, 256), f32),
            pltpu.VMEM((2, 1, HALF), f32),
            pltpu.VMEM((2 * NX_T * NY_T, 1, HALF), f32),
            pltpu.VMEM((NZ_T, 1, HALF), f32),
            pltpu.SemaphoreType.DMA((n_remote,)),
            pltpu.SemaphoreType.DMA((n_remote,)),
            pltpu.SemaphoreType.DMA((4,)),
        ],
        compiler_params=pltpu.CompilerParams(
            collective_id=0, has_side_effects=True, vmem_limit_bytes=24 * 2**20
        ),
        name="krylov",
    )(*arrays)
    return tuple(pl.pallas_call(
        combine_kernel,
        out_shape=(
            jax.ShapeDtypeStruct((4, 4, 6, 16, 256), f32),
            jax.ShapeDtypeStruct((3, 4, 6, 16, 256), f32),
            jax.ShapeDtypeStruct((4, 3), f32),
        ),
        in_specs=[vmem_spec] * 5,
        out_specs=(hbm_spec, hbm_spec, vmem_spec),
        scratch_shapes=[
            pltpu.VMEM((4, 4, 6, 16, 256), f32),
            pltpu.VMEM((3, 4, 6, 16, 256), f32),
            pltpu.SemaphoreType.DMA((4, 2)),
        ],
        compiler_params=pltpu.CompilerParams(vmem_limit_bytes=24 * 2**20),
        name="combine",
    )(*outs))


def solution(mesh):
    in_specs = (
        P(None, "slab", "sub", None),
        P(None, "slab", "sub", None),
        P("slab", "sub", None),
        P("slab", "sub", None),
    )
    out_specs = (P(None, None, "slab", "sub", None), P(None, None, "slab", "sub", None), P())
    return jax.shard_map(per_device, mesh=mesh, in_specs=in_specs, out_specs=out_specs, check_vma=False)
```

```python
import functools

import jax
import jax.numpy as jnp
from jax import lax
from jax.experimental import pallas as pl
from jax.experimental.pallas import tpu as pltpu
from jax.sharding import PartitionSpec as P

MESH_ID = pl.DeviceIdType.MESH
NX_T, NY_T, NZ_T = 4, 4, 8
ROWS = 24
HALF = 128


def lane_is(lane):
    return lax.broadcasted_iota(jnp.int32, (ROWS, HALF), 1) == lane


def get(ref, *lead):
    return ref[(*lead, slice(None), pl.ds(0, HALF))], ref[(*lead, slice(None), pl.ds(HALF, HALF))]


def put(ref, value, *lead):
    ref[(*lead, slice(None), pl.ds(0, HALF))] = value[0]
    ref[(*lead, slice(None), pl.ds(HALF, HALF))] = value[1]


def up_z(f, last):
    low, high = pltpu.roll(f[0], HALF - 1, 1), pltpu.roll(f[1], HALF - 1, 1)
    return jnp.where(last, high, low), jnp.where(last, 0.0, high)


def down_z(f, first):
    low, high = pltpu.roll(f[0], 1, 1), pltpu.roll(f[1], 1, 1)
    return jnp.where(first, 0.0, low), jnp.where(first, low, high)


def up_y(f):
    return tuple(pltpu.roll(h, ROWS - 1, 0) for h in f)


def down_y(f):
    return tuple(pltpu.roll(h, 1, 0) for h in f)


def krylov_kernel(
    start, wind, reac, mass,
    vec, w2, y1, q, gram_out,
    coef, work, t1, res, y0, part, slots_a, slots_b,
    send_sems, recv_sems, load_sems, told,
):
    slab, sub = lax.axis_index("slab"), lax.axis_index("sub")
    slabs = lax.axis_size("slab")
    other = 1 - sub
    z = lax.div(slab, NX_T * NY_T)
    has_left, has_right = slab > 0, slab < slabs - 1
    left, right = jnp.maximum(slab - 1, 0), jnp.minimum(slab + 1, slabs - 1)
    own_rows = pl.ds(pl.multiple_of(8 * sub, 8), 16)
    out_tile = pl.ds(8, 8)
    in_tile = pl.ds(pl.multiple_of(16 * sub, 8), 8)

    plane = 2 * NX_T * NY_T
    in_plane = lax.rem(2 * slab + sub, plane)

    def peers(stage):
        if stage == 0:
            for k in range(1, plane):
                at = lax.rem(in_plane + k, plane)
                yield (z * (NX_T * NY_T) + lax.div(at, 2), lax.rem(at, 2))
        else:
            for k in range(1, NZ_T):
                yield (slab + NX_T * NY_T * (lax.rem(z + k, NZ_T) - z), sub)

    loads = [
        pltpu.make_async_copy(start, vec.at[0, :, pl.ds(5, 6), own_rows], load_sems.at[0]),
        pltpu.make_async_copy(wind, coef.at[pl.ds(0, 3), pl.ds(2, 6), own_rows], load_sems.at[1]),
        pltpu.make_async_copy(reac, coef.at[3, pl.ds(2, 6), own_rows], load_sems.at[2]),
        pltpu.make_async_copy(mass, coef.at[4, pl.ds(2, 6), own_rows], load_sems.at[3]),
    ]
    for copy in loads:
        copy.start()

    x, y = lax.rem(slab, NX_T), lax.rem(lax.div(slab, NX_T), NY_T)

    def line_x():
        for k in range(1, 2 * NX_T):
            at = lax.rem(2 * x + sub + k, 2 * NX_T)
            yield (slab - x + lax.div(at, 2), lax.rem(at, 2))

    def line_y():
        for k in range(1, NY_T):
            yield (slab + NX_T * (lax.rem(y + k, NY_T) - y), sub)

    def near_z():
        for k in (1, NZ_T - 1):
            yield (slab + NX_T * NY_T * (lax.rem(z + k, NZ_T) - z), sub)

    def signal_all(sem, devices):
        for device in devices:
            pl.semaphore_signal(sem, inc=1, device_id=device, device_id_type=MESH_ID)
        return len(devices)

    def tell(turn):
        return signal_all(told.at[turn], [*line_y(), *near_z()] if turn == 0 else [*near_z()])

    def hear(turn, count):
        pl.semaphore_wait(told.at[turn], count)

    barrier = pltpu.get_barrier_semaphore()
    count = signal_all(barrier, [*line_x(), *line_y(), *near_z()])

    @pl.when(has_left)
    def _():
        pl.semaphore_signal(barrier, inc=1, device_id=(left, sub), device_id_type=MESH_ID)

    @pl.when(has_right)
    def _():
        pl.semaphore_signal(barrier, inc=1, device_id=(right, sub), device_id_type=MESH_ID)

    halo_rows = pl.ds(pl.multiple_of(16 * other, 8), 8)
    for k in range(3):
        for d in range(3):
            for plane_at in (3, 12):
                vec[k, d, plane_at, halo_rows] = jnp.zeros((8, 256), jnp.float32)
        for plane_at in (0, 11):
            q[k, plane_at, halo_rows] = jnp.zeros((8, 256), jnp.float32)

    def clear(planes, coef_planes, far_plane):
        for k in range(3):
            for f in range(4):
                vec[k, f, planes] = jnp.zeros((5, ROWS, 256), jnp.float32)
        for f in range(5):
            coef[f, coef_planes] = jnp.zeros((2, ROWS, 256), jnp.float32)
        for k in range(3):
            q[k, far_plane] = jnp.zeros((ROWS, 256), jnp.float32)

    @pl.when(jnp.logical_not(has_left))
    def _():
        clear(pl.ds(0, 5), pl.ds(0, 2), 0)

    @pl.when(jnp.logical_not(has_right))
    def _():
        clear(pl.ds(11, 5), pl.ds(8, 2), 11)

    pl.semaphore_wait(
        barrier, count + has_left.astype(jnp.int32) + has_right.astype(jnp.int32)
    )
    expected = tell(0)

    used = [0]

    def remote(src, dst, device):
        at = used[0]
        used[0] += 1
        return pltpu.make_async_remote_copy(
            src_ref=src, dst_ref=dst, send_sem=send_sems.at[at], recv_sem=recv_sems.at[at],
            device_id=device, device_id_type=MESH_ID,
        )

    started = []

    def go(copy, condition=None):
        started.append((copy, condition))
        if condition is None:
            copy.start()
        else:
            pl.when(condition)(copy.start)

    def arrive(copy, condition=None):
        if condition is None:
            copy.wait_recv()
        else:
            pl.when(condition)(copy.wait_recv)

    class Halo:
        def __init__(self, src_low, src_high, src_tile, buffer, low, high, own):
            self.to_right = remote(src_high, buffer(low, own_rows), (right, sub))
            self.to_left = remote(src_low, buffer(high, own_rows), (left, sub))
            self.to_other = remote(src_tile, buffer(own, in_tile), (slab, other))
            self.low_on = remote(buffer(low, out_tile), buffer(low, in_tile), (slab, other))
            self.high_on = remote(buffer(high, out_tile), buffer(high, in_tile), (slab, other))

        def send(self):
            go(self.to_right, has_right)
            go(self.to_left, has_left)
            go(self.to_other)

        def forward(self):
            arrive(self.to_right, has_left)
            go(self.low_on, has_left)
            arrive(self.to_left, has_right)
            go(self.high_on, has_right)

        def finish(self):
            arrive(self.low_on, has_left)
            arrive(self.high_on, has_right)

    class FarHalo:
        def __init__(self, to_right, to_left):
            self.to_right, self.to_left = to_right, to_left

        def send(self):
            go(self.to_right, has_right)
            go(self.to_left, has_left)

        def finish(self):
            arrive(self.to_right, has_left)
            arrive(self.to_left, has_right)

    def vec_halo(k):
        def pressure(planes, rows):
            return vec.at[k, 3, planes, rows]

        def velocity(planes, rows):
            return vec.at[k, pl.ds(0, 3), planes, rows]

        p_src = (
            pressure(pl.ds(5, 4), own_rows), pressure(pl.ds(7, 4), own_rows),
            pressure(pl.ds(5, 6), out_tile),
        )
        near_src = (
            velocity(pl.ds(5, 1), own_rows), velocity(pl.ds(10, 1), own_rows),
            velocity(pl.ds(5, 6), out_tile),
        )
        p_halo = Halo(*p_src, pressure, pl.ds(1, 4), pl.ds(11, 4), pl.ds(5, 6))
        near = Halo(*near_src, velocity, pl.ds(4, 1), pl.ds(11, 1), pl.ds(5, 6))
        far = FarHalo(
            remote(velocity(pl.ds(9, 1), own_rows), velocity(pl.ds(3, 1), own_rows), (right, sub)),
            remote(velocity(pl.ds(6, 1), own_rows), velocity(pl.ds(12, 1), own_rows), (left, sub)),
        )
        schur_far = FarHalo(
            remote(q.at[k, 6, own_rows], q.at[k, 0, own_rows], (right, sub)),
            remote(q.at[k, 5, own_rows], q.at[k, 11, own_rows], (left, sub)),
        )
        return p_halo, near, far, schur_far

    def coef_halo(buffer):
        parts = (
            buffer(pl.ds(2, 2), own_rows), buffer(pl.ds(6, 2), own_rows), buffer(pl.ds(2, 6), out_tile),
        )
        return Halo(*parts, buffer, pl.ds(0, 2), pl.ds(8, 2), pl.ds(2, 6))

    halos = [vec_halo(k) for k in range(3)]
    coef_halo = coef_halo(lambda planes, rows: coef.at[:, planes, rows])
    loads[0].wait()
    halos[0][0].send()
    for copy in loads[1:]:
        copy.wait()
    coef_halo.send()
    for halo in halos[0][1:3]:
        halo.send()

    last, first = lane_is(HALF - 1), lane_is(0)
    row = lax.broadcasted_iota(jnp.int32, (ROWS, HALF), 0)
    live = row != (ROWS - 1) * other

    def inside(plane):
        at = slab * 6 + plane - 5
        return jnp.logical_and(at >= 0, at < slabs * 6)

    def prepare(j, _):
        ok = jnp.logical_and(live, inside(j + 3))
        for d in range(3):
            half = [0.5 * h for h in get(coef, d, j)]
            put(work, [h - 1.0 for h in half], d, j)
            put(work, [-1.0 - h for h in half], d + 3, j)
        diagonal = [6.0 + h for h in get(coef, 3, j)]
        put(work, diagonal, 6, j)
        put(work, [jnp.where(ok, 1.0 / h, 0.0) for h in diagonal], 7, j)
        put(work, [jnp.where(ok, -1.0 / h, 0.0) for h in get(coef, 4, j)], 8, j)
        return 0

    def six(fxm, f, fxp):
        total = [a + b for a, b in zip(fxm, fxp)]
        for g in (up_y(f), down_y(f), up_z(f, last), down_z(f, first)):
            total = [a + b for a, b in zip(total, g)]
        return total

    def weights(j):
        return [get(work, i, j) for i in range(7)]

    def transport(fxm, f, fxp, w):
        total = [a * b for a, b in zip(w[6], f)]
        terms = ((0, fxp), (3, fxm), (1, up_y(f)), (4, down_y(f)), (2, up_z(f, last)), (5, down_z(f, first)))
        for i, g in terms:
            total = [t + a * b for t, a, b in zip(total, w[i], g)]
        return total

    def half_difference(a, b):
        return [0.5 * (m - n) for m, n in zip(a, b)]

    def gradient(fxm, f, fxp):
        return (
            half_difference(fxp, fxm),
            half_difference(up_y(f), down_y(f)),
            half_difference(up_z(f, last), down_z(f, first)),
        )

    def loop(count, body, plane, unroll):
        def step(i, _):
            body(plane(i))
            return 0

        lax.fori_loop(0, count, step, 0, unroll=unroll)

    def guess(k, j):
        scale = jnp.where(jnp.logical_and(live, inside(j)), 1.0 / 49.0, 0.0)
        f = [jnp.where(live, h, 0.0) for h in get(vec, k, 3, j)]
        total = six(get(vec, k, 3, j - 1), f, get(vec, k, 3, j + 1))
        put(t1, [scale * (7.0 * a + b) for a, b in zip(f, total)], j)

    def schur(k, j):
        value = transport(get(t1, j - 1), get(t1, j), get(t1, j + 1), weights(j - 3))
        put(q, [a * b for a, b in zip(value, get(work, 8, j - 3))], k, j - 2)

    def pressure_inner(k):
        loop(4, functools.partial(guess, k), lambda i: i + 6, 4)
        loop(2, functools.partial(schur, k), lambda i: i + 7, 2)

    def pressure_outer(k):
        loop(8, functools.partial(guess, k), lambda i: i + 2 + 4 * lax.div(i, 4), 4)
        loop(8, functools.partial(schur, k), lambda i: i + 3 + 2 * lax.div(i, 4), 4)

    def first_guess(k, j):
        slope = gradient(get(q, k, j), get(q, k, j + 1), get(q, k, j + 2))
        inverse = get(work, 7, j)
        for d in range(3):
            r = [a - b for a, b in zip(get(vec, k, d, j + 3), slope[d])]
            put(res, r, d, j)
            put(y0, [a * b for a, b in zip(r, inverse)], d, j)

    def second_guess(k, j):
        w = weights(j + 1)
        inverse = get(work, 7, j + 1)
        for d in range(3):
            f = get(y0, d, j + 1)
            value = transport(get(y0, d, j), f, get(y0, d, j + 2), w)
            r = get(res, d, j + 1)
            put(y1, [a + (b - c) * i for a, b, c, i in zip(f, r, value, inverse)], k, d, j)

    def velocity_inner(k):
        loop(8, functools.partial(first_guess, k), lambda i: i + 1, 4)
        loop(6, functools.partial(second_guess, k), lambda i: i + 1, 3)

    def velocity_outer(k, target, after_pressure=lambda: None):
        loop(2, functools.partial(first_guess, k), lambda i: 9 * i, 2)
        loop(2, functools.partial(second_guess, k), lambda i: 7 * i, 2)

        def store(f, j, value):
            for i, h in enumerate(value):
                mine = jnp.where(sub == 0, h[0:16], h[8:24])
                target(f, j)[own_rows if k < 2 else slice(None), pl.ds(HALF * i, HALF)] = mine

        def image_pressure(j, _):
            pc = get(q, k, j + 3)
            total = six(get(q, k, j + 2), pc, get(q, k, j + 4))
            yc, zc = get(y1, k, 1, j + 1), get(y1, k, 2, j + 1)
            ends = (
                (get(y1, k, 0, j + 2), get(y1, k, 0, j)), (up_y(yc), down_y(yc)),
                (up_z(zc, last), down_z(zc, first)),
            )
            flow = [a - b for a, b in zip(*ends[0])]
            for high, low in ends[1:]:
                flow = [t + (a - b) for t, a, b in zip(flow, high, low)]
            store(3, j, [-0.5 * (a + (6.0 * b - c)) for a, b, c in zip(flow, pc, total)])
            return 0

        lax.fori_loop(0, 6, image_pressure, 0, unroll=6)
        after_pressure()

        def image_velocity(j, _):
            w = weights(j + 2)
            slope = gradient(get(q, k, j + 2), get(q, k, j + 3), get(q, k, j + 4))
            for d in range(3):
                value = transport(get(y1, k, d, j), get(y1, k, d, j + 1), get(y1, k, d, j + 2), w)
                store(d, j, [a + b for a, b in zip(value, slope[d])])
            return 0

        lax.fori_loop(0, 6, image_velocity, 0, unroll=3)

    lane8 = lax.broadcasted_iota(jnp.int32, (8, HALF), 1)

    def vectors(i, f, j):
        return vec[i, f, 5 + j, own_rows, :] if i < 3 else w2[f, j]

    def dots(new, olds):
        def step(j, accs):
            accs = list(accs)
            for f in range(4):
                b = vectors(new, f, j)
                for i, old in enumerate(olds):
                    prod = b * (b if old == new else vectors(old, f, j))
                    accs[i] = accs[i] + (
                        (prod[0:8, 0:HALF] + prod[0:8, HALF:]) + (prod[8:16, 0:HALF] + prod[8:16, HALF:])
                    )
            return tuple(accs)

        zero = jnp.zeros((8, HALF), jnp.float32)
        return lax.fori_loop(0, 6, step, tuple(zero for _ in olds), unroll=2)

    def pack(total, sums, at):
        for i, s in enumerate(sums):
            total = jnp.where(lane8 == at + i, jnp.sum(s, axis=1, keepdims=True), total)
        return total

    def application(k, target, after_pressure=lambda: None):
        p_halo, near, far, schur_far = halos[k]
        arrive(p_halo.to_other)
        if k == 0:
            arrive(coef_halo.to_other)
            lax.fori_loop(2, 8, prepare, 0, unroll=2)
        pressure_inner(k)
        schur_far.send()
        p_halo.forward()
        if k == 0:
            coef_halo.forward()
        p_halo.finish()
        near.forward()
        if k == 0:
            coef_halo.finish()
            for planes in (0, 8):
                lax.fori_loop(planes, planes + 2, prepare, 0, unroll=2)
        pressure_outer(k)
        arrive(near.to_other)
        near.finish()
        velocity_inner(k)
        far.finish()
        schur_far.finish()
        velocity_outer(k, target, after_pressure)

    application(0, lambda f, j: vec.at[1, f, 5 + j], halos[1][0].send)
    gram = jnp.zeros((8, HALF), jnp.float32)
    at = 0
    for k in range(2):
        halos[k + 1][1].send()
        halos[k + 1][2].send()
        hear(k, expected)
        expected = tell(k + 1)
        if k == 0:
            gram = pack(gram, dots(0, (0,)), 0)
            at = 1
        olds = tuple(range(k + 2))
        gram = pack(gram, dots(k + 1, olds), at)
        at += len(olds)
        if k == 0:
            application(1, lambda f, j: vec.at[2, f, 5 + j], halos[2][0].send)
        else:
            application(2, lambda f, j: w2.at[f, j])
    hear(2, expected)
    gram = pack(gram, dots(3, (0, 1, 2, 3)), at)

    row_sum = jnp.sum(gram, axis=0, keepdims=True)
    for stage, (place, slots) in enumerate(((in_plane, slots_a), (z, slots_b))):
        part[stage] = row_sum
        slots[place] = row_sum
        copies = [remote(part.at[stage], slots.at[place], peer) for peer in peers(stage)]
        for copy in copies:
            go(copy)
        for copy in copies:
            arrive(copy)
        row_sum = jnp.sum(slots[...], axis=0)
    gram_out[...] = row_sum

    for copy, condition in started:
        if condition is None:
            copy.wait_send()
        else:
            pl.when(condition)(copy.wait_send)


def combine_kernel(vec, w2, y1, q, gram, basis, search, hess, b_out, s_out, out_sems):
    own_rows = pl.ds(pl.multiple_of(8 * lax.axis_index("sub"), 8), 16)

    total = gram[...]
    lane = lax.broadcasted_iota(jnp.int32, (1, HALF), 1)

    def entry(i):
        return jnp.broadcast_to(jnp.sum(jnp.where(lane == i, total, 0.0), axis=1, keepdims=True), (1, HALF))

    low = {}
    inverse = {}
    for i in range(4):
        for j in range(i + 1):
            value = entry(i * (i + 1) // 2 + j)
            for m in range(j):
                value = value - low[i, m] * low[j, m]
            if i == j:
                low[i, i] = jnp.sqrt(value)
                inverse[i] = 1.0 / low[i, i]
            else:
                low[i, j] = value * inverse[j]
    h = {}
    for j in range(3):
        for i in range(j + 2):
            value = low[j + 1, i]
            for m in range(j):
                if i <= m + 1:
                    value = value - low[j, m] * h[i, m]
            h[i, j] = value * inverse[j]
    at_row = lax.broadcasted_iota(jnp.int32, (4, HALF), 0)
    at_col = lax.broadcasted_iota(jnp.int32, (4, HALF), 1)
    table = jnp.zeros((4, HALF), jnp.float32)
    for (i, j), value in h.items():
        table = jnp.where(jnp.logical_and(at_row == i, at_col == j), value, table)
    hess[...] = table[:, 0:3]

    def wide(v):
        return jnp.concatenate([v, v], axis=1)

    scale = {key: wide(v) for key, v in low.items()}
    inv = {key: wide(v) for key, v in inverse.items()}

    writes = []
    for f in range(4):

        def body(j, _):
            raw = [vec[i, f, 5 + j, own_rows, :] for i in range(3)] + [w2[f, j]]
            found = [y1[i, f, 1 + j, own_rows, :] if f < 3 else q[i, 3 + j, own_rows, :] for i in range(3)]
            for values, dst in ((raw, b_out), (found, s_out)):
                done = []
                for i, value in enumerate(values):
                    for m in range(i):
                        value = value - scale[i, m] * done[m]
                    value = value * inv[i]
                    dst[i, f, j] = value
                    done.append(value)
            return 0

        lax.fori_loop(0, 6, body, 0, unroll=3)
        for i, (src, dst) in enumerate(((b_out, basis), (s_out, search))):
            copy = pltpu.make_async_copy(src.at[:, f], dst.at[:, f], out_sems.at[f, i])
            copy.start()
            writes.append(copy)
    for copy in writes:
        copy.wait()


def per_device(start, wind, reaction, mass):
    f32 = jnp.float32
    hbm_spec = pl.BlockSpec(memory_space=pltpu.HBM)
    vmem_spec = pl.BlockSpec(memory_space=pltpu.VMEM)
    n_remote = 14 * 3 + 5 + 2 * NX_T * NY_T + NZ_T
    kept = (
        jax.ShapeDtypeStruct((3, 4, 16, ROWS, 256), f32),
        jax.ShapeDtypeStruct((4, 6, 16, 256), f32),
        jax.ShapeDtypeStruct((3, 3, 8, ROWS, 256), f32),
        jax.ShapeDtypeStruct((3, 12, ROWS, 256), f32),
        jax.ShapeDtypeStruct((1, HALF), f32),
    )
    arrays = [pltpu.with_memory_space_constraint(a, pltpu.HBM) for a in (start, wind, reaction, mass)]
    outs = pl.pallas_call(
        krylov_kernel,
        out_shape=kept,
        in_specs=[hbm_spec] * 4,
        out_specs=(vmem_spec,) * 5,
        scratch_shapes=[
            pltpu.VMEM((5, 10, ROWS, 256), f32),
            pltpu.VMEM((9, 10, ROWS, 256), f32),
            pltpu.VMEM((16, ROWS, 256), f32),
            pltpu.VMEM((3, 10, ROWS, 256), f32),
            pltpu.VMEM((3, 10, ROWS, 256), f32),
            pltpu.VMEM((2, 1, HALF), f32),
            pltpu.VMEM((2 * NX_T * NY_T, 1, HALF), f32),
            pltpu.VMEM((NZ_T, 1, HALF), f32),
            pltpu.SemaphoreType.DMA((n_remote,)),
            pltpu.SemaphoreType.DMA((n_remote,)),
            pltpu.SemaphoreType.DMA((4,)),
            pltpu.SemaphoreType.REGULAR((3,)),
        ],
        compiler_params=pltpu.CompilerParams(
            collective_id=0, has_side_effects=True, vmem_limit_bytes=24 * 2**20
        ),
        name="krylov",
    )(*arrays)
    return tuple(pl.pallas_call(
        combine_kernel,
        out_shape=(
            jax.ShapeDtypeStruct((4, 4, 6, 16, 256), f32),
            jax.ShapeDtypeStruct((3, 4, 6, 16, 256), f32),
            jax.ShapeDtypeStruct((4, 3), f32),
        ),
        in_specs=[vmem_spec] * 5,
        out_specs=(hbm_spec, hbm_spec, vmem_spec),
        scratch_shapes=[
            pltpu.VMEM((4, 4, 6, 16, 256), f32),
            pltpu.VMEM((3, 4, 6, 16, 256), f32),
            pltpu.SemaphoreType.DMA((4, 2)),
        ],
        compiler_params=pltpu.CompilerParams(vmem_limit_bytes=24 * 2**20),
        name="combine",
    )(*outs))


def solution(mesh):
    in_specs = (
        P(None, "slab", "sub", None),
        P(None, "slab", "sub", None),
        P("slab", "sub", None),
        P("slab", "sub", None),
    )
    out_specs = (P(None, None, "slab", "sub", None), P(None, None, "slab", "sub", None), P())
    return jax.shard_map(per_device, mesh=mesh, in_specs=in_specs, out_specs=out_specs, check_vma=False)
```

```python
import functools

import jax
import jax.numpy as jnp
from jax import lax
from jax.experimental import pallas as pl
from jax.experimental.pallas import tpu as pltpu
from jax.sharding import PartitionSpec as P

MESH_ID = pl.DeviceIdType.MESH
NX_T, NY_T, NZ_T = 4, 4, 8
ROWS = 24
HALF = 128


def lane_is(lane):
    return lax.broadcasted_iota(jnp.int32, (ROWS, HALF), 1) == lane


def get(ref, *lead):
    return ref[(*lead, slice(None), pl.ds(0, HALF))], ref[(*lead, slice(None), pl.ds(HALF, HALF))]


def put(ref, value, *lead):
    ref[(*lead, slice(None), pl.ds(0, HALF))] = value[0]
    ref[(*lead, slice(None), pl.ds(HALF, HALF))] = value[1]


def up_z(f, last):
    low, high = pltpu.roll(f[0], HALF - 1, 1), pltpu.roll(f[1], HALF - 1, 1)
    return jnp.where(last, high, low), jnp.where(last, 0.0, high)


def down_z(f, first):
    low, high = pltpu.roll(f[0], 1, 1), pltpu.roll(f[1], 1, 1)
    return jnp.where(first, 0.0, low), jnp.where(first, low, high)


def up_y(f):
    return tuple(pltpu.roll(h, ROWS - 1, 0) for h in f)


def down_y(f):
    return tuple(pltpu.roll(h, 1, 0) for h in f)


def krylov_kernel(
    start, wind, reac, mass,
    vec, w2, y1, q, gram_out,
    coef, work, t1, res, y0, part, slots_a, slots_b,
    send_sems, recv_sems, load_sems, told,
):
    slab, sub = lax.axis_index("slab"), lax.axis_index("sub")
    slabs = lax.axis_size("slab")
    other = 1 - sub
    z = lax.div(slab, NX_T * NY_T)
    has_left, has_right = slab > 0, slab < slabs - 1
    left, right = jnp.maximum(slab - 1, 0), jnp.minimum(slab + 1, slabs - 1)
    own_rows = pl.ds(pl.multiple_of(8 * sub, 8), 16)
    out_tile = pl.ds(8, 8)
    in_tile = pl.ds(pl.multiple_of(16 * sub, 8), 8)

    plane = 2 * NX_T * NY_T
    in_plane = lax.rem(2 * slab + sub, plane)

    def peers(stage):
        if stage == 0:
            for k in range(1, plane):
                at = lax.rem(in_plane + k, plane)
                yield (z * (NX_T * NY_T) + lax.div(at, 2), lax.rem(at, 2))
        else:
            for k in range(1, NZ_T):
                yield (slab + NX_T * NY_T * (lax.rem(z + k, NZ_T) - z), sub)

    loads = [
        pltpu.make_async_copy(start, vec.at[0, :, pl.ds(5, 6), own_rows], load_sems.at[0]),
        pltpu.make_async_copy(wind, coef.at[pl.ds(0, 3), pl.ds(2, 6), own_rows], load_sems.at[1]),
        pltpu.make_async_copy(reac, coef.at[3, pl.ds(2, 6), own_rows], load_sems.at[2]),
        pltpu.make_async_copy(mass, coef.at[4, pl.ds(2, 6), own_rows], load_sems.at[3]),
    ]
    for copy in loads:
        copy.start()

    x, y = lax.rem(slab, NX_T), lax.rem(lax.div(slab, NX_T), NY_T)

    def line_x():
        for k in range(1, 2 * NX_T):
            at = lax.rem(2 * x + sub + k, 2 * NX_T)
            yield (slab - x + lax.div(at, 2), lax.rem(at, 2))

    def line_y():
        for k in range(1, NY_T):
            yield (slab + NX_T * (lax.rem(y + k, NY_T) - y), sub)

    def near_z():
        for k in (1, NZ_T - 1):
            yield (slab + NX_T * NY_T * (lax.rem(z + k, NZ_T) - z), sub)

    def signal_all(sem, devices):
        for device in devices:
            pl.semaphore_signal(sem, inc=1, device_id=device, device_id_type=MESH_ID)
        return len(devices)

    def tell(turn):
        return signal_all(told.at[turn], [*line_y(), *near_z()] if turn == 0 else [*near_z()])

    def hear(turn, count):
        pl.semaphore_wait(told.at[turn], count)

    barrier = pltpu.get_barrier_semaphore()
    count = signal_all(barrier, [*line_x(), *line_y(), *near_z()])

    @pl.when(has_left)
    def _():
        pl.semaphore_signal(barrier, inc=1, device_id=(left, sub), device_id_type=MESH_ID)

    @pl.when(has_right)
    def _():
        pl.semaphore_signal(barrier, inc=1, device_id=(right, sub), device_id_type=MESH_ID)

    halo_rows = pl.ds(pl.multiple_of(16 * other, 8), 8)
    for k in range(3):
        for d in range(3):
            for plane_at in (3, 12):
                vec[k, d, plane_at, halo_rows] = jnp.zeros((8, 256), jnp.float32)
        for plane_at in (0, 11):
            q[k, plane_at, halo_rows] = jnp.zeros((8, 256), jnp.float32)

    def clear(planes, coef_planes, far_plane):
        for k in range(3):
            for f in range(4):
                vec[k, f, planes] = jnp.zeros((5, ROWS, 256), jnp.float32)
        for f in range(5):
            coef[f, coef_planes] = jnp.zeros((2, ROWS, 256), jnp.float32)
        for k in range(3):
            q[k, far_plane] = jnp.zeros((ROWS, 256), jnp.float32)

    @pl.when(jnp.logical_not(has_left))
    def _():
        clear(pl.ds(0, 5), pl.ds(0, 2), 0)

    @pl.when(jnp.logical_not(has_right))
    def _():
        clear(pl.ds(11, 5), pl.ds(8, 2), 11)

    pl.semaphore_wait(
        barrier, count + has_left.astype(jnp.int32) + has_right.astype(jnp.int32)
    )
    expected = tell(0)

    used = {"send": 0, "receive": 0}

    def remote(src, dst, device):
        copy = pltpu.make_async_remote_copy(
            src_ref=src, dst_ref=dst, send_sem=send_sems.at[used["send"]],
            recv_sem=recv_sems.at[used["receive"]], device_id=device, device_id_type=MESH_ID,
        )
        slot_of[id(copy)] = used["send"]
        keep.append(copy)
        used["send"] += 1
        used["receive"] += 1
        return copy

    slot_of, keep, sending = {}, [], {}

    def sent(slot):
        copy, condition = sending.pop(slot)
        if condition is None:
            copy.wait_send()
        else:
            pl.when(condition)(copy.wait_send)

    def go(copy, condition=None):
        slot = slot_of[id(copy)]
        if slot in sending:
            sent(slot)
        sending[slot] = (copy, condition)
        if condition is None:
            copy.start()
        else:
            pl.when(condition)(copy.start)

    def arrive(copy, condition=None):
        if condition is None:
            copy.wait_recv()
        else:
            pl.when(condition)(copy.wait_recv)

    class Halo:
        def __init__(self, src_low, src_high, src_tile, buffer, low, high, own):
            self.to_right = remote(src_high, buffer(low, own_rows), (right, sub))
            self.to_left = remote(src_low, buffer(high, own_rows), (left, sub))
            self.to_other = remote(src_tile, buffer(own, in_tile), (slab, other))
            self.low_on = remote(buffer(low, out_tile), buffer(low, in_tile), (slab, other))
            self.high_on = remote(buffer(high, out_tile), buffer(high, in_tile), (slab, other))

        def send(self):
            go(self.to_right, has_right)
            go(self.to_left, has_left)
            go(self.to_other)

        def forward(self):
            arrive(self.to_right, has_left)
            go(self.low_on, has_left)
            arrive(self.to_left, has_right)
            go(self.high_on, has_right)

        def finish(self):
            arrive(self.low_on, has_left)
            arrive(self.high_on, has_right)

    class FarHalo:
        def __init__(self, to_right, to_left):
            self.to_right, self.to_left = to_right, to_left

        def send(self):
            go(self.to_right, has_right)
            go(self.to_left, has_left)

        def finish(self):
            arrive(self.to_right, has_left)
            arrive(self.to_left, has_right)

    def vec_halo(k):
        def pressure(planes, rows):
            return vec.at[k, 3, planes, rows]

        def velocity(planes, rows):
            return vec.at[k, pl.ds(0, 3), planes, rows]

        p_src = (
            pressure(pl.ds(5, 4), own_rows), pressure(pl.ds(7, 4), own_rows),
            pressure(pl.ds(5, 6), out_tile),
        )
        near_src = (
            velocity(pl.ds(5, 1), own_rows), velocity(pl.ds(10, 1), own_rows),
            velocity(pl.ds(5, 6), out_tile),
        )
        p_halo = Halo(*p_src, pressure, pl.ds(1, 4), pl.ds(11, 4), pl.ds(5, 6))
        near = Halo(*near_src, velocity, pl.ds(4, 1), pl.ds(11, 1), pl.ds(5, 6))
        far = FarHalo(
            remote(velocity(pl.ds(9, 1), own_rows), velocity(pl.ds(3, 1), own_rows), (right, sub)),
            remote(velocity(pl.ds(6, 1), own_rows), velocity(pl.ds(12, 1), own_rows), (left, sub)),
        )
        schur_far = FarHalo(
            remote(q.at[k, 6, own_rows], q.at[k, 0, own_rows], (right, sub)),
            remote(q.at[k, 5, own_rows], q.at[k, 11, own_rows], (left, sub)),
        )
        return p_halo, near, far, schur_far

    def coef_halo(buffer):
        parts = (
            buffer(pl.ds(2, 2), own_rows), buffer(pl.ds(6, 2), own_rows), buffer(pl.ds(2, 6), out_tile),
        )
        return Halo(*parts, buffer, pl.ds(0, 2), pl.ds(8, 2), pl.ds(2, 6))

    halos = []
    for k in range(3):
        used["send"] = 0
        halos.append(vec_halo(k))
    coef_halo = coef_halo(lambda planes, rows: coef.at[:, planes, rows])
    loads[0].wait()
    halos[0][0].send()
    for copy in loads[1:]:
        copy.wait()
    coef_halo.send()
    for halo in halos[0][1:3]:
        halo.send()

    last, first = lane_is(HALF - 1), lane_is(0)
    row = lax.broadcasted_iota(jnp.int32, (ROWS, HALF), 0)
    live = row != (ROWS - 1) * other

    def inside(plane):
        at = slab * 6 + plane - 5
        return jnp.logical_and(at >= 0, at < slabs * 6)

    def prepare(j, _):
        ok = jnp.logical_and(live, inside(j + 3))
        for d in range(3):
            half = [0.5 * h for h in get(coef, d, j)]
            put(work, [h - 1.0 for h in half], d, j)
            put(work, [-1.0 - h for h in half], d + 3, j)
        diagonal = [6.0 + h for h in get(coef, 3, j)]
        put(work, diagonal, 6, j)
        put(work, [jnp.where(ok, 1.0 / h, 0.0) for h in diagonal], 7, j)
        put(work, [jnp.where(ok, -1.0 / h, 0.0) for h in get(coef, 4, j)], 8, j)
        return 0

    def six(fxm, f, fxp):
        total = [a + b for a, b in zip(fxm, fxp)]
        for g in (up_y(f), down_y(f), up_z(f, last), down_z(f, first)):
            total = [a + b for a, b in zip(total, g)]
        return total

    def weights(j):
        return [get(work, i, j) for i in range(7)]

    def transport(fxm, f, fxp, w):
        total = [a * b for a, b in zip(w[6], f)]
        terms = ((0, fxp), (3, fxm), (1, up_y(f)), (4, down_y(f)), (2, up_z(f, last)), (5, down_z(f, first)))
        for i, g in terms:
            total = [t + a * b for t, a, b in zip(total, w[i], g)]
        return total

    def half_difference(a, b):
        return [0.5 * (m - n) for m, n in zip(a, b)]

    def gradient(fxm, f, fxp):
        return (
            half_difference(fxp, fxm),
            half_difference(up_y(f), down_y(f)),
            half_difference(up_z(f, last), down_z(f, first)),
        )

    def loop(count, body, plane, unroll):
        def step(i, _):
            body(plane(i))
            return 0

        lax.fori_loop(0, count, step, 0, unroll=unroll)

    def guess(k, j):
        scale = jnp.where(jnp.logical_and(live, inside(j)), 1.0 / 49.0, 0.0)
        f = [jnp.where(live, h, 0.0) for h in get(vec, k, 3, j)]
        total = six(get(vec, k, 3, j - 1), f, get(vec, k, 3, j + 1))
        put(t1, [scale * (7.0 * a + b) for a, b in zip(f, total)], j)

    def schur(k, j):
        value = transport(get(t1, j - 1), get(t1, j), get(t1, j + 1), weights(j - 3))
        put(q, [a * b for a, b in zip(value, get(work, 8, j - 3))], k, j - 2)

    def pressure_inner(k):
        loop(4, functools.partial(guess, k), lambda i: i + 6, 4)
        loop(2, functools.partial(schur, k), lambda i: i + 7, 2)

    def pressure_outer(k):
        loop(8, functools.partial(guess, k), lambda i: i + 2 + 4 * lax.div(i, 4), 4)
        loop(8, functools.partial(schur, k), lambda i: i + 3 + 2 * lax.div(i, 4), 4)

    def first_guess(k, j):
        slope = gradient(get(q, k, j), get(q, k, j + 1), get(q, k, j + 2))
        inverse = get(work, 7, j)
        for d in range(3):
            r = [a - b for a, b in zip(get(vec, k, d, j + 3), slope[d])]
            put(res, r, d, j)
            put(y0, [a * b for a, b in zip(r, inverse)], d, j)

    def second_guess(k, j):
        w = weights(j + 1)
        inverse = get(work, 7, j + 1)
        for d in range(3):
            f = get(y0, d, j + 1)
            value = transport(get(y0, d, j), f, get(y0, d, j + 2), w)
            r = get(res, d, j + 1)
            put(y1, [a + (b - c) * i for a, b, c, i in zip(f, r, value, inverse)], k, d, j)

    def velocity_inner(k):
        loop(8, functools.partial(first_guess, k), lambda i: i + 1, 4)
        loop(6, functools.partial(second_guess, k), lambda i: i + 1, 3)

    def velocity_outer(k, target, after_pressure=lambda: None):
        loop(2, functools.partial(first_guess, k), lambda i: 9 * i, 2)
        loop(2, functools.partial(second_guess, k), lambda i: 7 * i, 2)

        def store(f, j, value):
            for i, h in enumerate(value):
                mine = jnp.where(sub == 0, h[0:16], h[8:24])
                target(f, j)[own_rows if k < 2 else slice(None), pl.ds(HALF * i, HALF)] = mine

        def image_pressure(j, _):
            pc = get(q, k, j + 3)
            total = six(get(q, k, j + 2), pc, get(q, k, j + 4))
            yc, zc = get(y1, k, 1, j + 1), get(y1, k, 2, j + 1)
            ends = (
                (get(y1, k, 0, j + 2), get(y1, k, 0, j)), (up_y(yc), down_y(yc)),
                (up_z(zc, last), down_z(zc, first)),
            )
            flow = [a - b for a, b in zip(*ends[0])]
            for high, low in ends[1:]:
                flow = [t + (a - b) for t, a, b in zip(flow, high, low)]
            store(3, j, [-0.5 * (a + (6.0 * b - c)) for a, b, c in zip(flow, pc, total)])
            return 0

        lax.fori_loop(0, 6, image_pressure, 0, unroll=6)
        after_pressure()

        def image_velocity(j, _):
            w = weights(j + 2)
            slope = gradient(get(q, k, j + 2), get(q, k, j + 3), get(q, k, j + 4))
            for d in range(3):
                value = transport(get(y1, k, d, j), get(y1, k, d, j + 1), get(y1, k, d, j + 2), w)
                store(d, j, [a + b for a, b in zip(value, slope[d])])
            return 0

        lax.fori_loop(0, 6, image_velocity, 0, unroll=3)

    lane8 = lax.broadcasted_iota(jnp.int32, (8, HALF), 1)

    def vectors(i, f, j):
        return vec[i, f, 5 + j, own_rows, :] if i < 3 else w2[f, j]

    def dots(new, olds):
        def step(j, accs):
            accs = list(accs)
            for f in range(4):
                b = vectors(new, f, j)
                for i, old in enumerate(olds):
                    prod = b * (b if old == new else vectors(old, f, j))
                    accs[i] = accs[i] + (
                        (prod[0:8, 0:HALF] + prod[0:8, HALF:]) + (prod[8:16, 0:HALF] + prod[8:16, HALF:])
                    )
            return tuple(accs)

        zero = jnp.zeros((8, HALF), jnp.float32)
        return lax.fori_loop(0, 6, step, tuple(zero for _ in olds), unroll=2)

    def pack(total, sums, at):
        for i, s in enumerate(sums):
            total = jnp.where(lane8 == at + i, jnp.sum(s, axis=1, keepdims=True), total)
        return total

    def application(k, target, after_pressure=lambda: None):
        p_halo, near, far, schur_far = halos[k]
        arrive(p_halo.to_other)
        if k == 0:
            arrive(coef_halo.to_other)
            lax.fori_loop(2, 8, prepare, 0, unroll=2)
        pressure_inner(k)
        schur_far.send()
        p_halo.forward()
        if k == 0:
            coef_halo.forward()
        p_halo.finish()
        near.forward()
        if k == 0:
            coef_halo.finish()
            for planes in (0, 8):
                lax.fori_loop(planes, planes + 2, prepare, 0, unroll=2)
        pressure_outer(k)
        arrive(near.to_other)
        near.finish()
        velocity_inner(k)
        far.finish()
        schur_far.finish()
        velocity_outer(k, target, after_pressure)

    application(0, lambda f, j: vec.at[1, f, 5 + j], halos[1][0].send)
    gram = jnp.zeros((8, HALF), jnp.float32)
    at = 0
    for k in range(2):
        halos[k + 1][1].send()
        halos[k + 1][2].send()
        hear(k, expected)
        expected = tell(k + 1)
        if k == 0:
            gram = pack(gram, dots(0, (0,)), 0)
            at = 1
        olds = tuple(range(k + 2))
        gram = pack(gram, dots(k + 1, olds), at)
        at += len(olds)
        if k == 0:
            application(1, lambda f, j: vec.at[2, f, 5 + j], halos[2][0].send)
        else:
            application(2, lambda f, j: w2.at[f, j])
    hear(2, expected)
    gram = pack(gram, dots(3, (0, 1, 2, 3)), at)

    row_sum = jnp.sum(gram, axis=0, keepdims=True)
    for stage, (place, slots) in enumerate(((in_plane, slots_a), (z, slots_b))):
        part[stage] = row_sum
        slots[place] = row_sum
        send_sem, recv_sem = send_sems.at[used["send"] + stage], recv_sems.at[used["receive"] + stage]

        def message(src, dst, device):
            return pltpu.make_async_remote_copy(
                src_ref=src, dst_ref=dst, send_sem=send_sem, recv_sem=recv_sem,
                device_id=device, device_id_type=MESH_ID,
            )

        for peer in peers(stage):
            message(part.at[stage], slots.at[place], peer).start()
        rest = slots.at[pl.ds(0, slots.shape[0] - 1)]
        all_of_them = message(rest, rest, (slab, other))
        all_of_them.wait_recv()
        all_of_them.wait_send()
        row_sum = jnp.sum(slots[...], axis=0)
    gram_out[...] = row_sum

    for slot in list(sending):
        sent(slot)


def combine_kernel(vec, w2, y1, q, gram, basis, search, hess, b_out, s_out, out_sems):
    own_rows = pl.ds(pl.multiple_of(8 * lax.axis_index("sub"), 8), 16)

    total = gram[...]
    lane = lax.broadcasted_iota(jnp.int32, (1, HALF), 1)

    def entry(i):
        return jnp.broadcast_to(jnp.sum(jnp.where(lane == i, total, 0.0), axis=1, keepdims=True), (1, HALF))

    low = {}
    inverse = {}
    for i in range(4):
        for j in range(i + 1):
            value = entry(i * (i + 1) // 2 + j)
            for m in range(j):
                value = value - low[i, m] * low[j, m]
            if i == j:
                low[i, i] = jnp.sqrt(value)
                inverse[i] = 1.0 / low[i, i]
            else:
                low[i, j] = value * inverse[j]
    h = {}
    for j in range(3):
        for i in range(j + 2):
            value = low[j + 1, i]
            for m in range(j):
                if i <= m + 1:
                    value = value - low[j, m] * h[i, m]
            h[i, j] = value * inverse[j]
    at_row = lax.broadcasted_iota(jnp.int32, (4, HALF), 0)
    at_col = lax.broadcasted_iota(jnp.int32, (4, HALF), 1)
    table = jnp.zeros((4, HALF), jnp.float32)
    for (i, j), value in h.items():
        table = jnp.where(jnp.logical_and(at_row == i, at_col == j), value, table)
    hess[...] = table[:, 0:3]

    def wide(v):
        return jnp.concatenate([v, v], axis=1)

    scale = {key: wide(v) for key, v in low.items()}
    inv = {key: wide(v) for key, v in inverse.items()}

    writes = []
    for f in range(4):

        def body(j, _):
            raw = [vec[i, f, 5 + j, own_rows, :] for i in range(3)] + [w2[f, j]]
            found = [y1[i, f, 1 + j, own_rows, :] if f < 3 else q[i, 3 + j, own_rows, :] for i in range(3)]
            for values, dst in ((raw, b_out), (found, s_out)):
                done = []
                for i, value in enumerate(values):
                    for m in range(i):
                        value = value - scale[i, m] * done[m]
                    value = value * inv[i]
                    dst[i, f, j] = value
                    done.append(value)
            return 0

        lax.fori_loop(0, 6, body, 0, unroll=3)
        for i, (src, dst) in enumerate(((b_out, basis), (s_out, search))):
            copy = pltpu.make_async_copy(src.at[:, f], dst.at[:, f], out_sems.at[f, i])
            copy.start()
            writes.append(copy)
    for copy in writes:
        copy.wait()


def per_device(start, wind, reaction, mass):
    f32 = jnp.float32
    hbm_spec = pl.BlockSpec(memory_space=pltpu.HBM)
    vmem_spec = pl.BlockSpec(memory_space=pltpu.VMEM)
    n_send, n_receive = 14 + 5 + 2, 14 * 3 + 5 + 2
    kept = (
        jax.ShapeDtypeStruct((3, 4, 16, ROWS, 256), f32),
        jax.ShapeDtypeStruct((4, 6, 16, 256), f32),
        jax.ShapeDtypeStruct((3, 3, 8, ROWS, 256), f32),
        jax.ShapeDtypeStruct((3, 12, ROWS, 256), f32),
        jax.ShapeDtypeStruct((1, HALF), f32),
    )
    arrays = [pltpu.with_memory_space_constraint(a, pltpu.HBM) for a in (start, wind, reaction, mass)]
    outs = pl.pallas_call(
        krylov_kernel,
        out_shape=kept,
        in_specs=[hbm_spec] * 4,
        out_specs=(vmem_spec,) * 5,
        scratch_shapes=[
            pltpu.VMEM((5, 10, ROWS, 256), f32),
            pltpu.VMEM((9, 10, ROWS, 256), f32),
            pltpu.VMEM((16, ROWS, 256), f32),
            pltpu.VMEM((3, 10, ROWS, 256), f32),
            pltpu.VMEM((3, 10, ROWS, 256), f32),
            pltpu.VMEM((2, 1, HALF), f32),
            pltpu.VMEM((2 * NX_T * NY_T, 1, HALF), f32),
            pltpu.VMEM((NZ_T, 1, HALF), f32),
            pltpu.SemaphoreType.DMA((n_send,)),
            pltpu.SemaphoreType.DMA((n_receive,)),
            pltpu.SemaphoreType.DMA((4,)),
            pltpu.SemaphoreType.REGULAR((3,)),
        ],
        compiler_params=pltpu.CompilerParams(
            collective_id=0, has_side_effects=True, vmem_limit_bytes=24 * 2**20
        ),
        name="krylov",
    )(*arrays)
    return tuple(pl.pallas_call(
        combine_kernel,
        out_shape=(
            jax.ShapeDtypeStruct((4, 4, 6, 16, 256), f32),
            jax.ShapeDtypeStruct((3, 4, 6, 16, 256), f32),
            jax.ShapeDtypeStruct((4, 3), f32),
        ),
        in_specs=[vmem_spec] * 5,
        out_specs=(hbm_spec, hbm_spec, vmem_spec),
        scratch_shapes=[
            pltpu.VMEM((4, 4, 6, 16, 256), f32),
            pltpu.VMEM((3, 4, 6, 16, 256), f32),
            pltpu.SemaphoreType.DMA((4, 2)),
        ],
        compiler_params=pltpu.CompilerParams(vmem_limit_bytes=24 * 2**20),
        name="combine",
    )(*outs))


def solution(mesh):
    in_specs = (
        P(None, "slab", "sub", None),
        P(None, "slab", "sub", None),
        P("slab", "sub", None),
        P("slab", "sub", None),
    )
    out_specs = (P(None, None, "slab", "sub", None), P(None, None, "slab", "sub", None), P())
    return jax.shard_map(per_device, mesh=mesh, in_specs=in_specs, out_specs=out_specs, check_vma=False)
```

```python
import functools

import jax
import jax.numpy as jnp
from jax import lax
from jax.experimental import pallas as pl
from jax.experimental.pallas import tpu as pltpu
from jax.sharding import PartitionSpec as P

MESH_ID = pl.DeviceIdType.MESH
NX_T, NY_T, NZ_T = 4, 4, 8
ROWS = 24
HALF = 128


def lane_is(lane):
    return lax.broadcasted_iota(jnp.int32, (ROWS, HALF), 1) == lane


def get(ref, *lead):
    return ref[(*lead, slice(None), pl.ds(0, HALF))], ref[(*lead, slice(None), pl.ds(HALF, HALF))]


def put(ref, value, *lead):
    ref[(*lead, slice(None), pl.ds(0, HALF))] = value[0]
    ref[(*lead, slice(None), pl.ds(HALF, HALF))] = value[1]


def up_z(f, last):
    low, high = pltpu.roll(f[0], HALF - 1, 1), pltpu.roll(f[1], HALF - 1, 1)
    return jnp.where(last, high, low), jnp.where(last, 0.0, high)


def down_z(f, first):
    low, high = pltpu.roll(f[0], 1, 1), pltpu.roll(f[1], 1, 1)
    return jnp.where(first, 0.0, low), jnp.where(first, low, high)


def up_y(f):
    return tuple(pltpu.roll(h, ROWS - 1, 0) for h in f)


def down_y(f):
    return tuple(pltpu.roll(h, 1, 0) for h in f)


def krylov_kernel(
    start, wind, reac, mass,
    vec, w2, y1, q, gram_out,
    coef, work, t1, res, y0, part, slots_a, slots_b,
    send_sems, recv_sems, load_sems, told,
):
    slab, sub = lax.axis_index("slab"), lax.axis_index("sub")
    slabs = lax.axis_size("slab")
    other = 1 - sub
    z = lax.div(slab, NX_T * NY_T)
    has_left, has_right = slab > 0, slab < slabs - 1
    left, right = jnp.maximum(slab - 1, 0), jnp.minimum(slab + 1, slabs - 1)
    own_rows = pl.ds(pl.multiple_of(8 * sub, 8), 16)
    out_tile = pl.ds(8, 8)
    in_tile = pl.ds(pl.multiple_of(16 * sub, 8), 8)

    plane = 2 * NX_T * NY_T
    in_plane = lax.rem(2 * slab + sub, plane)

    def peers(stage):
        if stage == 0:
            for k in range(1, plane):
                at = lax.rem(in_plane + k, plane)
                yield (z * (NX_T * NY_T) + lax.div(at, 2), lax.rem(at, 2))
        else:
            for k in range(1, NZ_T):
                yield (slab + NX_T * NY_T * (lax.rem(z + k, NZ_T) - z), sub)

    loads = [
        pltpu.make_async_copy(start, vec.at[0, :, pl.ds(5, 6), own_rows], load_sems.at[0]),
        pltpu.make_async_copy(wind, coef.at[pl.ds(0, 3), pl.ds(2, 6), own_rows], load_sems.at[1]),
        pltpu.make_async_copy(reac, coef.at[3, pl.ds(2, 6), own_rows], load_sems.at[2]),
        pltpu.make_async_copy(mass, coef.at[4, pl.ds(2, 6), own_rows], load_sems.at[3]),
    ]
    for copy in loads:
        copy.start()

    x, y = lax.rem(slab, NX_T), lax.rem(lax.div(slab, NX_T), NY_T)

    def line_x():
        for k in range(1, 2 * NX_T):
            at = lax.rem(2 * x + sub + k, 2 * NX_T)
            yield (slab - x + lax.div(at, 2), lax.rem(at, 2))

    def line_y():
        for k in range(1, NY_T):
            yield (slab + NX_T * (lax.rem(y + k, NY_T) - y), sub)

    def near_z():
        for k in (1, NZ_T - 1):
            yield (slab + NX_T * NY_T * (lax.rem(z + k, NZ_T) - z), sub)

    def signal_all(sem, devices):
        for device in devices:
            pl.semaphore_signal(sem, inc=1, device_id=device, device_id_type=MESH_ID)
        return len(devices)

    def tell(turn):
        return signal_all(told.at[turn], [*line_y(), *near_z()] if turn == 0 else [*near_z()])

    def hear(turn, count):
        pl.semaphore_wait(told.at[turn], count)

    barrier = pltpu.get_barrier_semaphore()
    count = signal_all(barrier, [*line_x(), *line_y(), *near_z()])

    @pl.when(has_left)
    def _():
        pl.semaphore_signal(barrier, inc=1, device_id=(left, sub), device_id_type=MESH_ID)

    @pl.when(has_right)
    def _():
        pl.semaphore_signal(barrier, inc=1, device_id=(right, sub), device_id_type=MESH_ID)

    halo_rows = pl.ds(pl.multiple_of(16 * other, 8), 8)
    for k in range(3):
        for d in range(3):
            for plane_at in (3, 12):
                vec[k, d, plane_at, halo_rows] = jnp.zeros((8, 256), jnp.float32)
        for plane_at in (0, 11):
            q[k, plane_at, halo_rows] = jnp.zeros((8, 256), jnp.float32)

    def clear(planes, coef_planes, far_plane):
        for k in range(3):
            for f in range(4):
                vec[k, f, planes] = jnp.zeros((5, ROWS, 256), jnp.float32)
        for f in range(5):
            coef[f, coef_planes] = jnp.zeros((2, ROWS, 256), jnp.float32)
        for k in range(3):
            q[k, far_plane] = jnp.zeros((ROWS, 256), jnp.float32)

    @pl.when(jnp.logical_not(has_left))
    def _():
        clear(pl.ds(0, 5), pl.ds(0, 2), 0)

    @pl.when(jnp.logical_not(has_right))
    def _():
        clear(pl.ds(11, 5), pl.ds(8, 2), 11)

    pl.semaphore_wait(
        barrier, count + has_left.astype(jnp.int32) + has_right.astype(jnp.int32)
    )
    expected = [tell(0)]

    used = {"send": 0, "receive": 0}

    def remote(src, dst, device):
        copy = pltpu.make_async_remote_copy(
            src_ref=src, dst_ref=dst, send_sem=send_sems.at[used["send"]],
            recv_sem=recv_sems.at[used["receive"]], device_id=device, device_id_type=MESH_ID,
        )
        slot_of[id(copy)] = used["send"]
        keep.append(copy)
        used["send"] += 1
        used["receive"] += 1
        return copy

    slot_of, keep, sending = {}, [], {}

    def sent(slot):
        copy, condition = sending.pop(slot)
        if condition is None:
            copy.wait_send()
        else:
            pl.when(condition)(copy.wait_send)

    def go(copy, condition=None):
        slot = slot_of[id(copy)]
        if slot in sending:
            sent(slot)
        sending[slot] = (copy, condition)
        if condition is None:
            copy.start()
        else:
            pl.when(condition)(copy.start)

    def arrive(copy, condition=None):
        if condition is None:
            copy.wait_recv()
        else:
            pl.when(condition)(copy.wait_recv)

    class Halo:
        def __init__(self, src_low, src_high, src_tile, buffer, low, high, own):
            self.to_right = remote(src_high, buffer(low, own_rows), (right, sub))
            self.to_left = remote(src_low, buffer(high, own_rows), (left, sub))
            self.to_other = remote(src_tile, buffer(own, in_tile), (slab, other))
            self.low_on = remote(buffer(low, out_tile), buffer(low, in_tile), (slab, other))
            self.high_on = remote(buffer(high, out_tile), buffer(high, in_tile), (slab, other))

        def send(self):
            go(self.to_right, has_right)
            go(self.to_left, has_left)
            go(self.to_other)

        def forward(self):
            arrive(self.to_right, has_left)
            go(self.low_on, has_left)
            arrive(self.to_left, has_right)
            go(self.high_on, has_right)

        def finish(self):
            arrive(self.low_on, has_left)
            arrive(self.high_on, has_right)

    class FarHalo:
        def __init__(self, to_right, to_left):
            self.to_right, self.to_left = to_right, to_left

        def send(self):
            go(self.to_right, has_right)
            go(self.to_left, has_left)

        def finish(self):
            arrive(self.to_right, has_left)
            arrive(self.to_left, has_right)

    def vec_halo(k):
        def pressure(planes, rows):
            return vec.at[k, 3, planes, rows]

        def velocity(planes, rows):
            return vec.at[k, pl.ds(0, 3), planes, rows]

        p_src = (
            pressure(pl.ds(5, 4), own_rows), pressure(pl.ds(7, 4), own_rows),
            pressure(pl.ds(5, 6), out_tile),
        )
        near_src = (
            velocity(pl.ds(5, 1), own_rows), velocity(pl.ds(10, 1), own_rows),
            velocity(pl.ds(5, 6), out_tile),
        )
        p_halo = Halo(*p_src, pressure, pl.ds(1, 4), pl.ds(11, 4), pl.ds(5, 6))
        near = Halo(*near_src, velocity, pl.ds(4, 1), pl.ds(11, 1), pl.ds(5, 6))
        far = FarHalo(
            remote(velocity(pl.ds(9, 1), own_rows), velocity(pl.ds(3, 1), own_rows), (right, sub)),
            remote(velocity(pl.ds(6, 1), own_rows), velocity(pl.ds(12, 1), own_rows), (left, sub)),
        )
        schur_far = FarHalo(
            remote(q.at[k, 6, own_rows], q.at[k, 0, own_rows], (right, sub)),
            remote(q.at[k, 5, own_rows], q.at[k, 11, own_rows], (left, sub)),
        )
        return p_halo, near, far, schur_far

    def coef_halo(buffer):
        parts = (
            buffer(pl.ds(2, 2), own_rows), buffer(pl.ds(6, 2), own_rows), buffer(pl.ds(2, 6), out_tile),
        )
        return Halo(*parts, buffer, pl.ds(0, 2), pl.ds(8, 2), pl.ds(2, 6))

    halos = []
    for k in range(3):
        used["send"] = 0
        halos.append(vec_halo(k))
    coef_halo = coef_halo(lambda planes, rows: coef.at[:, planes, rows])
    loads[0].wait()
    halos[0][0].send()
    for copy in loads[1:]:
        copy.wait()
    coef_halo.send()
    for halo in halos[0][1:3]:
        halo.send()

    last, first = lane_is(HALF - 1), lane_is(0)
    row = lax.broadcasted_iota(jnp.int32, (ROWS, HALF), 0)
    live = row != (ROWS - 1) * other

    def inside(plane):
        at = slab * 6 + plane - 5
        return jnp.logical_and(at >= 0, at < slabs * 6)

    def prepare(j, _):
        ok = jnp.logical_and(live, inside(j + 3))
        for d in range(3):
            half = [0.5 * h for h in get(coef, d, j)]
            put(work, [h - 1.0 for h in half], d, j)
            put(work, [-1.0 - h for h in half], d + 3, j)
        diagonal = [6.0 + h for h in get(coef, 3, j)]
        put(work, diagonal, 6, j)
        put(work, [jnp.where(ok, 1.0 / h, 0.0) for h in diagonal], 7, j)
        put(work, [jnp.where(ok, -1.0 / h, 0.0) for h in get(coef, 4, j)], 8, j)
        return 0

    def six(fxm, f, fxp):
        total = [a + b for a, b in zip(fxm, fxp)]
        for g in (up_y(f), down_y(f), up_z(f, last), down_z(f, first)):
            total = [a + b for a, b in zip(total, g)]
        return total

    def weights(j):
        return [get(work, i, j) for i in range(7)]

    def transport(fxm, f, fxp, w):
        total = [a * b for a, b in zip(w[6], f)]
        terms = ((0, fxp), (3, fxm), (1, up_y(f)), (4, down_y(f)), (2, up_z(f, last)), (5, down_z(f, first)))
        for i, g in terms:
            total = [t + a * b for t, a, b in zip(total, w[i], g)]
        return total

    def half_difference(a, b):
        return [0.5 * (m - n) for m, n in zip(a, b)]

    def gradient(fxm, f, fxp):
        return (
            half_difference(fxp, fxm),
            half_difference(up_y(f), down_y(f)),
            half_difference(up_z(f, last), down_z(f, first)),
        )

    def loop(count, body, plane, unroll):
        def step(i, _):
            body(plane(i))
            return 0

        lax.fori_loop(0, count, step, 0, unroll=unroll)

    def guess(k, j):
        scale = jnp.where(jnp.logical_and(live, inside(j)), 1.0 / 49.0, 0.0)
        f = [jnp.where(live, h, 0.0) for h in get(vec, k, 3, j)]
        total = six(get(vec, k, 3, j - 1), f, get(vec, k, 3, j + 1))
        put(t1, [scale * (7.0 * a + b) for a, b in zip(f, total)], j)

    def schur(k, j):
        value = transport(get(t1, j - 1), get(t1, j), get(t1, j + 1), weights(j - 3))
        put(q, [a * b for a, b in zip(value, get(work, 8, j - 3))], k, j - 2)

    def pressure_inner(k):
        loop(4, functools.partial(guess, k), lambda i: i + 6, 4)
        loop(2, functools.partial(schur, k), lambda i: i + 7, 2)

    def pressure_outer(k):
        loop(8, functools.partial(guess, k), lambda i: i + 2 + 4 * lax.div(i, 4), 4)
        loop(8, functools.partial(schur, k), lambda i: i + 3 + 2 * lax.div(i, 4), 4)

    def first_guess(k, j):
        slope = gradient(get(q, k, j), get(q, k, j + 1), get(q, k, j + 2))
        inverse = get(work, 7, j)
        for d in range(3):
            r = [a - b for a, b in zip(get(vec, k, d, j + 3), slope[d])]
            put(res, r, d, j)
            put(y0, [a * b for a, b in zip(r, inverse)], d, j)

    def second_guess(k, j):
        w = weights(j + 1)
        inverse = get(work, 7, j + 1)
        for d in range(3):
            f = get(y0, d, j + 1)
            value = transport(get(y0, d, j), f, get(y0, d, j + 2), w)
            r = get(res, d, j + 1)
            put(y1, [a + (b - c) * i for a, b, c, i in zip(f, r, value, inverse)], k, d, j)

    def velocity_inner(k):
        loop(8, functools.partial(first_guess, k), lambda i: i + 1, 4)
        loop(6, functools.partial(second_guess, k), lambda i: i + 1, 3)

    def velocity_outer(k, target, after_pressure=lambda: None):
        loop(2, functools.partial(first_guess, k), lambda i: 9 * i, 2)
        loop(2, functools.partial(second_guess, k), lambda i: 7 * i, 2)

        def store(f, j, value):
            for i, h in enumerate(value):
                mine = jnp.where(sub == 0, h[0:16], h[8:24])
                target(f, j)[own_rows if k < 2 else slice(None), pl.ds(HALF * i, HALF)] = mine

        def image_pressure(j, _):
            pc = get(q, k, j + 3)
            total = six(get(q, k, j + 2), pc, get(q, k, j + 4))
            yc, zc = get(y1, k, 1, j + 1), get(y1, k, 2, j + 1)
            ends = (
                (get(y1, k, 0, j + 2), get(y1, k, 0, j)), (up_y(yc), down_y(yc)),
                (up_z(zc, last), down_z(zc, first)),
            )
            flow = [a - b for a, b in zip(*ends[0])]
            for high, low in ends[1:]:
                flow = [t + (a - b) for t, a, b in zip(flow, high, low)]
            store(3, j, [-0.5 * (a + (6.0 * b - c)) for a, b, c in zip(flow, pc, total)])
            return 0

        lax.fori_loop(0, 6, image_pressure, 0, unroll=6)
        after_pressure()

        def image_velocity(j, _):
            w = weights(j + 2)
            slope = gradient(get(q, k, j + 2), get(q, k, j + 3), get(q, k, j + 4))
            for d in range(3):
                value = transport(get(y1, k, d, j), get(y1, k, d, j + 1), get(y1, k, d, j + 2), w)
                store(d, j, [a + b for a, b in zip(value, slope[d])])
            return 0

        lax.fori_loop(0, 6, image_velocity, 0, unroll=3)

    lane8 = lax.broadcasted_iota(jnp.int32, (8, HALF), 1)

    def vectors(i, f, j):
        return vec[i, f, 5 + j, own_rows, :] if i < 3 else w2[f, j]

    def dots(pairs, shift=None):
        needed = sorted({i for pair in pairs for i in pair})

        def step(j, accs):
            accs = list(accs)
            for f in range(4):
                raw = {}
                for i in needed:
                    for at in (i,) if shift is None or i == 0 else (i - 1, i):
                        if at not in raw:
                            raw[at] = vectors(at, f, j)
                y = {i: raw[i] if shift is None or i == 0 else raw[i] - shift * raw[i - 1] for i in needed}
                for n, (i, k) in enumerate(pairs):
                    prod = y[i] * y[k]
                    accs[n] = accs[n] + (
                        (prod[0:8, 0:HALF] + prod[0:8, HALF:]) + (prod[8:16, 0:HALF] + prod[8:16, HALF:])
                    )
            return tuple(accs)

        zero = jnp.zeros((8, HALF), jnp.float32)
        return lax.fori_loop(0, 6, step, tuple(zero for _ in pairs), unroll=2)

    def pack(total, sums, at):
        for i, s in enumerate(sums):
            total = jnp.where(lane8 == at + i, jnp.sum(s, axis=1, keepdims=True), total)
        return total

    class Reduction:
        def __init__(self, n):
            self.n = n

        def message(self, stage, src, dst, device):
            at = 2 * self.n + stage
            return pltpu.make_async_remote_copy(
                src_ref=src, dst_ref=dst, send_sem=send_sems.at[used["send"] + at],
                recv_sem=recv_sems.at[used["receive"] + at], device_id=device, device_id_type=MESH_ID,
            )

        def send(self, stage, row):
            place, slots = ((in_plane, slots_a), (z, slots_b))[stage]
            part[self.n, stage] = row
            slots[self.n, place] = row
            for peer in peers(stage):
                self.message(stage, part.at[self.n, stage], slots.at[self.n, place], peer).start()

        def finish(self, stage):
            slots = (slots_a, slots_b)[stage]
            rest = slots.at[self.n, pl.ds(0, slots.shape[1] - 1)]
            everything = self.message(stage, rest, rest, (slab, other))
            everything.wait_recv()
            everything.wait_send()
            return jnp.sum(slots[self.n], axis=0)

        def whole(self, row):
            for stage in range(2):
                self.send(stage, row)
                row = self.finish(stage)
            return row

    reductions = [Reduction(0), Reduction(1)]

    def application(k, target, waiting, waited, after_pressure=lambda: None):
        p_halo, near, far, schur_far = halos[k]
        arrive(p_halo.to_other)
        if k == 0:
            arrive(coef_halo.to_other)
            lax.fori_loop(2, 8, prepare, 0, unroll=2)
        pressure_inner(k)
        schur_far.send()
        kept = waiting()
        p_halo.forward()
        if k == 0:
            coef_halo.forward()
        p_halo.finish()
        near.forward()
        waited()
        if k == 0:
            coef_halo.finish()
            for planes in (0, 8):
                lax.fori_loop(planes, planes + 2, prepare, 0, unroll=2)
        pressure_outer(k)
        arrive(near.to_other)
        near.finish()
        velocity_inner(k)
        far.finish()
        schur_far.finish()
        velocity_outer(k, target, after_pressure)
        return kept

    def pass_on(turn):
        hear(turn, expected[turn])
        expected.append(tell(turn + 1))

    def shift_known():
        row = reductions[0].finish(1)

        def entry(i):
            return jnp.sum(jnp.where(lane_row == i, row, 0.0), axis=1, keepdims=True)

        c = jnp.broadcast_to(entry(1) / entry(0), (1, HALF))
        c = jnp.concatenate([c, c], axis=1)
        pairs = ((0, 0), (1, 0), (1, 1), (2, 0), (2, 1), (2, 2))
        return c, pack(jnp.zeros((8, HALF), jnp.float32), dots(pairs, c), 0)

    def nothing():
        return None

    lane_row = lax.broadcasted_iota(jnp.int32, (1, HALF), 1)
    application(
        0, lambda f, j: vec.at[1, f, 5 + j], lambda: pass_on(0), lambda: pass_on(1), halos[1][0].send
    )
    halos[1][1].send()
    halos[1][2].send()
    hear(2, expected[2])
    opening = pack(jnp.zeros((8, HALF), jnp.float32), dots(((0, 0), (1, 0))), 0)
    reductions[0].send(0, jnp.sum(opening, axis=0, keepdims=True))
    application(
        1, lambda f, j: vec.at[2, f, 5 + j], nothing,
        lambda: reductions[0].send(1, reductions[0].finish(0)), halos[2][0].send,
    )
    halos[2][1].send()
    halos[2][2].send()
    shift, gram = application(2, lambda f, j: w2.at[f, j], shift_known, nothing)
    gram = pack(gram, dots(((3, 0), (3, 1), (3, 2), (3, 3)), shift), 6)

    total = reductions[1].whole(jnp.sum(gram, axis=0, keepdims=True))
    lane1 = lax.broadcasted_iota(jnp.int32, (1, HALF), 1)
    gram_out[...] = jnp.where(lane1 == 10, shift[:, 0:HALF], total)

    for slot in list(sending):
        sent(slot)


def combine_kernel(vec, w2, y1, q, gram, basis, search, hess, b_out, s_out, h_out, out_sems):
    own_rows = pl.ds(pl.multiple_of(8 * lax.axis_index("sub"), 8), 16)

    total = gram[...]
    lane = lax.broadcasted_iota(jnp.int32, (1, HALF), 1)

    def entry(i):
        return jnp.broadcast_to(jnp.sum(jnp.where(lane == i, total, 0.0), axis=1, keepdims=True), (1, HALF))

    low = {}
    inverse = {}
    for i in range(4):
        for j in range(i + 1):
            value = entry(i * (i + 1) // 2 + j)
            for m in range(j):
                value = value - low[i, m] * low[j, m]
            if i == j:
                low[i, i] = jnp.sqrt(value)
                inverse[i] = 1.0 / low[i, i]
            else:
                low[i, j] = value * inverse[j]
    shift = entry(10)
    h = {}
    for j in range(3):
        for i in range(j + 2):
            value = low[j + 1, i]
            if j == 0 and i == 0:
                value = value + shift * low[0, 0]
            for m in range(j):
                if i <= m + 1:
                    value = value - low[j, m] * h[i, m]
            h[i, j] = value * inverse[j]
    at_row = lax.broadcasted_iota(jnp.int32, (4, HALF), 0)
    at_col = lax.broadcasted_iota(jnp.int32, (4, HALF), 1)
    table = jnp.zeros((4, HALF), jnp.float32)
    for (i, j), value in h.items():
        table = jnp.where(jnp.logical_and(at_row == i, at_col == j), value, table)
    h_out[...] = table[:, 0:3]
    writes = [pltpu.make_async_copy(h_out, hess, out_sems.at[4, 0])]
    writes[0].start()

    def wide(v):
        return jnp.concatenate([v, v], axis=1)

    scale = {key: wide(v) for key, v in low.items()}
    inv = {key: wide(v) for key, v in inverse.items()}
    c = wide(shift)

    for f in range(4):

        def body(j, _):
            raw = [vec[i, f, 5 + j, own_rows, :] for i in range(3)] + [w2[f, j]]
            found = [y1[i, f, 1 + j, own_rows, :] if f < 3 else q[i, 3 + j, own_rows, :] for i in range(3)]
            for values, dst in ((raw, b_out), (found, s_out)):
                values = values[:1] + [b - c * a for a, b in zip(values, values[1:])]
                done = []
                for i, value in enumerate(values):
                    for m in range(i):
                        value = value - scale[i, m] * done[m]
                    value = value * inv[i]
                    dst[i, f, j] = value
                    done.append(value)
            return 0

        lax.fori_loop(0, 6, body, 0, unroll=3)
        for i, (src, dst) in enumerate(((b_out, basis), (s_out, search))):
            copy = pltpu.make_async_copy(src.at[:, f], dst.at[:, f], out_sems.at[f, i])
            copy.start()
            writes.append(copy)
    for copy in writes:
        copy.wait()


def per_device(start, wind, reaction, mass):
    f32 = jnp.float32
    hbm_spec = pl.BlockSpec(memory_space=pltpu.HBM)
    vmem_spec = pl.BlockSpec(memory_space=pltpu.VMEM)
    n_send, n_receive = 14 + 5 + 4, 14 * 3 + 5 + 4
    kept = (
        jax.ShapeDtypeStruct((3, 4, 16, ROWS, 256), f32),
        jax.ShapeDtypeStruct((4, 6, 16, 256), f32),
        jax.ShapeDtypeStruct((3, 3, 8, ROWS, 256), f32),
        jax.ShapeDtypeStruct((3, 12, ROWS, 256), f32),
        jax.ShapeDtypeStruct((1, HALF), f32),
    )
    arrays = [pltpu.with_memory_space_constraint(a, pltpu.HBM) for a in (start, wind, reaction, mass)]
    outs = pl.pallas_call(
        krylov_kernel,
        out_shape=kept,
        in_specs=[hbm_spec] * 4,
        out_specs=(vmem_spec,) * 5,
        scratch_shapes=[
            pltpu.VMEM((5, 10, ROWS, 256), f32),
            pltpu.VMEM((9, 10, ROWS, 256), f32),
            pltpu.VMEM((16, ROWS, 256), f32),
            pltpu.VMEM((3, 10, ROWS, 256), f32),
            pltpu.VMEM((3, 10, ROWS, 256), f32),
            pltpu.VMEM((2, 2, 1, HALF), f32),
            pltpu.VMEM((2, 2 * NX_T * NY_T, 1, HALF), f32),
            pltpu.VMEM((2, NZ_T, 1, HALF), f32),
            pltpu.SemaphoreType.DMA((n_send,)),
            pltpu.SemaphoreType.DMA((n_receive,)),
            pltpu.SemaphoreType.DMA((4,)),
            pltpu.SemaphoreType.REGULAR((3,)),
        ],
        compiler_params=pltpu.CompilerParams(
            collective_id=0, has_side_effects=True, vmem_limit_bytes=24 * 2**20
        ),
        name="krylov",
    )(*arrays)
    return tuple(pl.pallas_call(
        combine_kernel,
        out_shape=(
            jax.ShapeDtypeStruct((4, 4, 6, 16, 256), f32),
            jax.ShapeDtypeStruct((3, 4, 6, 16, 256), f32),
            jax.ShapeDtypeStruct((4, 3), f32),
        ),
        in_specs=[vmem_spec] * 5,
        out_specs=(hbm_spec, hbm_spec, hbm_spec),
        scratch_shapes=[
            pltpu.VMEM((4, 4, 6, 16, 256), f32),
            pltpu.VMEM((3, 4, 6, 16, 256), f32),
            pltpu.VMEM((4, 3), f32),
            pltpu.SemaphoreType.DMA((5, 2)),
        ],
        compiler_params=pltpu.CompilerParams(vmem_limit_bytes=24 * 2**20),
        name="combine",
    )(*outs))


def solution(mesh):
    in_specs = (
        P(None, "slab", "sub", None),
        P(None, "slab", "sub", None),
        P("slab", "sub", None),
        P("slab", "sub", None),
    )
    out_specs = (P(None, None, "slab", "sub", None), P(None, None, "slab", "sub", None), P())
    return jax.shard_map(per_device, mesh=mesh, in_specs=in_specs, out_specs=out_specs, check_vma=False)
```

```python
import functools

import jax
import jax.numpy as jnp
from jax import lax
from jax.experimental import pallas as pl
from jax.experimental.pallas import tpu as pltpu
from jax.sharding import PartitionSpec as P

MESH_ID = pl.DeviceIdType.MESH
NX_T, NY_T, NZ_T = 4, 4, 8
ROWS = 24
HALF = 128


def lane_is(lane):
    return lax.broadcasted_iota(jnp.int32, (ROWS, HALF), 1) == lane


def get(ref, *lead):
    return ref[(*lead, slice(None), pl.ds(0, HALF))], ref[(*lead, slice(None), pl.ds(HALF, HALF))]


def put(ref, value, *lead):
    ref[(*lead, slice(None), pl.ds(0, HALF))] = value[0]
    ref[(*lead, slice(None), pl.ds(HALF, HALF))] = value[1]


def up_z(f, last):
    low, high = pltpu.roll(f[0], HALF - 1, 1), pltpu.roll(f[1], HALF - 1, 1)
    return jnp.where(last, high, low), jnp.where(last, 0.0, high)


def down_z(f, first):
    low, high = pltpu.roll(f[0], 1, 1), pltpu.roll(f[1], 1, 1)
    return jnp.where(first, 0.0, low), jnp.where(first, low, high)


def up_y(f):
    return tuple(pltpu.roll(h, ROWS - 1, 0) for h in f)


def down_y(f):
    return tuple(pltpu.roll(h, 1, 0) for h in f)


def krylov_kernel(
    start, wind, reac, mass,
    vec, w2, y1, q, gram_out,
    coef, work, t1, res, y0, part, slots_a, slots_b,
    send_sems, recv_sems, load_sems, told,
):
    slab, sub = lax.axis_index("slab"), lax.axis_index("sub")
    slabs = lax.axis_size("slab")
    other = 1 - sub
    z = lax.div(slab, NX_T * NY_T)
    has_left, has_right = slab > 0, slab < slabs - 1
    left, right = jnp.maximum(slab - 1, 0), jnp.minimum(slab + 1, slabs - 1)
    own_rows = pl.ds(pl.multiple_of(8 * sub, 8), 16)
    out_tile = pl.ds(8, 8)
    in_tile = pl.ds(pl.multiple_of(16 * sub, 8), 8)

    plane = 2 * NX_T * NY_T
    in_plane = lax.rem(2 * slab + sub, plane)

    def peers(stage):
        if stage == 0:
            for k in range(1, plane):
                at = lax.rem(in_plane + k, plane)
                yield (z * (NX_T * NY_T) + lax.div(at, 2), lax.rem(at, 2))
        else:
            for k in range(1, NZ_T):
                yield (slab + NX_T * NY_T * (lax.rem(z + k, NZ_T) - z), sub)

    loads = [
        pltpu.make_async_copy(start, vec.at[0, :, pl.ds(5, 6), own_rows], load_sems.at[0]),
        pltpu.make_async_copy(wind, coef.at[pl.ds(0, 3), pl.ds(2, 6), own_rows], load_sems.at[1]),
        pltpu.make_async_copy(reac, coef.at[3, pl.ds(2, 6), own_rows], load_sems.at[2]),
        pltpu.make_async_copy(mass, coef.at[4, pl.ds(2, 6), own_rows], load_sems.at[3]),
    ]
    for copy in loads:
        copy.start()

    x, y = lax.rem(slab, NX_T), lax.rem(lax.div(slab, NX_T), NY_T)

    def line_x():
        for k in range(1, 2 * NX_T):
            at = lax.rem(2 * x + sub + k, 2 * NX_T)
            yield (slab - x + lax.div(at, 2), lax.rem(at, 2))

    def line_y():
        for k in range(1, NY_T):
            yield (slab + NX_T * (lax.rem(y + k, NY_T) - y), sub)

    def near_z():
        for k in (1, NZ_T - 1):
            yield (slab + NX_T * NY_T * (lax.rem(z + k, NZ_T) - z), sub)

    def signal_all(sem, devices):
        for device in devices:
            pl.semaphore_signal(sem, inc=1, device_id=device, device_id_type=MESH_ID)
        return len(devices)

    def tell(turn):
        return signal_all(told.at[turn], [*line_y(), *near_z()] if turn == 0 else [*near_z()])

    def hear(turn, count):
        pl.semaphore_wait(told.at[turn], count)

    barrier = pltpu.get_barrier_semaphore()
    count = signal_all(barrier, [*line_x(), *line_y(), *near_z()])

    @pl.when(has_left)
    def _():
        pl.semaphore_signal(barrier, inc=1, device_id=(left, sub), device_id_type=MESH_ID)

    @pl.when(has_right)
    def _():
        pl.semaphore_signal(barrier, inc=1, device_id=(right, sub), device_id_type=MESH_ID)

    halo_rows = pl.ds(pl.multiple_of(16 * other, 8), 8)
    for k in range(3):
        for d in range(3):
            for plane_at in (3, 12):
                vec[k, d, plane_at, halo_rows] = jnp.zeros((8, 256), jnp.float32)
        for plane_at in (0, 11):
            q[k, plane_at, halo_rows] = jnp.zeros((8, 256), jnp.float32)

    def clear(planes, coef_planes, far_plane):
        for k in range(3):
            for f in range(4):
                vec[k, f, planes] = jnp.zeros((5, ROWS, 256), jnp.float32)
        for f in range(5):
            coef[f, coef_planes] = jnp.zeros((2, ROWS, 256), jnp.float32)
        for k in range(3):
            q[k, far_plane] = jnp.zeros((ROWS, 256), jnp.float32)

    @pl.when(jnp.logical_not(has_left))
    def _():
        clear(pl.ds(0, 5), pl.ds(0, 2), 0)

    @pl.when(jnp.logical_not(has_right))
    def _():
        clear(pl.ds(11, 5), pl.ds(8, 2), 11)

    pl.semaphore_wait(
        barrier, count + has_left.astype(jnp.int32) + has_right.astype(jnp.int32)
    )
    expected = [tell(0)]

    used = {"send": 0, "receive": 0}

    def remote(src, dst, device):
        copy = pltpu.make_async_remote_copy(
            src_ref=src, dst_ref=dst, send_sem=send_sems.at[used["send"]],
            recv_sem=recv_sems.at[used["receive"]], device_id=device, device_id_type=MESH_ID,
        )
        slot_of[id(copy)] = used["send"]
        keep.append(copy)
        used["send"] += 1
        used["receive"] += 1
        return copy

    slot_of, keep, sending = {}, [], {}

    def sent(slot):
        copy, condition = sending.pop(slot)
        if condition is None:
            copy.wait_send()
        else:
            pl.when(condition)(copy.wait_send)

    def go(copy, condition=None):
        slot = slot_of[id(copy)]
        if slot in sending:
            sent(slot)
        sending[slot] = (copy, condition)
        if condition is None:
            copy.start()
        else:
            pl.when(condition)(copy.start)

    def arrive(copy, condition=None):
        if condition is None:
            copy.wait_recv()
        else:
            pl.when(condition)(copy.wait_recv)

    class Halo:
        def __init__(self, src_low, src_high, src_tile, buffer, low, high, own):
            self.to_right = remote(src_high, buffer(low, own_rows), (right, sub))
            self.to_left = remote(src_low, buffer(high, own_rows), (left, sub))
            self.to_other = remote(src_tile, buffer(own, in_tile), (slab, other))
            self.low_on = remote(buffer(low, out_tile), buffer(low, in_tile), (slab, other))
            self.high_on = remote(buffer(high, out_tile), buffer(high, in_tile), (slab, other))

        def send(self):
            go(self.to_right, has_right)
            go(self.to_left, has_left)
            go(self.to_other)

        def forward(self):
            arrive(self.to_right, has_left)
            go(self.low_on, has_left)
            arrive(self.to_left, has_right)
            go(self.high_on, has_right)

        def finish(self):
            arrive(self.low_on, has_left)
            arrive(self.high_on, has_right)

    class FarHalo:
        def __init__(self, to_right, to_left):
            self.to_right, self.to_left = to_right, to_left

        def send(self):
            go(self.to_right, has_right)
            go(self.to_left, has_left)

        def finish(self):
            arrive(self.to_right, has_left)
            arrive(self.to_left, has_right)

    def vec_halo(k):
        def pressure(planes, rows):
            return vec.at[k, 3, planes, rows]

        def velocity(planes, rows):
            return vec.at[k, pl.ds(0, 3), planes, rows]

        p_src = (
            pressure(pl.ds(5, 4), own_rows), pressure(pl.ds(7, 4), own_rows),
            pressure(pl.ds(5, 6), out_tile),
        )
        near_src = (
            velocity(pl.ds(5, 1), own_rows), velocity(pl.ds(10, 1), own_rows),
            velocity(pl.ds(5, 6), out_tile),
        )
        p_halo = Halo(*p_src, pressure, pl.ds(1, 4), pl.ds(11, 4), pl.ds(5, 6))
        near = Halo(*near_src, velocity, pl.ds(4, 1), pl.ds(11, 1), pl.ds(5, 6))
        far = FarHalo(
            remote(velocity(pl.ds(9, 1), own_rows), velocity(pl.ds(3, 1), own_rows), (right, sub)),
            remote(velocity(pl.ds(6, 1), own_rows), velocity(pl.ds(12, 1), own_rows), (left, sub)),
        )
        schur_far = FarHalo(
            remote(q.at[k, 6, own_rows], q.at[k, 0, own_rows], (right, sub)),
            remote(q.at[k, 5, own_rows], q.at[k, 11, own_rows], (left, sub)),
        )
        return p_halo, near, far, schur_far

    def coef_halo(buffer):
        parts = (
            buffer(pl.ds(2, 2), own_rows), buffer(pl.ds(6, 2), own_rows), buffer(pl.ds(2, 6), out_tile),
        )
        return Halo(*parts, buffer, pl.ds(0, 2), pl.ds(8, 2), pl.ds(2, 6))

    halos = []
    for k in range(3):
        used["send"] = 0
        halos.append(vec_halo(k))
    coef_halo = coef_halo(lambda planes, rows: coef.at[:, planes, rows])
    loads[0].wait()
    halos[0][0].send()
    for copy in loads[1:]:
        copy.wait()
    coef_halo.send()
    for halo in halos[0][1:3]:
        halo.send()

    last, first = lane_is(HALF - 1), lane_is(0)
    row = lax.broadcasted_iota(jnp.int32, (ROWS, HALF), 0)
    live = row != (ROWS - 1) * other

    def inside(plane):
        at = slab * 6 + plane - 5
        return jnp.logical_and(at >= 0, at < slabs * 6)

    def prepare(j, _):
        ok = jnp.logical_and(live, inside(j + 3))
        for d in range(3):
            half = [0.5 * h for h in get(coef, d, j)]
            put(work, [h - 1.0 for h in half], d, j)
            put(work, [-1.0 - h for h in half], d + 3, j)
        diagonal = [6.0 + h for h in get(coef, 3, j)]
        put(work, diagonal, 6, j)
        put(work, [jnp.where(ok, 1.0 / h, 0.0) for h in diagonal], 7, j)
        put(work, [jnp.where(ok, -1.0 / h, 0.0) for h in get(coef, 4, j)], 8, j)
        return 0

    def six(fxm, f, fxp):
        total = [a + b for a, b in zip(fxm, fxp)]
        for g in (up_y(f), down_y(f), up_z(f, last), down_z(f, first)):
            total = [a + b for a, b in zip(total, g)]
        return total

    def weights(j):
        return [get(work, i, j) for i in range(7)]

    def transport(fxm, f, fxp, w):
        total = [a * b for a, b in zip(w[6], f)]
        terms = ((0, fxp), (3, fxm), (1, up_y(f)), (4, down_y(f)), (2, up_z(f, last)), (5, down_z(f, first)))
        for i, g in terms:
            total = [t + a * b for t, a, b in zip(total, w[i], g)]
        return total

    def half_difference(a, b):
        return [0.5 * (m - n) for m, n in zip(a, b)]

    def gradient(fxm, f, fxp):
        return (
            half_difference(fxp, fxm),
            half_difference(up_y(f), down_y(f)),
            half_difference(up_z(f, last), down_z(f, first)),
        )

    def loop(count, body, plane, unroll):
        def step(i, _):
            body(plane(i))
            return 0

        lax.fori_loop(0, count, step, 0, unroll=unroll)

    def guess(k, j):
        scale = jnp.where(jnp.logical_and(live, inside(j)), 1.0 / 49.0, 0.0)
        f = [jnp.where(live, h, 0.0) for h in get(vec, k, 3, j)]
        total = six(get(vec, k, 3, j - 1), f, get(vec, k, 3, j + 1))
        put(t1, [scale * (7.0 * a + b) for a, b in zip(f, total)], j)

    def schur(k, j):
        value = transport(get(t1, j - 1), get(t1, j), get(t1, j + 1), weights(j - 3))
        put(q, [a * b for a, b in zip(value, get(work, 8, j - 3))], k, j - 2)

    def pressure_inner(k):
        loop(4, functools.partial(guess, k), lambda i: i + 6, 4)
        loop(2, functools.partial(schur, k), lambda i: i + 7, 2)

    def pressure_outer(k):
        loop(8, functools.partial(guess, k), lambda i: i + 2 + 4 * lax.div(i, 4), 8)
        loop(8, functools.partial(schur, k), lambda i: i + 3 + 2 * lax.div(i, 4), 8)

    def first_guess(k, j):
        slope = gradient(get(q, k, j), get(q, k, j + 1), get(q, k, j + 2))
        inverse = get(work, 7, j)
        for d in range(3):
            r = [a - b for a, b in zip(get(vec, k, d, j + 3), slope[d])]
            put(res, r, d, j)
            put(y0, [a * b for a, b in zip(r, inverse)], d, j)

    def second_guess(k, j):
        w = weights(j + 1)
        inverse = get(work, 7, j + 1)
        for d in range(3):
            f = get(y0, d, j + 1)
            value = transport(get(y0, d, j), f, get(y0, d, j + 2), w)
            r = get(res, d, j + 1)
            put(y1, [a + (b - c) * i for a, b, c, i in zip(f, r, value, inverse)], k, d, j)

    def velocity_inner(k):
        loop(8, functools.partial(first_guess, k), lambda i: i + 1, 8)
        loop(6, functools.partial(second_guess, k), lambda i: i + 1, 6)

    def velocity_outer(k, target, after_pressure=lambda: None):
        loop(2, functools.partial(first_guess, k), lambda i: 9 * i, 2)
        loop(2, functools.partial(second_guess, k), lambda i: 7 * i, 2)

        def store(f, j, value):
            for i, h in enumerate(value):
                mine = jnp.where(sub == 0, h[0:16], h[8:24])
                target(f, j)[own_rows if k < 2 else slice(None), pl.ds(HALF * i, HALF)] = mine

        def image_pressure(j, _):
            pc = get(q, k, j + 3)
            total = six(get(q, k, j + 2), pc, get(q, k, j + 4))
            yc, zc = get(y1, k, 1, j + 1), get(y1, k, 2, j + 1)
            ends = (
                (get(y1, k, 0, j + 2), get(y1, k, 0, j)), (up_y(yc), down_y(yc)),
                (up_z(zc, last), down_z(zc, first)),
            )
            flow = [a - b for a, b in zip(*ends[0])]
            for high, low in ends[1:]:
                flow = [t + (a - b) for t, a, b in zip(flow, high, low)]
            store(3, j, [-0.5 * (a + (6.0 * b - c)) for a, b, c in zip(flow, pc, total)])
            return 0

        lax.fori_loop(0, 6, image_pressure, 0, unroll=6)
        after_pressure()

        def image_velocity(j, _):
            w = weights(j + 2)
            slope = gradient(get(q, k, j + 2), get(q, k, j + 3), get(q, k, j + 4))
            for d in range(3):
                value = transport(get(y1, k, d, j), get(y1, k, d, j + 1), get(y1, k, d, j + 2), w)
                store(d, j, [a + b for a, b in zip(value, slope[d])])
            return 0

        lax.fori_loop(0, 6, image_velocity, 0, unroll=6)

    lane8 = lax.broadcasted_iota(jnp.int32, (8, HALF), 1)

    def vectors(i, f, j):
        return vec[i, f, 5 + j, own_rows, :] if i < 3 else w2[f, j]

    def dots(pairs, shift=None):
        needed = sorted({i for pair in pairs for i in pair})

        def step(j, accs):
            accs = list(accs)
            for f in range(4):
                raw = {}
                for i in needed:
                    for at in (i,) if shift is None or i == 0 else (i - 1, i):
                        if at not in raw:
                            raw[at] = vectors(at, f, j)
                y = {i: raw[i] if shift is None or i == 0 else raw[i] - shift * raw[i - 1] for i in needed}
                for n, (i, k) in enumerate(pairs):
                    prod = y[i] * y[k]
                    accs[n] = accs[n] + (
                        (prod[0:8, 0:HALF] + prod[0:8, HALF:]) + (prod[8:16, 0:HALF] + prod[8:16, HALF:])
                    )
            return tuple(accs)

        zero = jnp.zeros((8, HALF), jnp.float32)
        return lax.fori_loop(0, 6, step, tuple(zero for _ in pairs), unroll=2)

    def pack(total, sums, at):
        for i, s in enumerate(sums):
            total = jnp.where(lane8 == at + i, jnp.sum(s, axis=1, keepdims=True), total)
        return total

    class Reduction:
        def __init__(self, n):
            self.n = n

        def message(self, stage, src, dst, device):
            at = 2 * self.n + stage
            return pltpu.make_async_remote_copy(
                src_ref=src, dst_ref=dst, send_sem=send_sems.at[used["send"] + at],
                recv_sem=recv_sems.at[used["receive"] + at], device_id=device, device_id_type=MESH_ID,
            )

        def send(self, stage, row):
            place, slots = ((in_plane, slots_a), (z, slots_b))[stage]
            part[self.n, stage] = row
            slots[self.n, place] = row
            for peer in peers(stage):
                self.message(stage, part.at[self.n, stage], slots.at[self.n, place], peer).start()

        def finish(self, stage):
            slots = (slots_a, slots_b)[stage]
            rest = slots.at[self.n, pl.ds(0, slots.shape[1] - 1)]
            everything = self.message(stage, rest, rest, (slab, other))
            everything.wait_recv()
            everything.wait_send()
            return jnp.sum(slots[self.n], axis=0)

        def whole(self, row):
            for stage in range(2):
                self.send(stage, row)
                row = self.finish(stage)
            return row

    reductions = [Reduction(0), Reduction(1)]

    def application(k, target, waiting, waited, after_pressure=lambda: None):
        p_halo, near, far, schur_far = halos[k]
        arrive(p_halo.to_other)
        if k == 0:
            arrive(coef_halo.to_other)
            lax.fori_loop(2, 8, prepare, 0, unroll=2)
        pressure_inner(k)
        schur_far.send()
        kept = waiting()
        p_halo.forward()
        if k == 0:
            coef_halo.forward()
        p_halo.finish()
        near.forward()
        waited()
        if k == 0:
            coef_halo.finish()
            for planes in (0, 8):
                lax.fori_loop(planes, planes + 2, prepare, 0, unroll=2)
        pressure_outer(k)
        arrive(near.to_other)
        near.finish()
        velocity_inner(k)
        far.finish()
        schur_far.finish()
        velocity_outer(k, target, after_pressure)
        return kept

    def pass_on(turn):
        hear(turn, expected[turn])
        expected.append(tell(turn + 1))

    def shift_known():
        row = reductions[0].finish(1)

        def entry(i):
            return jnp.sum(jnp.where(lane_row == i, row, 0.0), axis=1, keepdims=True)

        c = jnp.broadcast_to(entry(1) / entry(0), (1, HALF))
        c = jnp.concatenate([c, c], axis=1)
        pairs = ((0, 0), (1, 0), (1, 1), (2, 0), (2, 1), (2, 2))
        return c, pack(jnp.zeros((8, HALF), jnp.float32), dots(pairs, c), 0)

    def nothing():
        return None

    lane_row = lax.broadcasted_iota(jnp.int32, (1, HALF), 1)
    application(
        0, lambda f, j: vec.at[1, f, 5 + j], lambda: pass_on(0), lambda: pass_on(1), halos[1][0].send
    )
    halos[1][1].send()
    halos[1][2].send()
    hear(2, expected[2])
    opening = pack(jnp.zeros((8, HALF), jnp.float32), dots(((0, 0), (1, 0))), 0)
    reductions[0].send(0, jnp.sum(opening, axis=0, keepdims=True))
    application(
        1, lambda f, j: vec.at[2, f, 5 + j], nothing,
        lambda: reductions[0].send(1, reductions[0].finish(0)), halos[2][0].send,
    )
    halos[2][1].send()
    halos[2][2].send()
    shift, gram = application(2, lambda f, j: w2.at[f, j], shift_known, nothing)
    gram = pack(gram, dots(((3, 0), (3, 1), (3, 2), (3, 3)), shift), 6)

    total = reductions[1].whole(jnp.sum(gram, axis=0, keepdims=True))
    lane1 = lax.broadcasted_iota(jnp.int32, (1, HALF), 1)
    gram_out[...] = jnp.where(lane1 == 10, shift[:, 0:HALF], total)

    for slot in list(sending):
        sent(slot)


def combine_kernel(vec, w2, y1, q, gram, basis, search, hess, b_out, s_out, h_out, out_sems):
    own_rows = pl.ds(pl.multiple_of(8 * lax.axis_index("sub"), 8), 16)

    total = gram[...]
    lane = lax.broadcasted_iota(jnp.int32, (1, HALF), 1)

    def entry(i):
        return jnp.broadcast_to(jnp.sum(jnp.where(lane == i, total, 0.0), axis=1, keepdims=True), (1, HALF))

    low = {}
    inverse = {}
    for i in range(4):
        for j in range(i + 1):
            value = entry(i * (i + 1) // 2 + j)
            for m in range(j):
                value = value - low[i, m] * low[j, m]
            if i == j:
                low[i, i] = jnp.sqrt(value)
                inverse[i] = 1.0 / low[i, i]
            else:
                low[i, j] = value * inverse[j]
    shift = entry(10)
    h = {}
    for j in range(3):
        for i in range(j + 2):
            value = low[j + 1, i]
            if j == 0 and i == 0:
                value = value + shift * low[0, 0]
            for m in range(j):
                if i <= m + 1:
                    value = value - low[j, m] * h[i, m]
            h[i, j] = value * inverse[j]
    at_row = lax.broadcasted_iota(jnp.int32, (4, HALF), 0)
    at_col = lax.broadcasted_iota(jnp.int32, (4, HALF), 1)
    table = jnp.zeros((4, HALF), jnp.float32)
    for (i, j), value in h.items():
        table = jnp.where(jnp.logical_and(at_row == i, at_col == j), value, table)
    h_out[...] = table[:, 0:3]
    writes = [pltpu.make_async_copy(h_out, hess, out_sems.at[4, 0])]
    writes[0].start()

    def wide(v):
        return jnp.concatenate([v, v], axis=1)

    scale = {key: wide(v) for key, v in low.items()}
    inv = {key: wide(v) for key, v in inverse.items()}
    c = wide(shift)

    for f in range(4):

        def body(j, _):
            raw = [vec[i, f, 5 + j, own_rows, :] for i in range(3)] + [w2[f, j]]
            found = [y1[i, f, 1 + j, own_rows, :] if f < 3 else q[i, 3 + j, own_rows, :] for i in range(3)]
            for values, dst in ((raw, b_out), (found, s_out)):
                values = values[:1] + [b - c * a for a, b in zip(values, values[1:])]
                done = []
                for i, value in enumerate(values):
                    for m in range(i):
                        value = value - scale[i, m] * done[m]
                    value = value * inv[i]
                    dst[i, f, j] = value
                    done.append(value)
            return 0

        lax.fori_loop(0, 6, body, 0, unroll=3)
        for i, (src, dst) in enumerate(((b_out, basis), (s_out, search))):
            copy = pltpu.make_async_copy(src.at[:, f], dst.at[:, f], out_sems.at[f, i])
            copy.start()
            writes.append(copy)
    for copy in writes:
        copy.wait()


def per_device(start, wind, reaction, mass):
    f32 = jnp.float32
    hbm_spec = pl.BlockSpec(memory_space=pltpu.HBM)
    vmem_spec = pl.BlockSpec(memory_space=pltpu.VMEM)
    n_send, n_receive = 14 + 5 + 4, 14 * 3 + 5 + 4
    kept = (
        jax.ShapeDtypeStruct((3, 4, 16, ROWS, 256), f32),
        jax.ShapeDtypeStruct((4, 6, 16, 256), f32),
        jax.ShapeDtypeStruct((3, 3, 8, ROWS, 256), f32),
        jax.ShapeDtypeStruct((3, 12, ROWS, 256), f32),
        jax.ShapeDtypeStruct((1, HALF), f32),
    )
    arrays = [pltpu.with_memory_space_constraint(a, pltpu.HBM) for a in (start, wind, reaction, mass)]
    outs = pl.pallas_call(
        krylov_kernel,
        out_shape=kept,
        in_specs=[hbm_spec] * 4,
        out_specs=(vmem_spec,) * 5,
        scratch_shapes=[
            pltpu.VMEM((5, 10, ROWS, 256), f32),
            pltpu.VMEM((9, 10, ROWS, 256), f32),
            pltpu.VMEM((16, ROWS, 256), f32),
            pltpu.VMEM((3, 10, ROWS, 256), f32),
            pltpu.VMEM((3, 10, ROWS, 256), f32),
            pltpu.VMEM((2, 2, 1, HALF), f32),
            pltpu.VMEM((2, 2 * NX_T * NY_T, 1, HALF), f32),
            pltpu.VMEM((2, NZ_T, 1, HALF), f32),
            pltpu.SemaphoreType.DMA((n_send,)),
            pltpu.SemaphoreType.DMA((n_receive,)),
            pltpu.SemaphoreType.DMA((4,)),
            pltpu.SemaphoreType.REGULAR((3,)),
        ],
        compiler_params=pltpu.CompilerParams(
            collective_id=0, has_side_effects=True, vmem_limit_bytes=24 * 2**20
        ),
        name="krylov",
    )(*arrays)
    return tuple(pl.pallas_call(
        combine_kernel,
        out_shape=(
            jax.ShapeDtypeStruct((4, 4, 6, 16, 256), f32),
            jax.ShapeDtypeStruct((3, 4, 6, 16, 256), f32),
            jax.ShapeDtypeStruct((4, 3), f32),
        ),
        in_specs=[vmem_spec] * 5,
        out_specs=(hbm_spec, hbm_spec, hbm_spec),
        scratch_shapes=[
            pltpu.VMEM((4, 4, 6, 16, 256), f32),
            pltpu.VMEM((3, 4, 6, 16, 256), f32),
            pltpu.VMEM((4, 3), f32),
            pltpu.SemaphoreType.DMA((5, 2)),
        ],
        compiler_params=pltpu.CompilerParams(vmem_limit_bytes=24 * 2**20),
        name="combine",
    )(*outs))


def solution(mesh):
    in_specs = (
        P(None, "slab", "sub", None),
        P(None, "slab", "sub", None),
        P("slab", "sub", None),
        P("slab", "sub", None),
    )
    out_specs = (P(None, None, "slab", "sub", None), P(None, None, "slab", "sub", None), P())
    return jax.shard_map(per_device, mesh=mesh, in_specs=in_specs, out_specs=out_specs, check_vma=False)
```

```python
import functools

import jax
import jax.numpy as jnp
from jax import lax
from jax.experimental import pallas as pl
from jax.experimental.pallas import tpu as pltpu
from jax.sharding import PartitionSpec as P

MESH_ID = pl.DeviceIdType.MESH
NX_T, NY_T, NZ_T = 4, 4, 8
ROWS = 24
HALF = 128


def lane_is(lane):
    return lax.broadcasted_iota(jnp.int32, (ROWS, HALF), 1) == lane


def get(ref, *lead):
    return ref[(*lead, slice(None), pl.ds(0, HALF))], ref[(*lead, slice(None), pl.ds(HALF, HALF))]


def put(ref, value, *lead):
    ref[(*lead, slice(None), pl.ds(0, HALF))] = value[0]
    ref[(*lead, slice(None), pl.ds(HALF, HALF))] = value[1]


def up_z(f, last):
    low, high = pltpu.roll(f[0], HALF - 1, 1), pltpu.roll(f[1], HALF - 1, 1)
    return jnp.where(last, high, low), jnp.where(last, 0.0, high)


def down_z(f, first):
    low, high = pltpu.roll(f[0], 1, 1), pltpu.roll(f[1], 1, 1)
    return jnp.where(first, 0.0, low), jnp.where(first, low, high)


def up_y(f):
    return tuple(pltpu.roll(h, ROWS - 1, 0) for h in f)


def down_y(f):
    return tuple(pltpu.roll(h, 1, 0) for h in f)


def krylov_kernel(
    start, wind, reac, mass,
    vec, w2, y1, q, gram_out,
    coef, work, t1, res, y0, part, slots_a, slots_b,
    send_sems, recv_sems, load_sems, told,
):
    slab, sub = lax.axis_index("slab"), lax.axis_index("sub")
    slabs = lax.axis_size("slab")
    other = 1 - sub
    z = lax.div(slab, NX_T * NY_T)
    has_left, has_right = slab > 0, slab < slabs - 1
    left, right = jnp.maximum(slab - 1, 0), jnp.minimum(slab + 1, slabs - 1)
    own_rows = pl.ds(pl.multiple_of(8 * sub, 8), 16)
    out_tile = pl.ds(8, 8)
    in_tile = pl.ds(pl.multiple_of(16 * sub, 8), 8)

    plane = 2 * NX_T * NY_T
    in_plane = lax.rem(2 * slab + sub, plane)

    def peers(stage):
        if stage == 0:
            for k in range(1, plane):
                at = lax.rem(in_plane + k, plane)
                yield (z * (NX_T * NY_T) + lax.div(at, 2), lax.rem(at, 2))
        else:
            for k in range(1, NZ_T):
                yield (slab + NX_T * NY_T * (lax.rem(z + k, NZ_T) - z), sub)

    loads = [
        pltpu.make_async_copy(start, vec.at[0, :, pl.ds(5, 6), own_rows], load_sems.at[0]),
        pltpu.make_async_copy(wind, coef.at[pl.ds(0, 3), pl.ds(2, 6), own_rows], load_sems.at[1]),
        pltpu.make_async_copy(reac, coef.at[3, pl.ds(2, 6), own_rows], load_sems.at[2]),
        pltpu.make_async_copy(mass, coef.at[4, pl.ds(2, 6), own_rows], load_sems.at[3]),
    ]
    for copy in loads:
        copy.start()

    x, y = lax.rem(slab, NX_T), lax.rem(lax.div(slab, NX_T), NY_T)

    def line_x():
        for k in range(1, 2 * NX_T):
            at = lax.rem(2 * x + sub + k, 2 * NX_T)
            yield (slab - x + lax.div(at, 2), lax.rem(at, 2))

    def line_y():
        for k in range(1, NY_T):
            yield (slab + NX_T * (lax.rem(y + k, NY_T) - y), sub)

    def near_z():
        for k in (1, NZ_T - 1):
            yield (slab + NX_T * NY_T * (lax.rem(z + k, NZ_T) - z), sub)

    def signal_all(sem, devices):
        for device in devices:
            pl.semaphore_signal(sem, inc=1, device_id=device, device_id_type=MESH_ID)
        return len(devices)

    def tell(turn):
        return signal_all(told.at[turn], [*line_y(), *near_z()] if turn == 0 else [*near_z()])

    def hear(turn, count):
        pl.semaphore_wait(told.at[turn], count)

    barrier = pltpu.get_barrier_semaphore()
    count = signal_all(barrier, [*line_x(), *line_y(), *near_z()])

    @pl.when(has_left)
    def _():
        pl.semaphore_signal(barrier, inc=1, device_id=(left, sub), device_id_type=MESH_ID)

    @pl.when(has_right)
    def _():
        pl.semaphore_signal(barrier, inc=1, device_id=(right, sub), device_id_type=MESH_ID)

    halo_rows = pl.ds(pl.multiple_of(16 * other, 8), 8)
    for k in range(3):
        for d in range(3):
            for plane_at in (3, 12):
                vec[k, d, plane_at, halo_rows] = jnp.zeros((8, 256), jnp.float32)
        for plane_at in (0, 11):
            q[k, plane_at, halo_rows] = jnp.zeros((8, 256), jnp.float32)

    def clear(planes, coef_planes, far_plane):
        for k in range(3):
            for f in range(4):
                vec[k, f, planes] = jnp.zeros((5, ROWS, 256), jnp.float32)
        for f in range(5):
            coef[f, coef_planes] = jnp.zeros((2, ROWS, 256), jnp.float32)
        for k in range(3):
            q[k, far_plane] = jnp.zeros((ROWS, 256), jnp.float32)

    @pl.when(jnp.logical_not(has_left))
    def _():
        clear(pl.ds(0, 5), pl.ds(0, 2), 0)

    @pl.when(jnp.logical_not(has_right))
    def _():
        clear(pl.ds(11, 5), pl.ds(8, 2), 11)

    pl.semaphore_wait(
        barrier, count + has_left.astype(jnp.int32) + has_right.astype(jnp.int32)
    )
    expected = [tell(0)]

    used = {"send": 0, "receive": 0}

    def remote(src, dst, device):
        copy = pltpu.make_async_remote_copy(
            src_ref=src, dst_ref=dst, send_sem=send_sems.at[used["send"]],
            recv_sem=recv_sems.at[used["receive"]], device_id=device, device_id_type=MESH_ID,
        )
        slot_of[id(copy)] = used["send"]
        keep.append(copy)
        used["send"] += 1
        used["receive"] += 1
        return copy

    slot_of, keep, sending = {}, [], {}

    def sent(slot):
        copy, condition = sending.pop(slot)
        if condition is None:
            copy.wait_send()
        else:
            pl.when(condition)(copy.wait_send)

    def go(copy, condition=None):
        slot = slot_of[id(copy)]
        if slot in sending:
            sent(slot)
        sending[slot] = (copy, condition)
        if condition is None:
            copy.start()
        else:
            pl.when(condition)(copy.start)

    def arrive(copy, condition=None):
        if condition is None:
            copy.wait_recv()
        else:
            pl.when(condition)(copy.wait_recv)

    class Halo:
        def __init__(self, src_low, src_high, src_tile, buffer, low, high, own):
            self.to_right = remote(src_high, buffer(low, own_rows), (right, sub))
            self.to_left = remote(src_low, buffer(high, own_rows), (left, sub))
            self.to_other = remote(src_tile, buffer(own, in_tile), (slab, other))
            self.low_on = remote(buffer(low, out_tile), buffer(low, in_tile), (slab, other))
            self.high_on = remote(buffer(high, out_tile), buffer(high, in_tile), (slab, other))

        def send(self):
            go(self.to_right, has_right)
            go(self.to_left, has_left)
            go(self.to_other)

        def forward(self):
            arrive(self.to_right, has_left)
            go(self.low_on, has_left)
            arrive(self.to_left, has_right)
            go(self.high_on, has_right)

        def finish(self):
            arrive(self.low_on, has_left)
            arrive(self.high_on, has_right)

    class FarHalo:
        def __init__(self, to_right, to_left):
            self.to_right, self.to_left = to_right, to_left

        def send(self):
            go(self.to_right, has_right)
            go(self.to_left, has_left)

        def finish(self):
            arrive(self.to_right, has_left)
            arrive(self.to_left, has_right)

    def vec_halo(k):
        def pressure(planes, rows):
            return vec.at[k, 3, planes, rows]

        def velocity(planes, rows):
            return vec.at[k, pl.ds(0, 3), planes, rows]

        p_src = (
            pressure(pl.ds(5, 4), own_rows), pressure(pl.ds(7, 4), own_rows),
            pressure(pl.ds(5, 6), out_tile),
        )
        near_src = (
            velocity(pl.ds(5, 1), own_rows), velocity(pl.ds(10, 1), own_rows),
            velocity(pl.ds(5, 6), out_tile),
        )
        p_halo = Halo(*p_src, pressure, pl.ds(1, 4), pl.ds(11, 4), pl.ds(5, 6))
        near = Halo(*near_src, velocity, pl.ds(4, 1), pl.ds(11, 1), pl.ds(5, 6))
        far = FarHalo(
            remote(velocity(pl.ds(9, 1), own_rows), velocity(pl.ds(3, 1), own_rows), (right, sub)),
            remote(velocity(pl.ds(6, 1), own_rows), velocity(pl.ds(12, 1), own_rows), (left, sub)),
        )
        schur_far = FarHalo(
            remote(q.at[k, 6, own_rows], q.at[k, 0, own_rows], (right, sub)),
            remote(q.at[k, 5, own_rows], q.at[k, 11, own_rows], (left, sub)),
        )
        return p_halo, near, far, schur_far

    def coef_halo(buffer):
        parts = (
            buffer(pl.ds(2, 2), own_rows), buffer(pl.ds(6, 2), own_rows), buffer(pl.ds(2, 6), out_tile),
        )
        return Halo(*parts, buffer, pl.ds(0, 2), pl.ds(8, 2), pl.ds(2, 6))

    halos = []
    for k in range(3):
        used["send"] = 0
        halos.append(vec_halo(k))
    coef_halo = coef_halo(lambda planes, rows: coef.at[:, planes, rows])
    loads[0].wait()
    halos[0][0].send()
    for copy in loads[1:]:
        copy.wait()
    coef_halo.send()
    for halo in halos[0][1:3]:
        halo.send()

    last, first = lane_is(HALF - 1), lane_is(0)
    row = lax.broadcasted_iota(jnp.int32, (ROWS, HALF), 0)
    live = row != (ROWS - 1) * other

    def inside(plane):
        at = slab * 6 + plane - 5
        return jnp.logical_and(at >= 0, at < slabs * 6)

    def prepare(j, _):
        ok = jnp.logical_and(live, inside(j + 3))
        for d in range(3):
            half = [0.5 * h for h in get(coef, d, j)]
            put(work, [h - 1.0 for h in half], d, j)
            put(work, [-1.0 - h for h in half], d + 3, j)
        diagonal = [6.0 + h for h in get(coef, 3, j)]
        put(work, diagonal, 6, j)
        put(work, [jnp.where(ok, 1.0 / h, 0.0) for h in diagonal], 7, j)
        put(work, [jnp.where(ok, -1.0 / h, 0.0) for h in get(coef, 4, j)], 8, j)
        return 0

    def six(fxm, f, fxp):
        total = [a + b for a, b in zip(fxm, fxp)]
        for g in (up_y(f), down_y(f), up_z(f, last), down_z(f, first)):
            total = [a + b for a, b in zip(total, g)]
        return total

    def weights(j):
        return [get(work, i, j) for i in range(7)]

    def transport(fxm, f, fxp, w):
        total = [a * b for a, b in zip(w[6], f)]
        terms = ((0, fxp), (3, fxm), (1, up_y(f)), (4, down_y(f)), (2, up_z(f, last)), (5, down_z(f, first)))
        for i, g in terms:
            total = [t + a * b for t, a, b in zip(total, w[i], g)]
        return total

    def half_difference(a, b):
        return [0.5 * (m - n) for m, n in zip(a, b)]

    def gradient(fxm, f, fxp):
        return (
            half_difference(fxp, fxm),
            half_difference(up_y(f), down_y(f)),
            half_difference(up_z(f, last), down_z(f, first)),
        )

    def loop(count, body, plane, unroll):
        def step(i, _):
            body(plane(i))
            return 0

        lax.fori_loop(0, count, step, 0, unroll=unroll)

    def guess(k, j):
        scale = jnp.where(jnp.logical_and(live, inside(j)), 1.0 / 49.0, 0.0)
        f = [jnp.where(live, h, 0.0) for h in get(vec, k, 3, j)]
        total = six(get(vec, k, 3, j - 1), f, get(vec, k, 3, j + 1))
        put(t1, [scale * (7.0 * a + b) for a, b in zip(f, total)], j)

    def schur(k, j):
        value = transport(get(t1, j - 1), get(t1, j), get(t1, j + 1), weights(j - 3))
        put(q, [a * b for a, b in zip(value, get(work, 8, j - 3))], k, j - 2)

    def pressure_inner(k):
        loop(4, functools.partial(guess, k), lambda i: i + 6, 4)
        loop(2, functools.partial(schur, k), lambda i: i + 7, 2)

    def pressure_outer(k):
        loop(8, functools.partial(guess, k), lambda i: i + 2 + 4 * lax.div(i, 4), 8)
        loop(8, functools.partial(schur, k), lambda i: i + 3 + 2 * lax.div(i, 4), 8)

    def first_guess(k, j):
        slope = gradient(get(q, k, j), get(q, k, j + 1), get(q, k, j + 2))
        inverse = get(work, 7, j)
        for d in range(3):
            r = [a - b for a, b in zip(get(vec, k, d, j + 3), slope[d])]
            put(res, r, d, j)
            put(y0, [a * b for a, b in zip(r, inverse)], d, j)

    def second_guess(k, j):
        w = weights(j + 1)
        inverse = get(work, 7, j + 1)
        for d in range(3):
            f = get(y0, d, j + 1)
            value = transport(get(y0, d, j), f, get(y0, d, j + 2), w)
            r = get(res, d, j + 1)
            put(y1, [a + (b - c) * i for a, b, c, i in zip(f, r, value, inverse)], k, d, j)

    def velocity_inner(k):
        loop(8, functools.partial(first_guess, k), lambda i: i + 1, 8)
        loop(6, functools.partial(second_guess, k), lambda i: i + 1, 6)

    def velocity_outer(k, target, after_pressure=lambda: None):
        loop(2, functools.partial(first_guess, k), lambda i: 9 * i, 2)
        loop(2, functools.partial(second_guess, k), lambda i: 7 * i, 2)

        def store(f, j, value):
            for i, h in enumerate(value):
                mine = jnp.where(sub == 0, h[0:16], h[8:24])
                target(f, j)[own_rows if k < 2 else slice(None), pl.ds(HALF * i, HALF)] = mine

        def image_pressure(j, _):
            pc = get(q, k, j + 3)
            total = six(get(q, k, j + 2), pc, get(q, k, j + 4))
            yc, zc = get(y1, k, 1, j + 1), get(y1, k, 2, j + 1)
            ends = (
                (get(y1, k, 0, j + 2), get(y1, k, 0, j)), (up_y(yc), down_y(yc)),
                (up_z(zc, last), down_z(zc, first)),
            )
            flow = [a - b for a, b in zip(*ends[0])]
            for high, low in ends[1:]:
                flow = [t + (a - b) for t, a, b in zip(flow, high, low)]
            store(3, j, [-0.5 * (a + (6.0 * b - c)) for a, b, c in zip(flow, pc, total)])
            return 0

        lax.fori_loop(0, 6, image_pressure, 0, unroll=6)
        after_pressure()

        def image_velocity(j, _):
            w = weights(j + 2)
            slope = gradient(get(q, k, j + 2), get(q, k, j + 3), get(q, k, j + 4))
            for d in range(3):
                value = transport(get(y1, k, d, j), get(y1, k, d, j + 1), get(y1, k, d, j + 2), w)
                store(d, j, [a + b for a, b in zip(value, slope[d])])
            return 0

        lax.fori_loop(0, 6, image_velocity, 0, unroll=6)

    lane8 = lax.broadcasted_iota(jnp.int32, (8, HALF), 1)

    def vectors(i, f, j):
        return vec[i, f, 5 + j, own_rows, :] if i < 3 else w2[f, j]

    def dots(pairs, shift=None):
        needed = sorted({i for pair in pairs for i in pair})

        def step(j, accs):
            accs = list(accs)
            for f in range(4):
                raw = {}
                for i in needed:
                    for at in (i,) if shift is None or i == 0 else (i - 1, i):
                        if at not in raw:
                            raw[at] = vectors(at, f, j)
                y = {i: raw[i] if shift is None or i == 0 else raw[i] - shift * raw[i - 1] for i in needed}
                for n, (i, k) in enumerate(pairs):
                    prod = y[i] * y[k]
                    accs[n] = accs[n] + (
                        (prod[0:8, 0:HALF] + prod[0:8, HALF:]) + (prod[8:16, 0:HALF] + prod[8:16, HALF:])
                    )
            return tuple(accs)

        zero = jnp.zeros((8, HALF), jnp.float32)
        return lax.fori_loop(0, 6, step, tuple(zero for _ in pairs), unroll=6)

    def pack(total, sums, at):
        for i, s in enumerate(sums):
            total = jnp.where(lane8 == at + i, jnp.sum(s, axis=1, keepdims=True), total)
        return total

    class Reduction:
        def __init__(self, n):
            self.n = n

        def message(self, stage, src, dst, device):
            at = 2 * self.n + stage
            return pltpu.make_async_remote_copy(
                src_ref=src, dst_ref=dst, send_sem=send_sems.at[used["send"] + at],
                recv_sem=recv_sems.at[used["receive"] + at], device_id=device, device_id_type=MESH_ID,
            )

        def send(self, stage, row):
            place, slots = ((in_plane, slots_a), (z, slots_b))[stage]
            part[self.n, stage] = row
            slots[self.n, place] = row
            for peer in peers(stage):
                self.message(stage, part.at[self.n, stage], slots.at[self.n, place], peer).start()

        def finish(self, stage):
            slots = (slots_a, slots_b)[stage]
            rest = slots.at[self.n, pl.ds(0, slots.shape[1] - 1)]
            everything = self.message(stage, rest, rest, (slab, other))
            everything.wait_recv()
            everything.wait_send()
            return jnp.sum(slots[self.n], axis=0)

        def whole(self, row):
            for stage in range(2):
                self.send(stage, row)
                row = self.finish(stage)
            return row

    reductions = [Reduction(0), Reduction(1)]

    def application(k, target, waiting, waited, after_pressure=lambda: None):
        p_halo, near, far, schur_far = halos[k]
        arrive(p_halo.to_other)
        if k == 0:
            arrive(coef_halo.to_other)
            lax.fori_loop(2, 8, prepare, 0, unroll=6)
        pressure_inner(k)
        schur_far.send()
        kept = waiting()
        p_halo.forward()
        if k == 0:
            coef_halo.forward()
        p_halo.finish()
        near.forward()
        waited()
        if k == 0:
            coef_halo.finish()
            for planes in (0, 8):
                lax.fori_loop(planes, planes + 2, prepare, 0, unroll=2)
        pressure_outer(k)
        arrive(near.to_other)
        near.finish()
        velocity_inner(k)
        far.finish()
        schur_far.finish()
        velocity_outer(k, target, after_pressure)
        return kept

    def pass_on(turn):
        hear(turn, expected[turn])
        expected.append(tell(turn + 1))

    def shift_known():
        row = reductions[0].finish(1)

        def entry(i):
            return jnp.sum(jnp.where(lane_row == i, row, 0.0), axis=1, keepdims=True)

        c = jnp.broadcast_to(entry(1) / entry(0), (1, HALF))
        c = jnp.concatenate([c, c], axis=1)
        pairs = ((0, 0), (1, 0), (1, 1), (2, 0), (2, 1), (2, 2))
        return c, pack(jnp.zeros((8, HALF), jnp.float32), dots(pairs, c), 0)

    def nothing():
        return None

    lane_row = lax.broadcasted_iota(jnp.int32, (1, HALF), 1)
    application(
        0, lambda f, j: vec.at[1, f, 5 + j], lambda: pass_on(0), lambda: pass_on(1), halos[1][0].send
    )
    halos[1][1].send()
    halos[1][2].send()
    hear(2, expected[2])
    opening = pack(jnp.zeros((8, HALF), jnp.float32), dots(((0, 0), (1, 0))), 0)
    reductions[0].send(0, jnp.sum(opening, axis=0, keepdims=True))
    application(
        1, lambda f, j: vec.at[2, f, 5 + j], nothing,
        lambda: reductions[0].send(1, reductions[0].finish(0)), halos[2][0].send,
    )
    halos[2][1].send()
    halos[2][2].send()
    shift, gram = application(2, lambda f, j: w2.at[f, j], shift_known, nothing)
    gram = pack(gram, dots(((3, 0), (3, 1), (3, 2), (3, 3)), shift), 6)

    total = reductions[1].whole(jnp.sum(gram, axis=0, keepdims=True))
    lane1 = lax.broadcasted_iota(jnp.int32, (1, HALF), 1)
    gram_out[...] = jnp.where(lane1 == 10, shift[:, 0:HALF], total)

    for slot in list(sending):
        sent(slot)


def combine_kernel(vec, w2, y1, q, gram, basis, search, hess, b_out, s_out, h_out, out_sems):
    own_rows = pl.ds(pl.multiple_of(8 * lax.axis_index("sub"), 8), 16)

    total = gram[...]
    lane = lax.broadcasted_iota(jnp.int32, (1, HALF), 1)

    def entry(i):
        return jnp.broadcast_to(jnp.sum(jnp.where(lane == i, total, 0.0), axis=1, keepdims=True), (1, HALF))

    low = {}
    inverse = {}
    for i in range(4):
        for j in range(i + 1):
            value = entry(i * (i + 1) // 2 + j)
            for m in range(j):
                value = value - low[i, m] * low[j, m]
            if i == j:
                low[i, i] = jnp.sqrt(value)
                inverse[i] = 1.0 / low[i, i]
            else:
                low[i, j] = value * inverse[j]
    shift = entry(10)
    h = {}
    for j in range(3):
        for i in range(j + 2):
            value = low[j + 1, i]
            if j == 0 and i == 0:
                value = value + shift * low[0, 0]
            for m in range(j):
                if i <= m + 1:
                    value = value - low[j, m] * h[i, m]
            h[i, j] = value * inverse[j]
    at_row = lax.broadcasted_iota(jnp.int32, (4, HALF), 0)
    at_col = lax.broadcasted_iota(jnp.int32, (4, HALF), 1)
    table = jnp.zeros((4, HALF), jnp.float32)
    for (i, j), value in h.items():
        table = jnp.where(jnp.logical_and(at_row == i, at_col == j), value, table)
    h_out[...] = table[:, 0:3]
    writes = [pltpu.make_async_copy(h_out, hess, out_sems.at[4, 0])]
    writes[0].start()

    def wide(v):
        return jnp.concatenate([v, v], axis=1)

    scale = {key: wide(v) for key, v in low.items()}
    inv = {key: wide(v) for key, v in inverse.items()}
    c = wide(shift)

    for f in range(4):

        def body(j, _):
            raw = [vec[i, f, 5 + j, own_rows, :] for i in range(3)] + [w2[f, j]]
            found = [y1[i, f, 1 + j, own_rows, :] if f < 3 else q[i, 3 + j, own_rows, :] for i in range(3)]
            for values, dst in ((raw, b_out), (found, s_out)):
                values = values[:1] + [b - c * a for a, b in zip(values, values[1:])]
                done = []
                for i, value in enumerate(values):
                    for m in range(i):
                        value = value - scale[i, m] * done[m]
                    value = value * inv[i]
                    dst[i, f, j] = value
                    done.append(value)
            return 0

        lax.fori_loop(0, 6, body, 0, unroll=3)
        for i, (src, dst) in enumerate(((b_out, basis), (s_out, search))):
            copy = pltpu.make_async_copy(src.at[:, f], dst.at[:, f], out_sems.at[f, i])
            copy.start()
            writes.append(copy)
    for copy in writes:
        copy.wait()


def per_device(start, wind, reaction, mass):
    f32 = jnp.float32
    hbm_spec = pl.BlockSpec(memory_space=pltpu.HBM)
    vmem_spec = pl.BlockSpec(memory_space=pltpu.VMEM)
    n_send, n_receive = 14 + 5 + 4, 14 * 3 + 5 + 4
    kept = (
        jax.ShapeDtypeStruct((3, 4, 16, ROWS, 256), f32),
        jax.ShapeDtypeStruct((4, 6, 16, 256), f32),
        jax.ShapeDtypeStruct((3, 3, 8, ROWS, 256), f32),
        jax.ShapeDtypeStruct((3, 12, ROWS, 256), f32),
        jax.ShapeDtypeStruct((1, HALF), f32),
    )
    arrays = [pltpu.with_memory_space_constraint(a, pltpu.HBM) for a in (start, wind, reaction, mass)]
    outs = pl.pallas_call(
        krylov_kernel,
        out_shape=kept,
        in_specs=[hbm_spec] * 4,
        out_specs=(vmem_spec,) * 5,
        scratch_shapes=[
            pltpu.VMEM((5, 10, ROWS, 256), f32),
            pltpu.VMEM((9, 10, ROWS, 256), f32),
            pltpu.VMEM((16, ROWS, 256), f32),
            pltpu.VMEM((3, 10, ROWS, 256), f32),
            pltpu.VMEM((3, 10, ROWS, 256), f32),
            pltpu.VMEM((2, 2, 1, HALF), f32),
            pltpu.VMEM((2, 2 * NX_T * NY_T, 1, HALF), f32),
            pltpu.VMEM((2, NZ_T, 1, HALF), f32),
            pltpu.SemaphoreType.DMA((n_send,)),
            pltpu.SemaphoreType.DMA((n_receive,)),
            pltpu.SemaphoreType.DMA((4,)),
            pltpu.SemaphoreType.REGULAR((3,)),
        ],
        compiler_params=pltpu.CompilerParams(
            collective_id=0, has_side_effects=True, vmem_limit_bytes=24 * 2**20
        ),
        name="krylov",
    )(*arrays)
    return tuple(pl.pallas_call(
        combine_kernel,
        out_shape=(
            jax.ShapeDtypeStruct((4, 4, 6, 16, 256), f32),
            jax.ShapeDtypeStruct((3, 4, 6, 16, 256), f32),
            jax.ShapeDtypeStruct((4, 3), f32),
        ),
        in_specs=[vmem_spec] * 5,
        out_specs=(hbm_spec, hbm_spec, hbm_spec),
        scratch_shapes=[
            pltpu.VMEM((4, 4, 6, 16, 256), f32),
            pltpu.VMEM((3, 4, 6, 16, 256), f32),
            pltpu.VMEM((4, 3), f32),
            pltpu.SemaphoreType.DMA((5, 2)),
        ],
        compiler_params=pltpu.CompilerParams(vmem_limit_bytes=24 * 2**20),
        name="combine",
    )(*outs))


def solution(mesh):
    in_specs = (
        P(None, "slab", "sub", None),
        P(None, "slab", "sub", None),
        P("slab", "sub", None),
        P("slab", "sub", None),
    )
    out_specs = (P(None, None, "slab", "sub", None), P(None, None, "slab", "sub", None), P())
    return jax.shard_map(per_device, mesh=mesh, in_specs=in_specs, out_specs=out_specs, check_vma=False)
```
